8 devices in a mesh: dp: 1 (over z), cz: 2 (over y), cy: 2 (over x), cx: 2 (over core).
Axes of the slice: x: 2, y: 2, z: 1, core: 2. Of those that a mesh axis runs over, the one named last changes fastest.
Arguments:
- x_tokens: bfloat16 [4096, 2048], P(('dp', 'cx', 'cz'), 'cy')
- w_up: bfloat16 [2048, 16384], P('cy', ('cz', 'cx'))
- w_down: bfloat16 [16384, 2048], P('cz', ('cy', 'cx'))
Outputs:
- output: bfloat16 [4096, 2048], P(('dp', 'cx', 'cz'), 'cy')
All inputs are finite; a program needn't handle non-finite values.
Results may differ from the reference program's by a relative error of at most 0.0114676.
Values are sent between devices in bfloat16 or wider.
A program may use at most 1 GiB of HBM per device.

```python
import jax
import jax.numpy as jnp
from jax import lax

MODEL_DIM = 2048
HIDDEN_DIM = 16384
TOKENS_DEV = 512
CUBE_DEVS = 8

NUM_TOKENS = TOKENS_DEV * CUBE_DEVS


def setup_inputs(seed: int = 0, part: int = 0) -> dict:
    base_key = jax.random.key(seed)
    key_x, key_up, key_down = jax.random.split(base_key, 3)
    key_x = jax.random.fold_in(key_x, part)
    x_tokens = jax.random.normal(key_x, (NUM_TOKENS, MODEL_DIM), jnp.float32)
    w_up = jax.random.normal(key_up, (MODEL_DIM, HIDDEN_DIM), jnp.float32) * MODEL_DIM ** -0.5
    w_down = jax.random.normal(key_down, (HIDDEN_DIM, MODEL_DIM), jnp.float32) * HIDDEN_DIM ** -0.5
    return {'x_tokens': x_tokens.astype(jnp.bfloat16), 'w_up': w_up.astype(jnp.bfloat16), 'w_down': w_down.astype(jnp.bfloat16)}


def mlp_block(row_block, w_up, w_down):
    pre_act = jnp.dot(row_block, w_up, preferred_element_type=jnp.float32).astype(jnp.bfloat16)
    hidden = jax.nn.gelu(pre_act.astype(jnp.float32), approximate=True).astype(jnp.bfloat16)
    return jnp.dot(hidden, w_down, preferred_element_type=jnp.float32).astype(jnp.bfloat16)


def reference(x_tokens, w_up, w_down):
    row_blocks = x_tokens.reshape(CUBE_DEVS, TOKENS_DEV, MODEL_DIM)
    out_blocks = lax.map(lambda row_block: mlp_block(row_block, w_up, w_down), row_blocks)
    return out_blocks.reshape(NUM_TOKENS, MODEL_DIM)
```

```python
import jax
import jax.numpy as jnp
from jax import lax
from jax.sharding import PartitionSpec as P

SWAP = ((0, 1), (1, 0))
Z_CHUNKS = 4


def solution(mesh):
    data_spec = P(('dp', 'cx', 'cz'), 'cy')
    up_spec = P('cy', ('cz', 'cx'))
    down_spec = P('cz', ('cy', 'cx'))

    def local_mlp(x, w_up, w_down):
        cy = lax.axis_index('cy')
        half = w_up.shape[1] // 2
        xk = jnp.concatenate([x, lax.ppermute(x, 'cy', SWAP)], axis=1)
        x_other = lax.ppermute(xk, 'cz', SWAP)
        xs = jnp.concatenate([xk, x_other], axis=0)
        keep = lax.dynamic_slice_in_dim(w_up, cy * half, half, axis=1)
        send = lax.dynamic_slice_in_dim(w_up, (1 - cy) * half, half, axis=1)
        w1 = jnp.concatenate([keep, lax.ppermute(send, 'cy', SWAP)], axis=0)
        w1 = lax.all_gather(w1, 'cx', axis=1, tiled=True)
        pre = jnp.dot(xs, w1, preferred_element_type=jnp.float32).astype(jnp.bfloat16)
        h = jax.nn.gelu(pre.astype(jnp.float32), approximate=True).astype(jnp.bfloat16)
        w2v = w_down.reshape(2, 2, half, w_down.shape[1])
        w2k = lax.dynamic_index_in_dim(w2v, cy, axis=1, keepdims=False).reshape(2 * half, -1)
        w2s = lax.dynamic_index_in_dim(w2v, 1 - cy, axis=1, keepdims=False).reshape(2 * half, -1)
        w2r = lax.ppermute(w2s, 'cy', SWAP)
        w2_own = lax.all_gather(w2k, 'cx', axis=1, tiled=True)
        w2_oth = lax.all_gather(w2r, 'cx', axis=1, tiled=True)
        rows = x.shape[0]

        def over_z(w):
            z = jnp.dot(h, w, preferred_element_type=jnp.float32)
            return z[:rows] + lax.ppermute(z[rows:], 'cz', SWAP)

        n = w2_own.shape[1] // Z_CHUNKS
        own = [over_z(w2_own[:, c * n:(c + 1) * n]) for c in range(Z_CHUNKS)]
        oth = [over_z(w2_oth[:, c * n:(c + 1) * n]) for c in range(Z_CHUNKS)]
        out = [a + lax.ppermute(b, 'cy', SWAP) for a, b in zip(own, oth)]
        return jnp.concatenate(out, axis=1).astype(jnp.bfloat16)

    return jax.shard_map(local_mlp, mesh=mesh, in_specs=(data_spec, up_spec, down_spec), out_specs=data_spec, check_vma=False)
```

```python
import functools

import jax
import jax.numpy as jnp
from jax import lax
from jax.experimental import pallas as pl
from jax.experimental.pallas import tpu as pltpu
from jax.sharding import PartitionSpec as P

MESH = pl.DeviceIdType.MESH
F32, BF16 = jnp.float32, jnp.bfloat16
N1 = 8
N2 = 4
MT = 512
ORDER = ((0, 0), (0, 1), (1, 0), (1, 1), (1, 2), (1, 3), (0, 2), (0, 3))


def gelu(c):
    return c * (0.5 * (1.0 + jnp.tanh(0.7978845608028654 * (c + 0.044715 * (c * c * c)))))


def kernel(x, w1, w2, out, g0, g1, xg, w1g, h, w2s, ry, rx, zs, zo, ob,
           lsem, osem, xs, xr, ws, wr, vs, vr, ts, tr, ys, yr, zys, zyr,
           ds1, dr1, fs1, fr1, ds2, dr2, fs2, fr2):
    cz, cy, cx = lax.axis_index('cz'), lax.axis_index('cy'), lax.axis_index('cx')
    X, Y, D = {'cy': 1 - cy}, {'cz': 1 - cz}, {'cx': 1 - cx}
    R, K = x.shape
    HB = w1.shape[1] // 2
    WC = HB // N1
    LC = w2.shape[1] // N2

    def remote(src, dst, s, r, dev):
        return pltpu.make_async_remote_copy(src, dst, s, r, device_id=dev, device_id_type=MESH)

    barrier = pltpu.get_barrier_semaphore()
    for dev in (X, Y, D):
        pl.semaphore_signal(barrier, inc=1, device_id=dev, device_id_type=MESH)
    pl.semaphore_wait(barrier, 3)

    own, oth = pl.ds(0, R), pl.ds(R, R)
    mine = pl.multiple_of(cx * HB, HB)
    keep = pl.multiple_of(cy * HB, HB)
    give = pl.multiple_of((1 - cy) * HB, HB)

    x_x = remote(x, xg.at[own, pl.ds(K, K)], xs.at[0], xr.at[0], X)
    y_x = remote(x, xg.at[oth, pl.ds(0, K)], ys.at[0], yr.at[0], Y)
    y_xf = remote(xg.at[own, pl.ds(K, K)], xg.at[oth, pl.ds(K, K)], ys.at[1], yr.at[1], Y)
    l_x = pltpu.make_async_copy(x, xg.at[own, pl.ds(0, K)], lsem.at[0])
    l_w1 = pltpu.make_async_copy(w1.at[:, pl.ds(keep, HB)], w1g.at[pl.ds(0, K), pl.ds(mine, HB)], lsem.at[1])
    d_w1 = remote(w1.at[:, pl.ds(keep, HB)], w1g.at[pl.ds(0, K), pl.ds(mine, HB)], ds1.at[0], dr1.at[0], D)

    def x_w1(j):
        return remote(w1.at[:, pl.ds(pl.multiple_of(give + j * WC, WC), WC)],
                      w1g.at[pl.ds(K, K), pl.ds(pl.multiple_of(mine + j * WC, WC), WC)],
                      ws.at[j], wr.at[j], X)

    def f_w1(j):
        blk = w1g.at[pl.ds(K, K), pl.ds(pl.multiple_of(mine + j * WC, WC), WC)]
        return remote(blk, blk, fs1.at[j], fr1.at[j], D)

    lanes = pl.ds(pl.multiple_of(cx * LC, LC), LC)
    lanes_p = pl.ds(pl.multiple_of((1 - cx) * LC, LC), LC)

    def x_w2(c, b):
        return remote(w2.at[pl.ds(pl.multiple_of(b * 2 * HB + give, HB), HB), pl.ds(c * LC, LC)],
                      g1.at[c, pl.ds(b * HB, HB), lanes], vs.at[c * 2 + b], vr.at[c * 2 + b], X)

    def f_w2(c):
        blk = g1.at[c, :, lanes]
        return remote(blk, blk, fs2.at[c], fr2.at[c], D)

    def d_w2(c, b):
        return remote(w2.at[pl.ds(pl.multiple_of(b * 2 * HB + keep, HB), HB), pl.ds(c * LC, LC)],
                      g0.at[c, pl.ds(b * HB, HB), :], ds2.at[c * 2 + b], dr2.at[c * 2 + b], D)

    def loads(q):
        kind, c = ORDER[q]
        s = q % 2
        if kind == 1:
            return [pltpu.make_async_copy(g1.at[c], w2s.at[s], lsem.at[2 + 3 * s])]
        got = [pltpu.make_async_copy(g0.at[c], w2s.at[s, :, lanes_p], lsem.at[2 + 3 * s])]
        for b in range(2):
            got.append(pltpu.make_async_copy(
                w2.at[pl.ds(pl.multiple_of(b * 2 * HB + keep, HB), HB), pl.ds(c * LC, LC)],
                w2s.at[s, pl.ds(b * HB, HB), lanes], lsem.at[3 + 3 * s + b]))
        return got

    def z_y(q):
        return remote(zs.at[q % 2], ry.at[q], zys.at[q], zyr.at[q], Y)

    def z_x(c):
        q = ORDER.index((1, c))
        return remote(ry.at[q], rx.at[c], ts.at[c], tr.at[c], X)

    x_x.start()
    y_x.start()
    l_x.start()
    l_w1.start()
    for j in range(N1):
        x_w1(j).start()
    d_w1.start()
    for c in range(N2):
        for b in range(2):
            d_w2(c, b).start()

    def layer1(row0, rows, block, j):
        col = pl.ds(pl.multiple_of(block * HB + j * WC, WC), WC)

        @pl.loop(0, rows // MT)
        def _(i):
            r = pl.ds(pl.multiple_of(row0 + i * MT, MT), MT)
            c = jnp.dot(xg[r, :], w1g[:, col], preferred_element_type=F32)
            h[r, col] = gelu(c.astype(BF16).astype(F32)).astype(BF16)

    x_x.wait_recv()
    y_xf.start()
    l_x.wait()
    l_w1.wait()
    d_w1.wait_recv()

    def prepare(q):
        kind, c = ORDER[q]
        if kind == 1:
            x_w2(c, 0).wait_recv()
            x_w2(c, 1).wait_recv()
            f_w2(c).start()
            f_w2(c).wait_recv()
        else:
            d_w2(c, 0).wait_recv()
            d_w2(c, 1).wait_recv()
        for cp in loads(q):
            cp.start()

    @pl.loop(0, N1 // 2)
    def _(j):
        x_w1(j).wait_recv()
        f_w1(j).start()
        layer1(0, R, cx, j)
        f_w1(j).wait_recv()
        layer1(0, R, 1 - cx, j)

    y_x.wait_recv()
    y_xf.wait_recv()

    @pl.loop(0, N1 // 2)
    def _(j):
        layer1(R, R, cx, j)
        layer1(R, R, 1 - cx, j)

    prepare(0)
    prepare(1)
    for c in range(N2):
        for b in range(2):
            x_w2(c, b).start()

    @pl.loop(N1 // 2, N1)
    def _(j):
        x_w1(j).wait_recv()
        f_w1(j).start()
        layer1(0, 2 * R, cx, j)
        f_w1(j).wait_recv()
        layer1(0, 2 * R, 1 - cx, j)

    def layer2(dst, row0, s):
        @pl.loop(0, R // MT)
        def _(i):
            r = pl.multiple_of(i * MT, MT)
            dst[pl.ds(r, MT), :] = jnp.dot(h[pl.ds(row0 + r, MT), :], w2s[s], preferred_element_type=F32)

    def absorb(q):
        z_y(q).wait()
        ry[q] = ry[q] + zo[q % 2]
        kind, c = ORDER[q]
        if kind == 1:
            z_x(c).start()

    def stores(c):
        return [pltpu.make_async_copy(ob.at[c % 2, :, pl.ds(k * LC, LC)],
                                      out.at[:, pl.ds(k * N2 * LC + c * LC, LC)], osem.at[2 * c + k])
                for k in range(2)]

    def finish(c):
        z_x(c).wait_recv()
        if c >= 2:
            for cp in stores(c - 2):
                cp.wait()
        ob[c % 2] = (ry[ORDER.index((0, c))] + rx[c]).astype(BF16)
        for cp in stores(c):
            cp.start()

    last = len(ORDER) - 1
    for q in range(len(ORDER)):
        for cp in loads(q):
            cp.wait()
        layer2(zs.at[q % 2], R, q % 2)
        z_y(q).start()
        layer2(zo.at[q % 2], 0, q % 2)
        if q >= 1:
            absorb(q - 1)
        if q + 2 <= last:
            prepare(q + 2)
        if q == 5:
            finish(0)
        if q == 6:
            finish(1)
    finish(2)
    z_x(3).wait_recv()
    rx[3] = rx[3] + zo[last % 2]
    z_y(last).wait()
    for cp in stores(1):
        cp.wait()
    ob[1] = (ry[last] + rx[3]).astype(BF16)
    for cp in stores(3):
        cp.start()
    for c in (2, 3):
        for cp in stores(c):
            cp.wait()
    for cp in [x_x, y_x, y_xf, d_w1] + [z_x(c) for c in range(N2)] + [f_w2(c) for c in range(N2)]:
        cp.wait_send()
    for c in range(N2):
        for b in range(2):
            x_w2(c, b).wait_send()
            d_w2(c, b).wait_send()

    @pl.loop(0, N1)
    def _(j):
        x_w1(j).wait_send()
        f_w1(j).wait_send()


def solution(mesh):
    data_spec = P(('dp', 'cx', 'cz'), 'cy')
    up_spec = P('cy', ('cz', 'cx'))
    down_spec = P('cz', ('cy', 'cx'))

    def local_mlp(x, w1, w2):
        R, K = x.shape
        HB = w1.shape[1] // 2
        LC = w2.shape[1] // N2
        nq = len(ORDER)
        dma = pltpu.SemaphoreType.DMA
        any_spec = pl.BlockSpec(memory_space=pl.ANY)
        scratch = [
            pltpu.VMEM((2 * R, 2 * K), BF16),
            pltpu.VMEM((2 * K, 2 * HB), BF16),
            pltpu.VMEM((2 * R, 2 * HB), BF16),
            pltpu.VMEM((2, 2 * HB, 2 * LC), BF16),
            pltpu.VMEM((nq, R, 2 * LC), F32),
            pltpu.VMEM((N2, R, 2 * LC), F32),
            pltpu.VMEM((2, R, 2 * LC), F32),
            pltpu.VMEM((2, R, 2 * LC), F32),
            pltpu.VMEM((2, R, 2 * LC), BF16),
            dma((8,)), dma((8,)),
            dma((1,)), dma((1,)),
            dma((N1,)), dma((N1,)),
            dma((2 * N2,)), dma((2 * N2,)),
            dma((N2,)), dma((N2,)),
            dma((2,)), dma((2,)),
            dma((nq,)), dma((nq,)),
            dma((1,)), dma((1,)), dma((N1,)), dma((N1,)),
            dma((2 * N2,)), dma((2 * N2,)), dma((N2,)), dma((N2,)),
        ]
        z, _, _ = pl.pallas_call(
            kernel,
            out_shape=(jax.ShapeDtypeStruct((R, K), BF16),
                       jax.ShapeDtypeStruct((N2, 2 * HB, LC), BF16),
                       jax.ShapeDtypeStruct((N2, 2 * HB, 2 * LC), BF16)),
            in_specs=[any_spec] * 3,
            out_specs=(any_spec,) * 3,
            scratch_shapes=scratch,
            compiler_params=pltpu.CompilerParams(
                collective_id=0, has_side_effects=True, vmem_limit_bytes=67043328),
            name='mlp',
        )(x, w1, w2)
        return z

    return jax.shard_map(local_mlp, mesh=mesh, in_specs=(data_spec, up_spec, down_spec), out_specs=data_spec, check_vma=False)
```

```python
import jax
import jax.numpy as jnp
from jax import lax
from jax.experimental import pallas as pl
from jax.experimental.pallas import tpu as pltpu
from jax.sharding import PartitionSpec as P

MESH = pl.DeviceIdType.MESH
F32, BF16 = jnp.float32, jnp.bfloat16
NE = 12
NL = 4
NA = 3
NQ = 4
MT = 512


def gelu(c):
    return c * (0.5 * (1.0 + jnp.tanh(0.7978845608028654 * (c + 0.044715 * (c * c * c)))))


def kernel(x, w1, w2, out, ap, bo, bp, co, cp, g0, eo, ep,
           xg, he, hl, w1s, w2s, w2l, zs, ry, zo, ob,
           lsem, lw, lv, lu, osem, xs, xr, ws, wr, ys, yr, zys, zyr,
           ds, dr, fs, fr):
    cz, cy, cx = lax.axis_index('cz'), lax.axis_index('cy'), lax.axis_index('cx')
    X, Y, D = {'cy': 1 - cy}, {'cz': 1 - cz}, {'cx': 1 - cx}
    R, K = x.shape
    B1 = w1.shape[1]
    WC = B1 // (NE + NL)
    EC, LC = NE * WC, NL * WC
    C2 = w2.shape[1]
    QC = 2 * C2 // NQ

    def remote(src, dst, s, r, dev):
        return pltpu.make_async_remote_copy(src, dst, s, r, device_id=dev, device_id_type=MESH)

    barrier = pltpu.get_barrier_semaphore()
    for dev in (X, Y, D):
        pl.semaphore_signal(barrier, inc=1, device_id=dev, device_id_type=MESH)
    pl.semaphore_wait(barrier, 3)

    own, oth = pl.ds(0, R), pl.ds(R, R)
    klo, khi = pl.ds(0, K), pl.ds(K, K)

    x_x = remote(x, xg.at[own, khi], xs.at[0], xr.at[0], X)
    y_x = remote(x, xg.at[oth, klo], ys.at[0], yr.at[0], Y)
    y_xf = remote(xg.at[own, khi], xg.at[oth, khi], ys.at[1], yr.at[1], Y)
    y_w1 = remote(w1.at[:, pl.ds(EC, LC)], co, ys.at[2], yr.at[2], Y)

    def y_w2(b):
        return remote(w2.at[pl.ds(b * B1 + EC, LC), :], eo.at[b], ys.at[3 + b], yr.at[3 + b], Y)

    l_x = pltpu.make_async_copy(x, xg.at[own, klo], lsem.at[0])
    d_w1 = remote(w1, ap, ds.at[0], dr.at[0], D)
    d_w2 = remote(w2, g0, ds.at[1], dr.at[1], D)
    d_co = remote(co, cp, ds.at[2], dr.at[2], D)
    d_eo = remote(eo, ep, ds.at[3], dr.at[3], D)

    def chunk(j):
        return pl.ds(j * WC if isinstance(j, int) else pl.multiple_of(j * WC, WC), WC)

    def x_w1(j):
        return remote(w1.at[:, chunk(j)], bo.at[j], ws.at[j], wr.at[j], X)

    def x_co(k):
        return remote(co.at[:, chunk(k)], bo.at[NE + NL + k], ws.at[NE + NL + k], wr.at[NE + NL + k], X)

    def f_w1(j):
        return remote(bo.at[j], bp.at[j], fs.at[j], fr.at[j], D)

    def quads(s, j, first, second):
        return [pltpu.make_async_copy(src, w1s.at[s, rows, pl.ds(c * WC, WC)], lw.at[s, i])
                for i, (src, rows, c) in enumerate((
                    (first, klo, 0), (second, klo, 1), (bo.at[j], khi, 0), (bp.at[j], khi, 1)))]

    def quads_near(s, j):
        return quads(s, j, w1.at[:, chunk(j)], ap.at[:, chunk(j)])

    def quads_far(s, k):
        return quads(s, NE + NL + k, co.at[:, chunk(k)], cp.at[:, chunk(k)])

    base = (pl.multiple_of(cx * B1, B1), pl.multiple_of((1 - cx) * B1, B1))

    def loads(q):
        src, c = (w2, q) if q < NQ // 2 else (g0, q - NQ // 2)
        return [pltpu.make_async_copy(src.at[pl.ds(base[b], EC), pl.ds(c * QC, QC)],
                                      w2s.at[q % 2, pl.ds(b * EC, EC), :], lv.at[q % 2, b]) for b in range(2)]

    def late_near(s, k):
        got = []
        for b in range(2):
            rows = pl.ds(pl.multiple_of(base[b] + EC + k * WC, WC), WC)
            for c, src in enumerate((w2, g0)):
                got.append(pltpu.make_async_copy(
                    src.at[rows, :], w2l.at[s, pl.ds(b * WC, WC), pl.ds(c * C2, C2)], lu.at[s, 2 * b + c]))
        return got

    def late_far(s, k):
        got = []
        for b, blk in enumerate((cx, 1 - cx)):
            for c, src in enumerate((eo, ep)):
                got.append(pltpu.make_async_copy(
                    src.at[blk, chunk(k), :], w2l.at[s, pl.ds(b * WC, WC), pl.ds(c * C2, C2)], lu.at[s, 2 * b + c]))
        return got

    def z_y(q):
        return remote(zs.at[q], ry.at[q], zys.at[q], zyr.at[q], Y)

    def layer1(dst, col, row0, rows, s, half):
        @pl.loop(0, rows // MT)
        def _(i):
            r = pl.multiple_of(i * MT, MT)
            c = jnp.dot(xg[pl.ds(row0 + r, MT), :], w1s[s, :, pl.ds(half * WC, WC)], preferred_element_type=F32)
            dst[pl.ds(row0 + r, MT), pl.ds(col, WC)] = gelu(c.astype(BF16).astype(F32)).astype(BF16)

    def step(j, k, near, quad, body):
        s = lax.rem(j, 2)
        q = quad(s, k)
        q[0].start()
        q[1].start()
        f = f_w1(j)
        (x_w1(j) if near else x_co(k)).wait_recv()
        f.start()
        q[2].start()
        q[0].wait()
        q[2].wait()
        body(s, 0)
        f.wait_recv()
        q[3].start()
        q[1].wait()
        q[3].wait()
        body(s, 1)

    x_x.start()
    y_x.start()
    l_x.start()
    for j in range(NE):
        x_w1(j).start()
    d_w1.start()
    d_w2.start()
    for q in range(2):
        for c in loads(q):
            c.start()

    x_x.wait_recv()
    y_xf.start()
    y_w1.start()
    y_w2(0).start()
    y_w2(1).start()
    l_x.wait()
    d_w1.wait_recv()

    def col(j, half):
        return pl.multiple_of(half * EC + j * WC, WC)

    @pl.loop(0, NA)
    def _(j):
        step(j, j, True, quads_near, lambda s, half: layer1(he, col(j, half), 0, R, s, half))

    y_x.wait_recv()
    y_xf.wait_recv()

    @pl.loop(0, NA)
    def _(j):
        s = lax.rem(j, 2)
        for c in quads_near(s, j):
            c.start()
        for c in quads_near(s, j):
            c.wait()
        for half in range(2):
            layer1(he, col(j, half), R, R, s, half)

    def early(lo, hi):
        @pl.loop(lo, hi)
        def _(j):
            step(j, j, True, quads_near, lambda s, half: layer1(he, col(j, half), 0, 2 * R, s, half))

    early(NA, 8)
    y_w1.wait_recv()
    for k in range(NL):
        x_w1(NE + k).start()
    for k in range(NL):
        x_co(k).start()
    d_co.start()
    y_w2(0).wait_recv()
    y_w2(1).wait_recv()
    d_eo.start()
    early(8, NE)

    d_w2.wait_recv()
    for q in range(NQ):
        for c in loads(q):
            c.wait()

        @pl.loop(0, R // MT)
        def _(i):
            r = pl.multiple_of(i * MT, MT)
            zs[q, pl.ds(r, MT), :] = jnp.dot(he[pl.ds(R + r, MT), :], w2s[q % 2], preferred_element_type=F32)

        z_y(q).start()

        @pl.loop(0, R // MT)
        def _(i):
            r = pl.multiple_of(i * MT, MT)
            zo[pl.ds(r, MT), pl.ds(q * QC, QC)] = jnp.dot(he[pl.ds(r, MT), :], w2s[q % 2], preferred_element_type=F32)

        if q + 2 < NQ:
            for c in loads(q + 2):
                c.start()

    d_co.wait_recv()
    d_eo.wait_recv()

    def late(near):
        off = NE if near else NE + NL
        quad = quads_near if near else quads_far
        lo = NE if near else 0

        @pl.loop(0, NL)
        def _(k):
            s = lax.rem(off + k, 2)
            lw2 = late_near(s, k) if near else late_far(s, k)
            for c in lw2:
                c.start()
            step(off + k, lo + k, near, quad, lambda s, half: layer1(hl, half * WC, 0, R, s, half))
            for c in lw2:
                c.wait()

            @pl.loop(0, R // MT)
            def _(i):
                r = pl.ds(pl.multiple_of(i * MT, MT), MT)
                zo[r, :] = zo[r, :] + jnp.dot(hl[r, :], w2l[s], preferred_element_type=F32)

    late(True)
    late(False)

    def store(q):
        half, c = divmod(q, NQ // 2)
        lanes = pl.multiple_of((1 - cx if half else cx) * C2 + c * QC, QC)
        return pltpu.make_async_copy(ob.at[:, pl.ds(q * QC, QC)], out.at[:, pl.ds(lanes, QC)], osem.at[q])

    for q in range(NQ):
        z_y(q).wait_recv()
        ob[:, pl.ds(q * QC, QC)] = (zo[:, pl.ds(q * QC, QC)] + ry[q]).astype(BF16)
        store(q).start()
    for q in range(NQ):
        z_y(q).wait_send()
        store(q).wait()
    for c in [x_x, y_x, y_xf, y_w1, y_w2(0), y_w2(1), d_w1, d_w2, d_co, d_eo]:
        c.wait_send()

    @pl.loop(0, NE + NL)
    def _(j):
        x_w1(j).wait_send()

    @pl.loop(0, NL)
    def _(k):
        x_co(k).wait_send()

    @pl.loop(0, NE + 2 * NL)
    def _(j):
        f_w1(j).wait_send()


def solution(mesh):
    data_spec = P(('dp', 'cx', 'cz'), 'cy')
    up_spec = P('cy', ('cz', 'cx'))
    down_spec = P('cz', ('cy', 'cx'))

    def local_mlp(x, w1, w2):
        R, K = x.shape
        B1 = w1.shape[1]
        WC = B1 // (NE + NL)
        EC, LC = NE * WC, NL * WC
        C2 = w2.shape[1]
        QC = 2 * C2 // NQ
        NX = NE + 2 * NL
        dma = pltpu.SemaphoreType.DMA
        any_spec = pl.BlockSpec(memory_space=pl.ANY)
        sds = jax.ShapeDtypeStruct
        outs = (
            sds((R, K), BF16),
            sds(w1.shape, BF16),
            sds((NX, K, WC), BF16),
            sds((NX, K, WC), BF16),
            sds((K, LC), BF16),
            sds((K, LC), BF16),
            sds(w2.shape, BF16),
            sds((2, LC, C2), BF16),
            sds((2, LC, C2), BF16),
        )
        scratch = [
            pltpu.VMEM((2 * R, 2 * K), BF16),
            pltpu.VMEM((2 * R, 2 * EC), BF16),
            pltpu.VMEM((R, 2 * WC), BF16),
            pltpu.VMEM((2, 2 * K, 2 * WC), BF16),
            pltpu.VMEM((2, 2 * EC, QC), BF16),
            pltpu.VMEM((2, 2 * WC, 2 * C2), BF16),
            pltpu.VMEM((NQ, R, QC), F32),
            pltpu.VMEM((NQ, R, QC), F32),
            pltpu.VMEM((R, 2 * C2), F32),
            pltpu.VMEM((R, 2 * C2), BF16),
            dma((1,)), dma((2, 4)), dma((2, 2)), dma((2, 4)), dma((NQ,)),
            dma((1,)), dma((1,)),
            dma((NX,)), dma((NX,)),
            dma((5,)), dma((5,)),
            dma((NQ,)), dma((NQ,)),
            dma((4,)), dma((4,)),
            dma((NX,)), dma((NX,)),
        ]
        return pl.pallas_call(
            kernel,
            out_shape=outs,
            in_specs=[any_spec] * 3,
            out_specs=(any_spec,) * len(outs),
            scratch_shapes=scratch,
            compiler_params=pltpu.CompilerParams(
                collective_id=0, has_side_effects=True, vmem_limit_bytes=67043328),
            name='mlp',
        )(x, w1, w2)[0]

    return jax.shard_map(local_mlp, mesh=mesh, in_specs=(data_spec, up_spec, down_spec), out_specs=data_spec, check_vma=False)
```

```python
import jax
import jax.numpy as jnp
from jax import lax
from jax.experimental import pallas as pl
from jax.experimental.pallas import tpu as pltpu
from jax.sharding import PartitionSpec as P

MESH = pl.DeviceIdType.MESH
F32, BF16 = jnp.float32, jnp.bfloat16
NE = 12
NL = 4
NA = 3
NQ = 4
MT = 512


def gelu(c):
    return c * (0.5 * (1.0 + jnp.tanh(0.7978845608028654 * (c + 0.044715 * (c * c * c)))))


def kernel(x, w1, w2, out, ap, bo, bp, co, cp, g0, eo, ep,
           xg, he, hl, w1s, w1d, w2s, w2l, zs, ry, zo, ob,
           lsem, lw, lv, lu, osem, xs, xr, ws, wr, ys, yr, zys, zyr,
           ds, dr, fs, fr):
    cz, cy, cx = lax.axis_index('cz'), lax.axis_index('cy'), lax.axis_index('cx')
    X, Y, D = {'cy': 1 - cy}, {'cz': 1 - cz}, {'cx': 1 - cx}
    R, K = x.shape
    B1 = w1.shape[1]
    WC = B1 // (NE + NL)
    EC, LC = NE * WC, NL * WC
    C2 = w2.shape[1]
    QC = 2 * C2 // NQ

    def remote(src, dst, s, r, dev):
        return pltpu.make_async_remote_copy(src, dst, s, r, device_id=dev, device_id_type=MESH)

    barrier = pltpu.get_barrier_semaphore()
    for dev in (X, Y, D):
        pl.semaphore_signal(barrier, inc=1, device_id=dev, device_id_type=MESH)
    pl.semaphore_wait(barrier, 3)

    own, oth = pl.ds(0, R), pl.ds(R, R)
    klo, khi = pl.ds(0, K), pl.ds(K, K)

    x_x = remote(x, xg.at[own, khi], xs.at[0], xr.at[0], X)
    y_x = remote(x, xg.at[oth, klo], ys.at[0], yr.at[0], Y)
    y_xf = remote(xg.at[own, khi], xg.at[oth, khi], ys.at[1], yr.at[1], Y)
    y_w1 = remote(w1.at[:, pl.ds(EC, LC)], co, ys.at[2], yr.at[2], Y)

    def y_w2(b):
        return remote(w2.at[pl.ds(b * B1 + EC, LC), :], eo.at[b], ys.at[3 + b], yr.at[3 + b], Y)

    l_x = pltpu.make_async_copy(x, xg.at[own, klo], lsem.at[0])
    d_w1 = remote(w1, ap, ds.at[0], dr.at[0], D)
    d_w2 = remote(w2, g0, ds.at[1], dr.at[1], D)
    d_co = remote(co, cp, ds.at[2], dr.at[2], D)
    d_eo = remote(eo, ep, ds.at[3], dr.at[3], D)

    def chunk(j):
        return pl.ds(j * WC if isinstance(j, int) else pl.multiple_of(j * WC, WC), WC)

    lo_c, hi_c = pl.ds(0, WC), pl.ds(WC, WC)

    def x_w1(j):
        dst = w1d.at[0, :, lo_c] if isinstance(j, int) and j == NE - 1 else bo.at[j]
        return remote(w1.at[:, chunk(j)], dst, ws.at[j], wr.at[j], X)

    def x_co(k):
        dst = w1d.at[1, :, lo_c] if isinstance(k, int) and k == NL - 1 else bo.at[NE + NL + k]
        return remote(co.at[:, chunk(k)], dst, ws.at[NE + NL + k], wr.at[NE + NL + k], X)

    def f_w1(j):
        return remote(bo.at[j], bp.at[j], fs.at[j], fr.at[j], D)

    def f_w1d(i):
        j = (NE - 1, NE + 2 * NL - 1)[i]
        return remote(w1d.at[i, :, lo_c], w1d.at[i, :, hi_c], fs.at[j], fr.at[j], D)

    def quads(s, j, first, second):
        return [pltpu.make_async_copy(src, w1s.at[s, rows, pl.ds(c * WC, WC)], lw.at[s, i])
                for i, (src, rows, c) in enumerate((
                    (first, klo, 0), (second, klo, 1), (bo.at[j], khi, 0), (bp.at[j], khi, 1)))]

    def quads_near(s, j):
        return quads(s, j, w1.at[:, chunk(j)], ap.at[:, chunk(j)])

    def quads_far(s, k):
        return quads(s, NE + NL + k, co.at[:, chunk(k)], cp.at[:, chunk(k)])

    base = (pl.multiple_of(cx * B1, B1), pl.multiple_of((1 - cx) * B1, B1))

    def loads(q):
        src, c = (w2, q) if q < NQ // 2 else (g0, q - NQ // 2)
        return [pltpu.make_async_copy(src.at[pl.ds(base[b], EC), pl.ds(c * QC, QC)],
                                      w2s.at[q % 2, pl.ds(b * EC, EC), :], lv.at[q % 2, b]) for b in range(2)]

    def late_near(s, k):
        got = []
        for b in range(2):
            rows = pl.ds(pl.multiple_of(base[b] + EC + k * WC, WC), WC)
            for c, src in enumerate((w2, g0)):
                got.append(pltpu.make_async_copy(
                    src.at[rows, :], w2l.at[s, pl.ds(b * WC, WC), pl.ds(c * C2, C2)], lu.at[s, 2 * b + c]))
        return got

    def late_far(s, k):
        got = []
        for b, blk in enumerate((cx, 1 - cx)):
            for c, src in enumerate((eo, ep)):
                got.append(pltpu.make_async_copy(
                    src.at[blk, chunk(k), :], w2l.at[s, pl.ds(b * WC, WC), pl.ds(c * C2, C2)], lu.at[s, 2 * b + c]))
        return got

    NP = R // MT

    def z_y(q, i):
        rows = pl.ds(i * MT if isinstance(i, int) else pl.multiple_of(i * MT, MT), MT)
        return remote(zs.at[q, rows, :], ry.at[q, rows, :], zys.at[q * NP + i], zyr.at[q * NP + i], Y)

    def layer1(dst, col, row0, rows, s, half):
        @pl.loop(0, rows // MT)
        def _(i):
            r = pl.multiple_of(i * MT, MT)
            c = jnp.dot(xg[pl.ds(row0 + r, MT), :], w1s[s, :, pl.ds(half * WC, WC)], preferred_element_type=F32)
            dst[pl.ds(row0 + r, MT), pl.ds(col, WC)] = gelu(c.astype(BF16).astype(F32)).astype(BF16)

    def layer1d(dst, col, row0, rows, s, half, i):
        lanes = pl.ds(half * WC, WC)

        @pl.loop(0, rows // MT)
        def _(n):
            r = pl.ds(pl.multiple_of(row0 + n * MT, MT), MT)
            c = (jnp.dot(xg[r, klo], w1s[s, klo, lanes], preferred_element_type=F32)
                 + jnp.dot(xg[r, khi], w1d[i, :, lanes], preferred_element_type=F32))
            dst[r, pl.ds(col, WC)] = gelu(c.astype(BF16).astype(F32)).astype(BF16)

    def step(j, k, near, quad, body):
        s = lax.rem(j, 2)
        q = quad(s, k)
        q[0].start()
        q[1].start()
        f = f_w1(j)
        with jax.named_scope('xw'):
            (x_w1(j) if near else x_co(k)).wait_recv()
        f.start()
        q[2].start()
        q[0].wait()
        q[2].wait()
        body(s, 0)
        f.wait_recv()
        q[3].start()
        q[1].wait()
        q[3].wait()
        body(s, 1)

    x_x.start()
    y_x.start()
    l_x.start()
    for j in range(NE):
        x_w1(j).start()
    d_w1.start()
    d_w2.start()
    for q in range(2):
        for c in loads(q):
            c.start()

    with jax.named_scope('xx'):
        x_x.wait_recv()
    y_xf.start()
    y_w1.start()
    y_w2(0).start()
    y_w2(1).start()
    l_x.wait()
    d_w1.wait_recv()

    def col(j, half):
        return pl.multiple_of(half * EC + j * WC, WC)

    @pl.loop(0, NA)
    def _(j):
        step(j, j, True, quads_near, lambda s, half: layer1(he, col(j, half), 0, R, s, half))

    with jax.named_scope('yx'):
        y_x.wait_recv()
        y_xf.wait_recv()

    @pl.loop(0, NA)
    def _(j):
        s = lax.rem(j, 2)
        for c in quads_near(s, j):
            c.start()
        for c in quads_near(s, j):
            c.wait()
        for half in range(2):
            layer1(he, col(j, half), R, R, s, half)

    def early(lo, hi):
        @pl.loop(lo, hi)
        def _(j):
            step(j, j, True, quads_near, lambda s, half: layer1(he, col(j, half), 0, 2 * R, s, half))

    early(NA, 8)
    y_w1.wait_recv()
    for k in range(NL):
        x_w1(NE + k).start()
    for k in range(NL):
        x_co(k).start()
    d_co.start()
    early(8, NE - 1)

    j, s = NE - 1, (NE - 1) % 2
    near = quads_near(s, j)
    near[0].start()
    near[1].start()
    d_w2.wait_recv()
    for c in loads(0) + loads(1):
        c.wait()
    near[0].wait()
    near[1].wait()
    with jax.named_scope('xw_last'):
        x_w1(j).wait_recv()
    f_w1d(0).start()
    with jax.named_scope('c0_last'):
        layer1d(he, col(j, 0), R, R, s, 0, 0)
    with jax.named_scope('fw_last'):
        f_w1d(0).wait_recv()
    with jax.named_scope('c1_last'):
        layer1d(he, col(j, 1), R, R, s, 1, 0)

    def z_other(q):
        @pl.loop(0, NP)
        def _(i):
            r = pl.multiple_of(i * MT, MT)
            zs[q, pl.ds(r, MT), :] = jnp.dot(he[pl.ds(R + r, MT), :], w2s[q % 2], preferred_element_type=F32)
            z_y(q, i).start()

    def z_own(q):
        @pl.loop(0, NP)
        def _(i):
            r = pl.ds(pl.multiple_of(i * MT, MT), MT)
            zo[r, pl.ds(q * QC, QC)] = jnp.dot(he[r, :], w2s[q % 2], preferred_element_type=F32)

    z_other(0)
    layer1d(he, col(j, 0), 0, R, s, 0, 0)
    layer1d(he, col(j, 1), 0, R, s, 1, 0)
    for q in range(NQ):
        if q:
            if q >= 2:
                for c in loads(q):
                    c.wait()
            with jax.named_scope('zs'):
                z_other(q)
        with jax.named_scope('zo'):
            z_own(q)
        if q + 2 < NQ:
            for c in loads(q + 2):
                c.start()
        if q == 0:
            with jax.named_scope('yw2'):
                y_w2(0).wait_recv()
                y_w2(1).wait_recv()
            d_eo.start()

    d_co.wait_recv()
    d_eo.wait_recv()

    def second(s):
        for c in quads_near(s, 0)[1::2]:
            c.wait()
        layer1(hl, WC, 0, R, s, 1)
        layer2(s)

    def layer2(s):
        for c in late_near(s, 0):
            c.wait()

        @pl.loop(0, NP)
        def _(i):
            r = pl.ds(pl.multiple_of(i * MT, MT), MT)
            zo[r, :] = zo[r, :] + jnp.dot(hl[r, :], w2l[s], preferred_element_type=F32)

    def late(near, n):
        off = NE if near else NE + NL

        @pl.loop(0, n)
        def _(k):
            s = lax.rem(off + k, 2)
            quad = quads_near(s, NE + k) if near else quads_far(s, k)
            for c in quad[:2] + (late_near(s, k) if near else late_far(s, k)):
                c.start()
            with jax.named_scope('xl'):
                (x_w1(NE + k) if near else x_co(k)).wait_recv()
            f = f_w1(off + k)
            f.start()
            quad[2].start()
            if near:
                @pl.when(k > 0)
                def _():
                    second(1 - s)
            else:
                second(1 - s)
            quad[0].wait()
            quad[2].wait()
            with jax.named_scope('c0'):
                layer1(hl, 0, 0, R, s, 0)
            with jax.named_scope('fw'):
                f.wait_recv()
            quad[3].start()

    late(True, NL)
    late(False, NL - 1)
    k, s = NL - 1, (NE + 2 * NL - 1) % 2
    quad = quads_far(s, k)
    for c in quad[:2] + late_far(s, k):
        c.start()
    second(1 - s)
    quad[0].wait()
    quad[1].wait()
    with jax.named_scope('xl_last'):
        x_co(k).wait_recv()
    f_w1d(1).start()
    with jax.named_scope('c0'):
        layer1d(hl, 0, 0, R, s, 0, 1)
    with jax.named_scope('fw'):
        f_w1d(1).wait_recv()
    with jax.named_scope('c1'):
        layer1d(hl, WC, 0, R, s, 1, 1)
    with jax.named_scope('l2'):
        layer2(s)

    def store(q, i):
        half, c = divmod(q, NQ // 2)
        rows = pl.ds(i * MT, MT)
        lanes = pl.multiple_of((1 - cx if half else cx) * C2 + c * QC, QC)
        return pltpu.make_async_copy(ob.at[rows, pl.ds(q * QC, QC)], out.at[rows, pl.ds(lanes, QC)], osem.at[q * NP + i])

    pieces = [(q, i) for q in range(NQ) for i in range(NP)]
    for q, i in pieces:
        with jax.named_scope('zw'):
            z_y(q, i).wait_recv()
        r, l = pl.ds(i * MT, MT), pl.ds(q * QC, QC)
        ob[r, l] = (zo[r, l] + ry[q, r, :]).astype(BF16)
        store(q, i).start()
    with jax.named_scope('drain'):
        for q, i in pieces:
            z_y(q, i).wait_send()
    for c in [x_x, y_x, y_xf, y_w1, y_w2(0), y_w2(1), d_w1, d_w2, d_co, d_eo, f_w1d(0), f_w1d(1), x_w1(NE - 1), x_co(NL - 1)]:
        c.wait_send()

    def drain(lo, hi, copy):
        @pl.loop(lo, hi)
        def _(j):
            copy(j).wait_send()

    drain(0, NE - 1, x_w1)
    drain(NE, NE + NL, x_w1)
    drain(0, NL - 1, x_co)
    drain(0, NE - 1, f_w1)
    drain(NE, NE + 2 * NL - 1, f_w1)
    with jax.named_scope('store'):
        for q, i in pieces:
            store(q, i).wait()


def solution(mesh):
    data_spec = P(('dp', 'cx', 'cz'), 'cy')
    up_spec = P('cy', ('cz', 'cx'))
    down_spec = P('cz', ('cy', 'cx'))

    def local_mlp(x, w1, w2):
        R, K = x.shape
        B1 = w1.shape[1]
        WC = B1 // (NE + NL)
        EC, LC = NE * WC, NL * WC
        C2 = w2.shape[1]
        QC = 2 * C2 // NQ
        NX = NE + 2 * NL
        dma = pltpu.SemaphoreType.DMA
        any_spec = pl.BlockSpec(memory_space=pl.ANY)
        sds = jax.ShapeDtypeStruct
        outs = (
            sds((R, K), BF16),
            sds(w1.shape, BF16),
            sds((NX, K, WC), BF16),
            sds((NX, K, WC), BF16),
            sds((K, LC), BF16),
            sds((K, LC), BF16),
            sds(w2.shape, BF16),
            sds((2, LC, C2), BF16),
            sds((2, LC, C2), BF16),
        )
        scratch = [
            pltpu.VMEM((2 * R, 2 * K), BF16),
            pltpu.VMEM((2 * R, 2 * EC), BF16),
            pltpu.VMEM((R, 2 * WC), BF16),
            pltpu.VMEM((2, 2 * K, 2 * WC), BF16),
            pltpu.VMEM((2, K, 2 * WC), BF16),
            pltpu.VMEM((2, 2 * EC, QC), BF16),
            pltpu.VMEM((2, 2 * WC, 2 * C2), BF16),
            pltpu.VMEM((NQ, R, QC), F32),
            pltpu.VMEM((NQ, R, QC), F32),
            pltpu.VMEM((R, 2 * C2), F32),
            pltpu.VMEM((R, 2 * C2), BF16),
            dma((1,)), dma((2, 4)), dma((2, 2)), dma((2, 4)), dma((NQ * R // MT,)),
            dma((1,)), dma((1,)),
            dma((NX,)), dma((NX,)),
            dma((5,)), dma((5,)),
            dma((NQ * R // MT,)), dma((NQ * R // MT,)),
            dma((4,)), dma((4,)),
            dma((NX,)), dma((NX,)),
        ]
        return pl.pallas_call(
            kernel,
            out_shape=outs,
            in_specs=[any_spec] * 3,
            out_specs=(any_spec,) * len(outs),
            scratch_shapes=scratch,
            compiler_params=pltpu.CompilerParams(
                collective_id=0, has_side_effects=True, vmem_limit_bytes=67043328),
            name='mlp',
        )(x, w1, w2)[0]

    return jax.shard_map(local_mlp, mesh=mesh, in_specs=(data_spec, up_spec, down_spec), out_specs=data_spec, check_vma=False)
```

```python
import jax
import jax.numpy as jnp
from jax import lax
from jax.experimental import pallas as pl
from jax.experimental.pallas import tpu as pltpu
from jax.sharding import PartitionSpec as P

MESH = pl.DeviceIdType.MESH
F32, BF16 = jnp.float32, jnp.bfloat16
NE = 12
NL = 4
NA = 3
NQ = 4
MT = 512


def gelu(c):
    return c * (0.5 * (1.0 + jnp.tanh(0.7978845608028654 * (c + 0.044715 * (c * c * c)))))


def kernel(x, w1, w2, out, ap, bo, bp, co, cp, g0, eo, ep,
           xg, he, hl, w1s, w1d, w2s, w2l, zs, ry, zo, ob,
           lsem, lw, lv, lu, osem, xs, xr, ws, wr, ys, yr, zys, zyr,
           ds, dr, fs, fr):
    cz, cy, cx = lax.axis_index('cz'), lax.axis_index('cy'), lax.axis_index('cx')
    X, Y, D = {'cy': 1 - cy}, {'cz': 1 - cz}, {'cx': 1 - cx}
    R, K = x.shape
    B1 = w1.shape[1]
    WC = B1 // (NE + NL)
    EC, LC = NE * WC, NL * WC
    C2 = w2.shape[1]
    QC = 2 * C2 // NQ

    def remote(src, dst, s, r, dev):
        return pltpu.make_async_remote_copy(src, dst, s, r, device_id=dev, device_id_type=MESH)

    barrier = pltpu.get_barrier_semaphore()
    for dev in (X, Y, D):
        pl.semaphore_signal(barrier, inc=1, device_id=dev, device_id_type=MESH)
    pl.semaphore_wait(barrier, 3)

    own, oth = pl.ds(0, R), pl.ds(R, R)
    klo, khi = pl.ds(0, K), pl.ds(K, K)

    x_x = remote(x, xg.at[own, khi], xs.at[0], xr.at[0], X)
    y_x = remote(x, xg.at[oth, klo], ys, yr.at[0], Y)
    y_xf = remote(xg.at[own, khi], xg.at[oth, khi], ys, yr.at[1], Y)
    y_w1 = remote(w1.at[:, pl.ds(EC, LC)], co, ys, yr.at[2], Y)

    def y_w2(b):
        return remote(w2.at[pl.ds(b * B1 + EC, LC), :], eo.at[b], ys, yr.at[3], Y)

    l_x = pltpu.make_async_copy(x, xg.at[own, klo], lsem.at[0])
    d_w1 = remote(w1, ap, ds.at[0], dr.at[0], D)
    d_w2 = remote(w2, g0, ds.at[1], dr.at[1], D)
    d_co = remote(co, cp, ds.at[2], dr.at[2], D)
    d_eo = remote(eo, ep, ds.at[3], dr.at[3], D)

    def chunk(j):
        return pl.ds(j * WC if isinstance(j, int) else pl.multiple_of(j * WC, WC), WC)

    lo_c, hi_c = pl.ds(0, WC), pl.ds(WC, WC)

    def x_w1(j):
        dst = w1d.at[0, :, lo_c] if isinstance(j, int) and j == NE - 1 else bo.at[j]
        return remote(w1.at[:, chunk(j)], dst, ws, wr.at[j], X)

    def x_co(k):
        dst = w1d.at[1, :, lo_c] if isinstance(k, int) and k == NL - 1 else bo.at[NE + NL + k]
        return remote(co.at[:, chunk(k)], dst, ws, wr.at[NE + NL + k], X)

    def f_w1(j):
        return remote(bo.at[j], bp.at[j], fs, fr.at[j], D)

    def f_w1d(i):
        j = (NE - 1, NE + 2 * NL - 1)[i]
        return remote(w1d.at[i, :, lo_c], w1d.at[i, :, hi_c], fs, fr.at[j], D)

    def quads(s, j, first, second):
        return [pltpu.make_async_copy(src, w1s.at[s, rows, pl.ds(c * WC, WC)], lw.at[s, i])
                for src, rows, c, i in (
                    (first, klo, 0, 0), (second, klo, 1, 0), (bo.at[j], khi, 0, 1), (bp.at[j], khi, 1, 2))]

    def wait_tiles(s, i):
        if i == 0:
            pltpu.make_async_copy(w1.at[:, pl.ds(0, 2 * WC)], w1s.at[s, klo, :], lw.at[s, 0]).wait()
        else:
            pltpu.make_async_copy(bo.at[0], w1s.at[s, khi, pl.ds((i - 1) * WC, WC)], lw.at[s, i]).wait()

    def wait_w2s(q):
        pltpu.make_async_copy(w2.at[pl.ds(0, 2 * EC), pl.ds(0, QC)], w2s.at[q % 2], lv.at[q % 2]).wait()

    def wait_w2l(s):
        pltpu.make_async_copy(w1.at[pl.ds(0, 2 * WC), pl.ds(0, 2 * C2)], w2l.at[s], lu.at[s]).wait()

    def quads_near(s, j):
        return quads(s, j, w1.at[:, chunk(j)], ap.at[:, chunk(j)])

    def quads_far(s, k):
        return quads(s, NE + NL + k, co.at[:, chunk(k)], cp.at[:, chunk(k)])

    base = (pl.multiple_of(cx * B1, B1), pl.multiple_of((1 - cx) * B1, B1))

    def loads(q):
        src, c = (w2, q) if q < NQ // 2 else (g0, q - NQ // 2)
        return [pltpu.make_async_copy(src.at[pl.ds(base[b], EC), pl.ds(c * QC, QC)],
                                      w2s.at[q % 2, pl.ds(b * EC, EC), :], lv.at[q % 2]) for b in range(2)]

    def late_near(s, k):
        got = []
        for b in range(2):
            rows = pl.ds(pl.multiple_of(base[b] + EC + k * WC, WC), WC)
            for c, src in enumerate((w2, g0)):
                got.append(pltpu.make_async_copy(
                    src.at[rows, :], w2l.at[s, pl.ds(b * WC, WC), pl.ds(c * C2, C2)], lu.at[s]))
        return got

    def late_far(s, k):
        got = []
        for b, blk in enumerate((cx, 1 - cx)):
            for c, src in enumerate((eo, ep)):
                got.append(pltpu.make_async_copy(
                    src.at[blk, chunk(k), :], w2l.at[s, pl.ds(b * WC, WC), pl.ds(c * C2, C2)], lu.at[s]))
        return got

    NP = R // MT

    def z_y(q, i):
        rows = pl.ds(i * MT if isinstance(i, int) else pl.multiple_of(i * MT, MT), MT)
        return remote(zs.at[q, rows, :], ry.at[q, rows, :], zys, zyr.at[0 if q < NQ - 1 else 1 + i], Y)

    def layer1(dst, col, row0, rows, s, half):
        @pl.loop(0, rows // MT)
        def _(i):
            r = pl.multiple_of(i * MT, MT)
            c = jnp.dot(xg[pl.ds(row0 + r, MT), :], w1s[s, :, pl.ds(half * WC, WC)], preferred_element_type=F32)
            dst[pl.ds(row0 + r, MT), pl.ds(col, WC)] = gelu(c.astype(BF16).astype(F32)).astype(BF16)

    def layer1d(dst, col, row0, rows, s, half, i):
        lanes = pl.ds(half * WC, WC)

        @pl.loop(0, rows // MT)
        def _(n):
            r = pl.ds(pl.multiple_of(row0 + n * MT, MT), MT)
            c = (jnp.dot(xg[r, klo], w1s[s, klo, lanes], preferred_element_type=F32)
                 + jnp.dot(xg[r, khi], w1d[i, :, lanes], preferred_element_type=F32))
            dst[r, pl.ds(col, WC)] = gelu(c.astype(BF16).astype(F32)).astype(BF16)

    def step(j):
        s = lax.rem(j, 2)
        q = quads_near(s, j)
        q[0].start()
        q[1].start()
        x_w1(j).wait_recv()
        f_w1(j).start()
        q[2].start()
        wait_tiles(s, 0)
        wait_tiles(s, 1)
        layer1(he, col(j, 0), 0, R, s, 0)
        f_w1(j).wait_recv()
        q[3].start()
        wait_tiles(s, 2)
        layer1(he, col(j, 1), 0, R, s, 1)

    def col(j, half):
        return half * EC + j * WC if isinstance(j, int) else pl.multiple_of(half * EC + j * WC, WC)

    x_x.start()
    y_x.start()
    l_x.start()
    for j in range(NE):
        x_w1(j).start()
    d_w1.start()
    d_w2.start()
    for q in range(2):
        for c in loads(q):
            c.start()

    with jax.named_scope('xx'):
        x_x.wait_recv()
    y_xf.start()
    y_w1.start()
    y_w2(0).start()
    y_w2(1).start()
    l_x.wait()
    d_w1.wait_recv()

    @pl.loop(0, NA)
    def _(j):
        step(j)

    with jax.named_scope('yx'):
        y_x.wait_recv()
        y_xf.wait_recv()

    for n, j in enumerate((2, 1, 0)):
        if n == 2:
            for i in range(3):
                wait_tiles(0, i)
        for half in range(2):
            layer1(he, col(j, half), R, R, j % 2, half)
        if n == 0:
            for c in quads_near(0, 0):
                c.start()
        if n == 1:
            for c in quads_near(NA % 2, NA)[:2]:
                c.start()

    def early_second(j, s):
        wait_tiles(s, 2)
        layer1(he, col(j, 1), 0, 2 * R, s, 1)

    def early(lo, hi):
        @pl.loop(lo, hi)
        def _(j):
            s = lax.rem(j, 2)
            with jax.named_scope('xw'):
                x_w1(j).wait_recv()
            f_w1(j).start()
            q = quads_near(s, j)
            q[2].start()
            if lo == NA:
                @pl.when(j > lo)
                def _():
                    early_second(j - 1, 1 - s)
            else:
                early_second(j - 1, 1 - s)
            for c in quads_near(1 - s, j + 1)[:2]:
                c.start()
            wait_tiles(s, 0)
            wait_tiles(s, 1)
            layer1(he, col(j, 0), 0, 2 * R, s, 0)
            f_w1(j).wait_recv()
            q[3].start()

    early(NA, 8)
    y_w1.wait_recv()
    for k in range(NL):
        x_w1(NE + k).start()
    for k in range(NL):
        x_co(k).start()
    d_co.start()
    early(8, NE - 1)
    early_second(NE - 2, (NE - 2) % 2)

    d_w2.wait_recv()
    wait_w2s(0)
    wait_w2s(1)
    PC = EC - WC

    @pl.loop(0, NP)
    def _(i):
        r = pl.multiple_of(i * MT, MT)
        zs[0, pl.ds(r, MT), :] = (
            jnp.dot(he[pl.ds(R + r, MT), pl.ds(0, PC)], w2s[0, pl.ds(0, PC), :], preferred_element_type=F32)
            + jnp.dot(he[pl.ds(R + r, MT), pl.ds(EC, PC)], w2s[0, pl.ds(EC, PC), :], preferred_element_type=F32))

    j, s = NE - 1, (NE - 1) % 2
    wait_tiles(s, 0)
    with jax.named_scope('xw_last'):
        x_w1(j).wait_recv()
    f_w1d(0).start()

    @pl.loop(0, NP)
    def _(i):
        r = pl.multiple_of(i * MT, MT)
        layer1d(he, col(j, 0), R + r, MT, s, 0, 0)

        @pl.when(i == 0)
        def _():
            f_w1d(0).wait_recv()

        layer1d(he, col(j, 1), R + r, MT, s, 1, 0)
        zs[0, pl.ds(r, MT), :] = zs[0, pl.ds(r, MT), :] + (
            jnp.dot(he[pl.ds(R + r, MT), pl.ds(PC, WC)], w2s[0, pl.ds(PC, WC), :], preferred_element_type=F32)
            + jnp.dot(he[pl.ds(R + r, MT), pl.ds(EC + PC, WC)], w2s[0, pl.ds(EC + PC, WC), :], preferred_element_type=F32))
        z_y(0, i).start()

    def z_other(q):
        @pl.loop(0, NP)
        def _(i):
            r = pl.multiple_of(i * MT, MT)
            zs[q, pl.ds(r, MT), :] = jnp.dot(he[pl.ds(R + r, MT), :], w2s[q % 2], preferred_element_type=F32)
            z_y(q, i).start()

    def z_own(q):
        @pl.loop(0, NP)
        def _(i):
            r = pl.ds(pl.multiple_of(i * MT, MT), MT)
            zo[r, pl.ds(q * QC, QC)] = jnp.dot(he[r, :], w2s[q % 2], preferred_element_type=F32)

    layer1d(he, col(j, 0), 0, R, s, 0, 0)
    layer1d(he, col(j, 1), 0, R, s, 1, 0)
    for q in range(NQ):
        if q:
            if q >= 2:
                wait_w2s(q)
            with jax.named_scope('zs'):
                z_other(q)
        with jax.named_scope('zo'):
            z_own(q)
        if q + 2 < NQ:
            for c in loads(q + 2):
                c.start()
        if q == 0:
            with jax.named_scope('yw2'):
                remote(eo, eo, ys, yr.at[3], Y).wait_recv()
            d_eo.start()

    d_co.wait_recv()
    d_eo.wait_recv()

    def second(s):
        wait_tiles(s, 2)
        layer1(hl, WC, 0, R, s, 1)
        layer2(s)

    def layer2(s):
        wait_w2l(s)

        @pl.loop(0, NP)
        def _(i):
            r = pl.ds(pl.multiple_of(i * MT, MT), MT)
            zo[r, :] = zo[r, :] + jnp.dot(hl[r, :], w2l[s], preferred_element_type=F32)

    def late(near, n):
        off = NE if near else NE + NL

        @pl.loop(0, n)
        def _(k):
            s = lax.rem(off + k, 2)
            quad = quads_near(s, NE + k) if near else quads_far(s, k)
            for c in quad[:2] + (late_near(s, k) if near else late_far(s, k)):
                c.start()
            with jax.named_scope('xl'):
                (x_w1(NE + k) if near else x_co(k)).wait_recv()
            f = f_w1(off + k)
            f.start()
            quad[2].start()
            if near:
                @pl.when(k > 0)
                def _():
                    second(1 - s)
            else:
                second(1 - s)
            wait_tiles(s, 0)
            wait_tiles(s, 1)
            with jax.named_scope('c0'):
                layer1(hl, 0, 0, R, s, 0)
            with jax.named_scope('fw'):
                f.wait_recv()
            quad[3].start()

    late(True, NL)
    late(False, NL - 1)
    k, s = NL - 1, (NE + 2 * NL - 1) % 2
    quad = quads_far(s, k)
    for c in quad[:2] + late_far(s, k):
        c.start()
    second(1 - s)
    wait_tiles(s, 0)
    with jax.named_scope('xl_last'):
        x_co(k).wait_recv()
    f_w1d(1).start()
    with jax.named_scope('c0'):
        layer1d(hl, 0, 0, R, s, 0, 1)
    with jax.named_scope('fw'):
        f_w1d(1).wait_recv()
    with jax.named_scope('c1'):
        layer1d(hl, WC, 0, R, s, 1, 1)
    with jax.named_scope('l2'):
        layer2(s)

    def store(q, i):
        half, c = divmod(q, NQ // 2)
        rows = pl.ds(i * MT, MT)
        lanes = pl.multiple_of((1 - cx if half else cx) * C2 + c * QC, QC)
        return pltpu.make_async_copy(ob.at[rows, pl.ds(q * QC, QC)], out.at[rows, pl.ds(lanes, QC)], osem)

    def finish(q, i):
        r, l = pl.ds(i * MT, MT), pl.ds(q * QC, QC)
        ob[r, l] = (zo[r, l] + ry[q, r, :]).astype(BF16)
        store(q, i).start()

    few = pl.ds(0, NQ - 1)
    remote(zs.at[few], ry.at[few], zys, zyr.at[0], Y).wait_recv()
    for q in range(NQ - 1):
        for i in range(NP):
            finish(q, i)
    for i in range(NP):
        with jax.named_scope('zw'):
            z_y(NQ - 1, i).wait_recv()
        finish(NQ - 1, i)
    remote(zs, ry, zys, zyr.at[0], Y).wait_send()
    remote(bo, bp, ws, wr.at[0], X).wait_send()
    remote(bo, bp, fs, fr.at[0], D).wait_send()
    remote(w1, ap, ys, yr.at[0], Y).wait_send()
    for c in (x_x, d_w1, d_w2, d_co, d_eo):
        c.wait_send()
    with jax.named_scope('store'):
        pltpu.make_async_copy(ob, out, osem).wait()


def solution(mesh):
    data_spec = P(('dp', 'cx', 'cz'), 'cy')
    up_spec = P('cy', ('cz', 'cx'))
    down_spec = P('cz', ('cy', 'cx'))

    def local_mlp(x, w1, w2):
        R, K = x.shape
        B1 = w1.shape[1]
        WC = B1 // (NE + NL)
        EC, LC = NE * WC, NL * WC
        C2 = w2.shape[1]
        QC = 2 * C2 // NQ
        NX = NE + 2 * NL
        dma = pltpu.SemaphoreType.DMA
        any_spec = pl.BlockSpec(memory_space=pl.ANY)
        sds = jax.ShapeDtypeStruct
        outs = (
            sds((R, K), BF16),
            sds(w1.shape, BF16),
            sds((NX, K, WC), BF16),
            sds((NX, K, WC), BF16),
            sds((K, LC), BF16),
            sds((K, LC), BF16),
            sds(w2.shape, BF16),
            sds((2, LC, C2), BF16),
            sds((2, LC, C2), BF16),
        )
        scratch = [
            pltpu.VMEM((2 * R, 2 * K), BF16),
            pltpu.VMEM((2 * R, 2 * EC), BF16),
            pltpu.VMEM((R, 2 * WC), BF16),
            pltpu.VMEM((2, 2 * K, 2 * WC), BF16),
            pltpu.VMEM((2, K, 2 * WC), BF16),
            pltpu.VMEM((2, 2 * EC, QC), BF16),
            pltpu.VMEM((2, 2 * WC, 2 * C2), BF16),
            pltpu.VMEM((NQ, R, QC), F32),
            pltpu.VMEM((NQ, R, QC), F32),
            pltpu.VMEM((R, 2 * C2), F32),
            pltpu.VMEM((R, 2 * C2), BF16),
            dma((1,)), dma((2, 3)), dma((2,)), dma((2,)), dma,
            dma((1,)), dma((1,)),
            dma, dma((NX,)),
            dma, dma((4,)),
            dma, dma((1 + R // MT,)),
            dma((4,)), dma((4,)),
            dma, dma((NX,)),
        ]
        return pl.pallas_call(
            kernel,
            out_shape=outs,
            in_specs=[any_spec] * 3,
            out_specs=(any_spec,) * len(outs),
            scratch_shapes=scratch,
            compiler_params=pltpu.CompilerParams(
                collective_id=0, has_side_effects=True, vmem_limit_bytes=67043328),
            name='mlp',
        )(x, w1, w2)[0]

    return jax.shard_map(local_mlp, mesh=mesh, in_specs=(data_spec, up_spec, down_spec), out_specs=data_spec, check_vma=False)
```

```python
import jax
import jax.numpy as jnp
from jax import lax
from jax.experimental import pallas as pl
from jax.experimental.pallas import tpu as pltpu
from jax.sharding import PartitionSpec as P

MESH = pl.DeviceIdType.MESH
F32, BF16 = jnp.float32, jnp.bfloat16
NE = 12
NL = 4
NA = 3
NQ = 4
MT = 512


def gelu(c):
    return c * (0.5 * (1.0 + jnp.tanh(0.7978845608028654 * (c + 0.044715 * (c * c * c)))))


def kernel(x, w1, w2, out, ap, bo, bp, co, cp, g0, eo, ep,
           xg, he, hl, w1s, w1d, w2s, w2l, zs, ry, zo, ob,
           lsem, lw, lv, lu, osem, xs, xr, ws, wr, ys, yr, zys, zyr,
           ds, dr, fs, fr):
    cz, cy, cx = lax.axis_index('cz'), lax.axis_index('cy'), lax.axis_index('cx')
    X, Y, D = {'cy': 1 - cy}, {'cz': 1 - cz}, {'cx': 1 - cx}
    R, K = x.shape
    B1 = w1.shape[1]
    WC = B1 // (NE + NL)
    EC, LC = NE * WC, NL * WC
    C2 = w2.shape[1]
    QC = 2 * C2 // NQ

    def remote(src, dst, s, r, dev):
        return pltpu.make_async_remote_copy(src, dst, s, r, device_id=dev, device_id_type=MESH)

    barrier = pltpu.get_barrier_semaphore()
    for dev in (X, Y, D):
        pl.semaphore_signal(barrier, inc=1, device_id=dev, device_id_type=MESH)
    pl.semaphore_wait(barrier, 3)

    own, oth = pl.ds(0, R), pl.ds(R, R)
    klo, khi = pl.ds(0, K), pl.ds(K, K)

    x_x = remote(x, xg.at[own, khi], xs.at[0], xr.at[0], X)
    y_x = remote(x, xg.at[oth, klo], ys, yr.at[0], Y)
    y_xf = remote(xg.at[own, khi], xg.at[oth, khi], ys, yr.at[1], Y)
    y_w1 = remote(w1.at[:, pl.ds(EC, LC)], co, ys, yr.at[2], Y)

    def y_w2(b):
        return remote(w2.at[pl.ds(b * B1 + EC, LC), :], eo.at[b], ys, yr.at[3], Y)

    l_x = pltpu.make_async_copy(x, xg.at[own, klo], lsem.at[0])
    d_w1 = remote(w1, ap, ds.at[0], dr.at[0], D)
    d_w2 = remote(w2, g0, ds.at[1], dr.at[1], D)
    d_co = remote(co, cp, ds.at[2], dr.at[2], D)
    d_eo = remote(eo, ep, ds.at[3], dr.at[3], D)

    def chunk(j):
        return pl.ds(j * WC if isinstance(j, int) else pl.multiple_of(j * WC, WC), WC)

    lo_c, hi_c = pl.ds(0, WC), pl.ds(WC, WC)

    def x_w1(j):
        dst = w1d.at[0, :, lo_c] if isinstance(j, int) and j == NE - 1 else bo.at[j]
        return remote(w1.at[:, chunk(j)], dst, ws, wr.at[j], X)

    def x_co(k):
        dst = w1d.at[1, :, lo_c] if isinstance(k, int) and k == NL - 1 else bo.at[NE + NL + k]
        return remote(co.at[:, chunk(k)], dst, ws, wr.at[NE + NL + k], X)

    def f_w1(j):
        return remote(bo.at[j], bp.at[j], fs, fr.at[j], D)

    def f_w1d(i):
        j = (NE - 1, NE + 2 * NL - 1)[i]
        return remote(w1d.at[i, :, lo_c], w1d.at[i, :, hi_c], fs, fr.at[j], D)

    def quads(s, j, first, second):
        return [pltpu.make_async_copy(src, w1s.at[s, rows, pl.ds(c * WC, WC)], lw.at[s, i])
                for src, rows, c, i in (
                    (first, klo, 0, 0), (second, klo, 1, 0), (bo.at[j], khi, 0, 1), (bp.at[j], khi, 1, 2))]

    def wait_tiles(s, i):
        if i == 0:
            pltpu.make_async_copy(w1.at[:, pl.ds(0, 2 * WC)], w1s.at[s, klo, :], lw.at[s, 0]).wait()
        else:
            pltpu.make_async_copy(bo.at[0], w1s.at[s, khi, pl.ds((i - 1) * WC, WC)], lw.at[s, i]).wait()

    def wait_w2s(q):
        pltpu.make_async_copy(w2.at[pl.ds(0, 2 * EC), pl.ds(0, QC)], w2s.at[q % 2], lv.at[q % 2]).wait()

    def wait_w2l(s):
        pltpu.make_async_copy(w1.at[pl.ds(0, 2 * WC), pl.ds(0, 2 * C2)], w2l.at[s], lu.at[s]).wait()

    def quads_near(s, j):
        return quads(s, j, w1.at[:, chunk(j)], ap.at[:, chunk(j)])

    def quads_far(s, k):
        return quads(s, NE + NL + k, co.at[:, chunk(k)], cp.at[:, chunk(k)])

    base = (pl.multiple_of(cx * B1, B1), pl.multiple_of((1 - cx) * B1, B1))

    def loads(q):
        src, c = (w2, q) if q < NQ // 2 else (g0, q - NQ // 2)
        return [pltpu.make_async_copy(src.at[pl.ds(base[b], EC), pl.ds(c * QC, QC)],
                                      w2s.at[q % 2, pl.ds(b * EC, EC), :], lv.at[q % 2]) for b in range(2)]

    def late_near(s, k):
        got = []
        for b in range(2):
            rows = pl.ds(pl.multiple_of(base[b] + EC + k * WC, WC), WC)
            for c, src in enumerate((w2, g0)):
                got.append(pltpu.make_async_copy(
                    src.at[rows, :], w2l.at[s, pl.ds(b * WC, WC), pl.ds(c * C2, C2)], lu.at[s]))
        return got

    def late_far(s, k):
        got = []
        for b, blk in enumerate((cx, 1 - cx)):
            for c, src in enumerate((eo, ep)):
                got.append(pltpu.make_async_copy(
                    src.at[blk, chunk(k), :], w2l.at[s, pl.ds(b * WC, WC), pl.ds(c * C2, C2)], lu.at[s]))
        return got

    NP = R // MT

    def z_y(q, i):
        rows = pl.ds(i * MT if isinstance(i, int) else pl.multiple_of(i * MT, MT), MT)
        return remote(zs.at[q, rows, :], ry.at[q, rows, :], zys.at[0 if q < 2 else 1], zyr.at[0 if q < NQ - 1 else 1 + i], Y)

    def layer1(dst, col, row0, rows, s, half):
        @pl.loop(0, rows // MT)
        def _(i):
            r = pl.multiple_of(i * MT, MT)
            c = jnp.dot(xg[pl.ds(row0 + r, MT), :], w1s[s, :, pl.ds(half * WC, WC)], preferred_element_type=F32)
            dst[pl.ds(row0 + r, MT), pl.ds(col, WC)] = gelu(c.astype(BF16).astype(F32)).astype(BF16)

    def layer1d(dst, col, row0, rows, s, half, i):
        lanes = pl.ds(half * WC, WC)

        @pl.loop(0, rows // MT)
        def _(n):
            r = pl.ds(pl.multiple_of(row0 + n * MT, MT), MT)
            c = (jnp.dot(xg[r, klo], w1s[s, klo, lanes], preferred_element_type=F32)
                 + jnp.dot(xg[r, khi], w1d[i, :, lanes], preferred_element_type=F32))
            dst[r, pl.ds(col, WC)] = gelu(c.astype(BF16).astype(F32)).astype(BF16)

    def step(j):
        s = lax.rem(j, 2)
        q = quads_near(s, j)
        q[0].start()
        q[1].start()
        x_w1(j).wait_recv()
        f_w1(j).start()
        q[2].start()
        wait_tiles(s, 0)
        wait_tiles(s, 1)
        layer1(he, col(j, 0), 0, R, s, 0)
        f_w1(j).wait_recv()
        q[3].start()
        wait_tiles(s, 2)
        layer1(he, col(j, 1), 0, R, s, 1)

    def col(j, half):
        return half * EC + j * WC if isinstance(j, int) else pl.multiple_of(half * EC + j * WC, WC)

    x_x.start()
    y_x.start()
    l_x.start()
    for j in range(NE):
        x_w1(j).start()
    d_w1.start()
    d_w2.start()
    for q in range(2):
        for c in loads(q):
            c.start()

    with jax.named_scope('xx'):
        x_x.wait_recv()
    y_xf.start()
    y_w1.start()
    y_w2(0).start()
    y_w2(1).start()
    l_x.wait()
    d_w1.wait_recv()

    @pl.loop(0, NA)
    def _(j):
        step(j)

    with jax.named_scope('yx'):
        y_x.wait_recv()
        y_xf.wait_recv()

    for n, j in enumerate((2, 1, 0)):
        if n == 2:
            for i in range(3):
                wait_tiles(0, i)
        for half in range(2):
            layer1(he, col(j, half), R, R, j % 2, half)
        if n == 0:
            for c in quads_near(0, 0):
                c.start()
        if n == 1:
            for c in quads_near(NA % 2, NA)[:2]:
                c.start()

    def early_second(j, s):
        wait_tiles(s, 2)
        layer1(he, col(j, 1), 0, 2 * R, s, 1)

    def early(lo, hi):
        @pl.loop(lo, hi)
        def _(j):
            s = lax.rem(j, 2)
            with jax.named_scope('xw'):
                x_w1(j).wait_recv()
            f_w1(j).start()
            q = quads_near(s, j)
            q[2].start()
            if lo == NA:
                @pl.when(j > lo)
                def _():
                    early_second(j - 1, 1 - s)
            else:
                early_second(j - 1, 1 - s)
            for c in quads_near(1 - s, j + 1)[:2]:
                c.start()
            wait_tiles(s, 0)
            wait_tiles(s, 1)
            layer1(he, col(j, 0), 0, 2 * R, s, 0)
            f_w1(j).wait_recv()
            q[3].start()

    early(NA, 8)
    y_w1.wait_recv()
    for k in range(NL):
        x_w1(NE + k).start()
    for k in range(NL):
        x_co(k).start()
    d_co.start()
    early(8, 9)

    def z_part(lo, hi, first):
        lanes = [pl.ds(b * EC + lo * WC, (hi - lo) * WC) for b in range(2)]

        @pl.loop(0, NP)
        def _(i):
            r = pl.multiple_of(i * MT, MT)
            z = sum(jnp.dot(he[pl.ds(R + r, MT), l], w2s[0, l, :], preferred_element_type=F32) for l in lanes)
            zs[0, pl.ds(r, MT), :] = z if first else zs[0, pl.ds(r, MT), :] + z

    d_w2.wait_recv()
    wait_w2s(0)
    wait_w2s(1)
    z_part(0, 8, True)
    early(9, NE - 2)
    early_second(NE - 3, (NE - 3) % 2)
    j, s = NE - 2, (NE - 2) % 2
    with jax.named_scope('xw'):
        x_w1(j).wait_recv()
    f_w1(j).start()
    q = quads_near(s, j)
    q[2].start()
    for c in quads_near(1 - s, j + 1)[:2]:
        c.start()
    wait_tiles(s, 0)
    wait_tiles(s, 1)
    layer1(he, col(j, 0), 0, 2 * R, s, 0)
    f_w1(j).wait_recv()
    q[3].start()
    early_second(j, s)
    z_part(8, NE - 1, False)
    PC = EC - WC

    j, s = NE - 1, (NE - 1) % 2
    wait_tiles(s, 0)
    with jax.named_scope('xw_last'):
        x_w1(j).wait_recv()
    f_w1d(0).start()

    @pl.loop(0, NP)
    def _(i):
        r = pl.multiple_of(i * MT, MT)
        layer1d(he, col(j, 0), R + r, MT, s, 0, 0)

        @pl.when(i == 0)
        def _():
            f_w1d(0).wait_recv()

        layer1d(he, col(j, 1), R + r, MT, s, 1, 0)
        zs[0, pl.ds(r, MT), :] = zs[0, pl.ds(r, MT), :] + (
            jnp.dot(he[pl.ds(R + r, MT), pl.ds(PC, WC)], w2s[0, pl.ds(PC, WC), :], preferred_element_type=F32)
            + jnp.dot(he[pl.ds(R + r, MT), pl.ds(EC + PC, WC)], w2s[0, pl.ds(EC + PC, WC), :], preferred_element_type=F32))
        z_y(0, i).start()

    def z_other(q):
        @pl.loop(0, NP)
        def _(i):
            r = pl.multiple_of(i * MT, MT)
            zs[q, pl.ds(r, MT), :] = jnp.dot(he[pl.ds(R + r, MT), :], w2s[q % 2], preferred_element_type=F32)
            z_y(q, i).start()

    def z_own(q):
        @pl.loop(0, NP)
        def _(i):
            r = pl.ds(pl.multiple_of(i * MT, MT), MT)
            zo[r, pl.ds(q * QC, QC)] = jnp.dot(he[r, :], w2s[q % 2], preferred_element_type=F32)

    layer1d(he, col(j, 0), 0, R, s, 0, 0)
    layer1d(he, col(j, 1), 0, R, s, 1, 0)
    for q in range(NQ):
        if q:
            if q >= 2:
                wait_w2s(q)
            with jax.named_scope('zs'):
                z_other(q)
        with jax.named_scope('zo'):
            z_own(q)
        if q + 2 < NQ:
            for c in loads(q + 2):
                c.start()
        if q == 0:
            with jax.named_scope('yw2'):
                remote(eo, eo, ys, yr.at[3], Y).wait_recv()
            d_eo.start()

    d_co.wait_recv()
    d_eo.wait_recv()

    def second(s):
        wait_tiles(s, 2)
        layer1(hl, WC, 0, R, s, 1)
        layer2(s)

    def layer2(s):
        wait_w2l(s)

        @pl.loop(0, NP)
        def _(i):
            r = pl.ds(pl.multiple_of(i * MT, MT), MT)
            zo[r, :] = zo[r, :] + jnp.dot(hl[r, :], w2l[s], preferred_element_type=F32)

    def late_step(near, k, s, before):
        off = NE if near else NE + NL
        quad = quads_near(s, NE + k) if near else quads_far(s, k)
        for c in quad[:2] + (late_near(s, k) if near else late_far(s, k)):
            c.start()
        with jax.named_scope('xl'):
            (x_w1(NE + k) if near else x_co(k)).wait_recv()
        f = f_w1(off + k)
        f.start()
        quad[2].start()
        before()
        wait_tiles(s, 0)
        wait_tiles(s, 1)
        with jax.named_scope('c0'):
            layer1(hl, 0, 0, R, s, 0)
        with jax.named_scope('fw'):
            f.wait_recv()
        quad[3].start()

    @pl.loop(0, NL)
    def _(k):
        s = lax.rem(NE + k, 2)

        def before():
            @pl.when(k > 0)
            def _():
                second(1 - s)

        late_step(True, k, s, before)

    @pl.loop(0, NL - 2)
    def _(k):
        s = lax.rem(NE + NL + k, 2)
        late_step(False, k, s, lambda: second(1 - s))

    k, s = NL - 2, (NE + 2 * NL - 2) % 2
    second(1 - s)
    late_step(False, k, s, lambda: None)
    second(s)
    k, s = NL - 1, 1 - s
    for c in quads_far(s, k)[:2] + late_far(s, k):
        c.start()
    wait_tiles(s, 0)

    def sent(n):
        two = pl.ds(2 * n, 2)
        return remote(zs.at[two], ry.at[two], zys.at[n], zyr.at[0], Y)

    sent(0).wait_send()
    for half in range(2):
        @pl.loop(0, NP)
        def _(i):
            r = pl.ds(pl.multiple_of(i * MT, MT), MT)
            zs[half, r, :] = jnp.dot(xg[r, klo], w1s[s, klo, pl.ds(half * WC, WC)], preferred_element_type=F32)

    def last(half):
        @pl.loop(0, NP)
        def _(i):
            r = pl.ds(pl.multiple_of(i * MT, MT), MT)
            c = zs[half, r, :] + jnp.dot(xg[r, khi], w1d[1, :, pl.ds(half * WC, WC)], preferred_element_type=F32)
            hl[r, pl.ds(half * WC, WC)] = gelu(c.astype(BF16).astype(F32)).astype(BF16)

    with jax.named_scope('xl_last'):
        x_co(k).wait_recv()
    f_w1d(1).start()
    with jax.named_scope('c0'):
        last(0)
    with jax.named_scope('fw'):
        f_w1d(1).wait_recv()
    with jax.named_scope('c1'):
        last(1)
    with jax.named_scope('l2'):
        layer2(s)

    def store(q, i):
        half, c = divmod(q, NQ // 2)
        rows = pl.ds(i * MT, MT)
        lanes = pl.multiple_of((1 - cx if half else cx) * C2 + c * QC, QC)
        return pltpu.make_async_copy(ob.at[rows, pl.ds(q * QC, QC)], out.at[rows, pl.ds(lanes, QC)], osem)

    def finish(q, i):
        r, l = pl.ds(i * MT, MT), pl.ds(q * QC, QC)
        ob[r, l] = (zo[r, l] + ry[q, r, :]).astype(BF16)
        store(q, i).start()

    few = pl.ds(0, NQ - 1)
    remote(zs.at[few], ry.at[few], zys.at[0], zyr.at[0], Y).wait_recv()
    for q in range(NQ - 1):
        for i in range(NP):
            finish(q, i)
    for i in range(NP):
        with jax.named_scope('zw'):
            z_y(NQ - 1, i).wait_recv()
        finish(NQ - 1, i)
    sent(1).wait_send()
    remote(bo, bp, ws, wr.at[0], X).wait_send()
    remote(bo, bp, fs, fr.at[0], D).wait_send()
    remote(w1, ap, ys, yr.at[0], Y).wait_send()
    for c in (x_x, d_w1, d_w2, d_co, d_eo):
        c.wait_send()
    with jax.named_scope('store'):
        pltpu.make_async_copy(ob, out, osem).wait()


def solution(mesh):
    data_spec = P(('dp', 'cx', 'cz'), 'cy')
    up_spec = P('cy', ('cz', 'cx'))
    down_spec = P('cz', ('cy', 'cx'))

    def local_mlp(x, w1, w2):
        R, K = x.shape
        B1 = w1.shape[1]
        WC = B1 // (NE + NL)
        EC, LC = NE * WC, NL * WC
        C2 = w2.shape[1]
        QC = 2 * C2 // NQ
        NX = NE + 2 * NL
        dma = pltpu.SemaphoreType.DMA
        any_spec = pl.BlockSpec(memory_space=pl.ANY)
        sds = jax.ShapeDtypeStruct
        outs = (
            sds((R, K), BF16),
            sds(w1.shape, BF16),
            sds((NX, K, WC), BF16),
            sds((NX, K, WC), BF16),
            sds((K, LC), BF16),
            sds((K, LC), BF16),
            sds(w2.shape, BF16),
            sds((2, LC, C2), BF16),
            sds((2, LC, C2), BF16),
        )
        scratch = [
            pltpu.VMEM((2 * R, 2 * K), BF16),
            pltpu.VMEM((2 * R, 2 * EC), BF16),
            pltpu.VMEM((R, 2 * WC), BF16),
            pltpu.VMEM((2, 2 * K, 2 * WC), BF16),
            pltpu.VMEM((2, K, 2 * WC), BF16),
            pltpu.VMEM((2, 2 * EC, QC), BF16),
            pltpu.VMEM((2, 2 * WC, 2 * C2), BF16),
            pltpu.VMEM((NQ, R, QC), F32),
            pltpu.VMEM((NQ, R, QC), F32),
            pltpu.VMEM((R, 2 * C2), F32),
            pltpu.VMEM((R, 2 * C2), BF16),
            dma((1,)), dma((2, 3)), dma((2,)), dma((2,)), dma,
            dma((1,)), dma((1,)),
            dma, dma((NX,)),
            dma, dma((4,)),
            dma((2,)), dma((1 + R // MT,)),
            dma((4,)), dma((4,)),
            dma, dma((NX,)),
        ]
        return pl.pallas_call(
            kernel,
            out_shape=outs,
            in_specs=[any_spec] * 3,
            out_specs=(any_spec,) * len(outs),
            scratch_shapes=scratch,
            compiler_params=pltpu.CompilerParams(
                collective_id=0, has_side_effects=True, vmem_limit_bytes=67043328),
            name='mlp',
        )(x, w1, w2)[0]

    return jax.shard_map(local_mlp, mesh=mesh, in_specs=(data_spec, up_spec, down_spec), out_specs=data_spec, check_vma=False)
```

```python
import jax
import jax.numpy as jnp
from jax import lax
from jax.experimental import pallas as pl
from jax.experimental.pallas import tpu as pltpu
from jax.sharding import PartitionSpec as P

MESH = pl.DeviceIdType.MESH
F32, BF16 = jnp.float32, jnp.bfloat16
NE = 12
NL = 4
NA = 3
NQ = 4
MT = 512


def gelu(c):
    return c * (0.5 * (1.0 + jnp.tanh(0.7978845608028654 * (c + 0.044715 * (c * c * c)))))


def kernel(x, w1, w2, out, ap, bo, bp, co, cp, g0, eo, ep,
           xg, he, hl, w1s, w1d, w2s, w2l, zs, ry, zo,
           lsem, lw, lv, lu, xs, xr, ws, wr, ys, yr, zys, zyr,
           ds, dr, fs, fr):
    cz, cy, cx = lax.axis_index('cz'), lax.axis_index('cy'), lax.axis_index('cx')
    X, Y, D = {'cy': 1 - cy}, {'cz': 1 - cz}, {'cx': 1 - cx}
    R, K = x.shape
    B1 = w1.shape[1]
    WC = B1 // (NE + NL)
    EC, LC = NE * WC, NL * WC
    C2 = w2.shape[1]
    QC = 2 * C2 // NQ

    def remote(src, dst, s, r, dev):
        return pltpu.make_async_remote_copy(src, dst, s, r, device_id=dev, device_id_type=MESH)

    barrier = pltpu.get_barrier_semaphore()
    for dev in (X, Y, D):
        pl.semaphore_signal(barrier, inc=1, device_id=dev, device_id_type=MESH)
    pl.semaphore_wait(barrier, 3)

    own, oth = pl.ds(0, R), pl.ds(R, R)
    klo, khi = pl.ds(0, K), pl.ds(K, K)

    x_x = remote(x, xg.at[own, khi], xs.at[0], xr.at[0], X)
    y_x = remote(x, xg.at[oth, klo], ys, yr.at[0], Y)
    y_xf = remote(xg.at[own, khi], xg.at[oth, khi], ys, yr.at[1], Y)
    y_w1 = remote(w1.at[:, pl.ds(EC, LC)], co, ys, yr.at[2], Y)

    def y_w2(b):
        return remote(w2.at[pl.ds(b * B1 + EC, LC), :], eo.at[b], ys, yr.at[3], Y)

    l_x = pltpu.make_async_copy(x, xg.at[own, klo], lsem.at[0])
    d_w1 = remote(w1, ap, ds.at[0], dr.at[0], D)
    d_w2 = remote(w2, g0, ds.at[1], dr.at[1], D)
    d_co = remote(co, cp, ds.at[2], dr.at[2], D)
    d_eo = remote(eo, ep, ds.at[3], dr.at[3], D)

    def chunk(j):
        return pl.ds(j * WC if isinstance(j, int) else pl.multiple_of(j * WC, WC), WC)

    lo_c, hi_c = pl.ds(0, WC), pl.ds(WC, WC)

    def x_w1(j):
        dst = w1d.at[0, :, lo_c] if isinstance(j, int) and j == NE - 1 else bo.at[j]
        return remote(w1.at[:, chunk(j)], dst, ws, wr.at[j], X)

    def x_co(k):
        dst = w1d.at[1, :, lo_c] if isinstance(k, int) and k == NL - 1 else bo.at[NE + NL + k]
        return remote(co.at[:, chunk(k)], dst, ws, wr.at[NE + NL + k], X)

    def f_w1(j):
        return remote(bo.at[j], bp.at[j], fs, fr.at[j], D)

    def f_w1d(i):
        j = (NE - 1, NE + 2 * NL - 1)[i]
        return remote(w1d.at[i, :, lo_c], w1d.at[i, :, hi_c], fs, fr.at[j], D)

    def quads(s, j, first, second):
        return [pltpu.make_async_copy(src, w1s.at[s, rows, pl.ds(c * WC, WC)], lw.at[s, i])
                for src, rows, c, i in (
                    (first, klo, 0, 0), (second, klo, 1, 0), (bo.at[j], khi, 0, 1), (bp.at[j], khi, 1, 2))]

    def wait_tiles(s, i):
        if i == 0:
            pltpu.make_async_copy(w1.at[:, pl.ds(0, 2 * WC)], w1s.at[s, klo, :], lw.at[s, 0]).wait()
        else:
            pltpu.make_async_copy(bo.at[0], w1s.at[s, khi, pl.ds((i - 1) * WC, WC)], lw.at[s, i]).wait()

    def wait_w2s(q):
        pltpu.make_async_copy(w2.at[pl.ds(0, 2 * EC), pl.ds(0, QC)], w2s.at[q % 2], lv.at[q % 2]).wait()

    def wait_w2l(s):
        pltpu.make_async_copy(w1.at[pl.ds(0, 2 * WC), pl.ds(0, 2 * C2)], w2l.at[s], lu.at[s]).wait()

    def quads_near(s, j):
        return quads(s, j, w1.at[:, chunk(j)], ap.at[:, chunk(j)])

    def quads_far(s, k):
        return quads(s, NE + NL + k, co.at[:, chunk(k)], cp.at[:, chunk(k)])

    base = (pl.multiple_of(cx * B1, B1), pl.multiple_of((1 - cx) * B1, B1))

    def loads(q):
        src, c = (w2, q) if q < NQ // 2 else (g0, q - NQ // 2)
        return [pltpu.make_async_copy(src.at[pl.ds(base[b], EC), pl.ds(c * QC, QC)],
                                      w2s.at[q % 2, pl.ds(b * EC, EC), :], lv.at[q % 2]) for b in range(2)]

    def late_near(s, k):
        got = []
        for b in range(2):
            rows = pl.ds(pl.multiple_of(base[b] + EC + k * WC, WC), WC)
            for c, src in enumerate((w2, g0)):
                got.append(pltpu.make_async_copy(
                    src.at[rows, :], w2l.at[s, pl.ds(b * WC, WC), pl.ds(c * C2, C2)], lu.at[s]))
        return got

    def late_far(s, k):
        got = []
        for b, blk in enumerate((cx, 1 - cx)):
            for c, src in enumerate((eo, ep)):
                got.append(pltpu.make_async_copy(
                    src.at[blk, chunk(k), :], w2l.at[s, pl.ds(b * WC, WC), pl.ds(c * C2, C2)], lu.at[s]))
        return got

    NP = R // MT

    def z_y(q, i):
        rows = pl.ds(i * MT if isinstance(i, int) else pl.multiple_of(i * MT, MT), MT)
        return remote(zs.at[q, rows, :], ry.at[q, rows, :], zys.at[0 if q < 2 else 1], zyr.at[0 if q < NQ - 1 else 1 + i], Y)

    def layer1(dst, col, row0, rows, s, half):
        @pl.loop(0, rows // MT)
        def _(i):
            r = pl.multiple_of(i * MT, MT)
            c = jnp.dot(xg[pl.ds(row0 + r, MT), :], w1s[s, :, pl.ds(half * WC, WC)], preferred_element_type=F32)
            dst[pl.ds(row0 + r, MT), pl.ds(col, WC)] = gelu(c.astype(BF16).astype(F32)).astype(BF16)

    def layer1d(dst, col, row0, rows, s, half, i):
        lanes = pl.ds(half * WC, WC)

        @pl.loop(0, rows // MT)
        def _(n):
            r = pl.ds(pl.multiple_of(row0 + n * MT, MT), MT)
            c = (jnp.dot(xg[r, klo], w1s[s, klo, lanes], preferred_element_type=F32)
                 + jnp.dot(xg[r, khi], w1d[i, :, lanes], preferred_element_type=F32))
            dst[r, pl.ds(col, WC)] = gelu(c.astype(BF16).astype(F32)).astype(BF16)

    def step(j):
        s = lax.rem(j, 2)
        q = quads_near(s, j)
        q[0].start()
        q[1].start()
        x_w1(j).wait_recv()
        f_w1(j).start()
        q[2].start()
        wait_tiles(s, 0)
        wait_tiles(s, 1)
        layer1(he, col(j, 0), 0, R, s, 0)
        f_w1(j).wait_recv()
        q[3].start()
        wait_tiles(s, 2)
        layer1(he, col(j, 1), 0, R, s, 1)

    def col(j, half):
        return half * EC + j * WC if isinstance(j, int) else pl.multiple_of(half * EC + j * WC, WC)

    x_x.start()
    y_x.start()
    l_x.start()
    for j in range(NE):
        x_w1(j).start()
    d_w1.start()
    d_w2.start()
    for q in range(2):
        for c in loads(q):
            c.start()

    with jax.named_scope('xx'):
        x_x.wait_recv()
    y_xf.start()
    y_w1.start()
    y_w2(0).start()
    y_w2(1).start()
    l_x.wait()
    d_w1.wait_recv()

    @pl.loop(0, NA)
    def _(j):
        step(j)

    with jax.named_scope('yx'):
        y_x.wait_recv()
        y_xf.wait_recv()

    for n, j in enumerate((2, 1, 0)):
        if n == 2:
            for i in range(3):
                wait_tiles(0, i)
        for half in range(2):
            layer1(he, col(j, half), R, R, j % 2, half)
        if n == 0:
            for c in quads_near(0, 0):
                c.start()
        if n == 1:
            for c in quads_near(NA % 2, NA)[:2]:
                c.start()

    def early_second(j, s):
        wait_tiles(s, 2)
        layer1(he, col(j, 1), 0, 2 * R, s, 1)

    def early(lo, hi):
        @pl.loop(lo, hi)
        def _(j):
            s = lax.rem(j, 2)
            with jax.named_scope('xw'):
                x_w1(j).wait_recv()
            f_w1(j).start()
            q = quads_near(s, j)
            q[2].start()
            if lo == NA:
                @pl.when(j > lo)
                def _():
                    early_second(j - 1, 1 - s)
            else:
                early_second(j - 1, 1 - s)
            for c in quads_near(1 - s, j + 1)[:2]:
                c.start()
            wait_tiles(s, 0)
            wait_tiles(s, 1)
            layer1(he, col(j, 0), 0, 2 * R, s, 0)
            f_w1(j).wait_recv()
            q[3].start()

    early(NA, 8)
    y_w1.wait_recv()
    for k in range(NL):
        x_w1(NE + k).start()
    for k in range(NL):
        x_co(k).start()
    d_co.start()
    early(8, 9)

    def z_part(lo, hi, first):
        lanes = [pl.ds(b * EC + lo * WC, (hi - lo) * WC) for b in range(2)]

        @pl.loop(0, NP)
        def _(i):
            r = pl.multiple_of(i * MT, MT)
            z = sum(jnp.dot(he[pl.ds(R + r, MT), l], w2s[0, l, :], preferred_element_type=F32) for l in lanes)
            zs[0, pl.ds(r, MT), :] = z if first else zs[0, pl.ds(r, MT), :] + z

    d_w2.wait_recv()
    wait_w2s(0)
    wait_w2s(1)
    z_part(0, 8, True)
    early(9, NE - 2)
    early_second(NE - 3, (NE - 3) % 2)
    j, s = NE - 2, (NE - 2) % 2
    with jax.named_scope('xw'):
        x_w1(j).wait_recv()
    f_w1(j).start()
    q = quads_near(s, j)
    q[2].start()
    for c in quads_near(1 - s, j + 1)[:2]:
        c.start()
    wait_tiles(s, 0)
    wait_tiles(s, 1)
    layer1(he, col(j, 0), 0, 2 * R, s, 0)
    f_w1(j).wait_recv()
    q[3].start()
    early_second(j, s)
    z_part(8, NE - 1, False)
    PC = EC - WC

    j, s = NE - 1, (NE - 1) % 2
    wait_tiles(s, 0)
    with jax.named_scope('xw_last'):
        x_w1(j).wait_recv()
    f_w1d(0).start()

    @pl.loop(0, NP)
    def _(i):
        r = pl.multiple_of(i * MT, MT)
        layer1d(he, col(j, 0), R + r, MT, s, 0, 0)

        @pl.when(i == 0)
        def _():
            f_w1d(0).wait_recv()

        layer1d(he, col(j, 1), R + r, MT, s, 1, 0)
        zs[0, pl.ds(r, MT), :] = zs[0, pl.ds(r, MT), :] + (
            jnp.dot(he[pl.ds(R + r, MT), pl.ds(PC, WC)], w2s[0, pl.ds(PC, WC), :], preferred_element_type=F32)
            + jnp.dot(he[pl.ds(R + r, MT), pl.ds(EC + PC, WC)], w2s[0, pl.ds(EC + PC, WC), :], preferred_element_type=F32))
        z_y(0, i).start()

    def z_other(q):
        @pl.loop(0, NP)
        def _(i):
            r = pl.multiple_of(i * MT, MT)
            zs[q, pl.ds(r, MT), :] = jnp.dot(he[pl.ds(R + r, MT), :], w2s[q % 2], preferred_element_type=F32)
            z_y(q, i).start()

    def z_own(q):
        @pl.loop(0, NP)
        def _(i):
            r = pl.ds(pl.multiple_of(i * MT, MT), MT)
            zo[r, pl.ds(q * QC, QC)] = jnp.dot(he[r, :], w2s[q % 2], preferred_element_type=F32)

    layer1d(he, col(j, 0), 0, R, s, 0, 0)
    layer1d(he, col(j, 1), 0, R, s, 1, 0)
    for q in range(NQ):
        if q:
            if q >= 2:
                wait_w2s(q)
            with jax.named_scope('zs'):
                z_other(q)
        with jax.named_scope('zo'):
            z_own(q)
        if q + 2 < NQ:
            for c in loads(q + 2):
                c.start()
        if q == 0:
            with jax.named_scope('yw2'):
                remote(eo, eo, ys, yr.at[3], Y).wait_recv()
            d_eo.start()

    d_co.wait_recv()
    d_eo.wait_recv()

    def second(s):
        wait_tiles(s, 2)
        layer1(hl, WC, 0, R, s, 1)
        layer2(s)

    def layer2(s):
        wait_w2l(s)

        @pl.loop(0, NP)
        def _(i):
            r = pl.ds(pl.multiple_of(i * MT, MT), MT)
            zo[r, :] = zo[r, :] + jnp.dot(hl[r, :], w2l[s], preferred_element_type=F32)

    def late_step(near, k, s, before):
        off = NE if near else NE + NL
        quad = quads_near(s, NE + k) if near else quads_far(s, k)
        for c in quad[:2] + (late_near(s, k) if near else late_far(s, k)):
            c.start()
        with jax.named_scope('xl'):
            (x_w1(NE + k) if near else x_co(k)).wait_recv()
        f = f_w1(off + k)
        f.start()
        quad[2].start()
        before()
        wait_tiles(s, 0)
        wait_tiles(s, 1)
        with jax.named_scope('c0'):
            layer1(hl, 0, 0, R, s, 0)
        with jax.named_scope('fw'):
            f.wait_recv()
        quad[3].start()

    @pl.loop(0, NL)
    def _(k):
        s = lax.rem(NE + k, 2)

        def before():
            @pl.when(k > 0)
            def _():
                second(1 - s)

        late_step(True, k, s, before)

    @pl.loop(0, NL - 2)
    def _(k):
        s = lax.rem(NE + NL + k, 2)
        late_step(False, k, s, lambda: second(1 - s))

    k, s = NL - 2, (NE + 2 * NL - 2) % 2
    second(1 - s)
    late_step(False, k, s, lambda: None)
    second(s)
    k, s = NL - 1, 1 - s
    for c in quads_far(s, k)[:2] + late_far(s, k):
        c.start()
    wait_tiles(s, 0)

    def sent(n):
        two = pl.ds(2 * n, 2)
        return remote(zs.at[two], ry.at[two], zys.at[n], zyr.at[0], Y)

    sent(0).wait_send()
    for half in range(2):
        @pl.loop(0, NP)
        def _(i):
            r = pl.ds(pl.multiple_of(i * MT, MT), MT)
            zs[half, r, :] = jnp.dot(xg[r, klo], w1s[s, klo, pl.ds(half * WC, WC)], preferred_element_type=F32)

    def last(half):
        @pl.loop(0, NP)
        def _(i):
            r = pl.ds(pl.multiple_of(i * MT, MT), MT)
            c = zs[half, r, :] + jnp.dot(xg[r, khi], w1d[1, :, pl.ds(half * WC, WC)], preferred_element_type=F32)
            hl[r, pl.ds(half * WC, WC)] = gelu(c.astype(BF16).astype(F32)).astype(BF16)

    with jax.named_scope('xl_last'):
        x_co(k).wait_recv()
    f_w1d(1).start()
    with jax.named_scope('c0'):
        last(0)
    with jax.named_scope('fw'):
        f_w1d(1).wait_recv()
    with jax.named_scope('c1'):
        last(1)
    with jax.named_scope('l2'):
        layer2(s)

    def finish(q, i):
        r, l = pl.ds(i * MT, MT), pl.ds(q * QC, QC)
        half, c = divmod(q, NQ // 2)
        lanes = pl.multiple_of((1 - cx if half else cx) * C2 + c * QC, QC)
        out[r, pl.ds(lanes, QC)] = (zo[r, l] + ry[q, r, :]).astype(BF16)

    few = pl.ds(0, NQ - 1)
    remote(zs.at[few], ry.at[few], zys.at[0], zyr.at[0], Y).wait_recv()
    for q in range(NQ - 1):
        for i in range(NP):
            finish(q, i)
    for i in range(NP):
        with jax.named_scope('zw'):
            z_y(NQ - 1, i).wait_recv()
        finish(NQ - 1, i)
    sent(1).wait_send()
    remote(bo, bp, ws, wr.at[0], X).wait_send()
    remote(bo, bp, fs, fr.at[0], D).wait_send()
    remote(w1, ap, ys, yr.at[0], Y).wait_send()
    for c in (x_x, d_w1, d_w2, d_co, d_eo):
        c.wait_send()


def solution(mesh):
    data_spec = P(('dp', 'cx', 'cz'), 'cy')
    up_spec = P('cy', ('cz', 'cx'))
    down_spec = P('cz', ('cy', 'cx'))

    def local_mlp(x, w1, w2):
        R, K = x.shape
        B1 = w1.shape[1]
        WC = B1 // (NE + NL)
        EC, LC = NE * WC, NL * WC
        C2 = w2.shape[1]
        QC = 2 * C2 // NQ
        NX = NE + 2 * NL
        dma = pltpu.SemaphoreType.DMA
        any_spec = pl.BlockSpec(memory_space=pl.ANY)
        sds = jax.ShapeDtypeStruct
        outs = (
            pltpu.VMEM((R, K), BF16),
            sds(w1.shape, BF16),
            sds((NX, K, WC), BF16),
            sds((NX, K, WC), BF16),
            sds((K, LC), BF16),
            sds((K, LC), BF16),
            sds(w2.shape, BF16),
            sds((2, LC, C2), BF16),
            sds((2, LC, C2), BF16),
        )
        scratch = [
            pltpu.VMEM((2 * R, 2 * K), BF16),
            pltpu.VMEM((2 * R, 2 * EC), BF16),
            pltpu.VMEM((R, 2 * WC), BF16),
            pltpu.VMEM((2, 2 * K, 2 * WC), BF16),
            pltpu.VMEM((2, K, 2 * WC), BF16),
            pltpu.VMEM((2, 2 * EC, QC), BF16),
            pltpu.VMEM((2, 2 * WC, 2 * C2), BF16),
            pltpu.VMEM((NQ, R, QC), F32),
            pltpu.VMEM((NQ, R, QC), F32),
            pltpu.VMEM((R, 2 * C2), F32),
            dma((1,)), dma((2, 3)), dma((2,)), dma((2,)),
            dma((1,)), dma((1,)),
            dma, dma((NX,)),
            dma, dma((4,)),
            dma((2,)), dma((1 + R // MT,)),
            dma((4,)), dma((4,)),
            dma, dma((NX,)),
        ]
        return pl.pallas_call(
            kernel,
            out_shape=outs,
            in_specs=[any_spec] * 3,
            out_specs=(pl.BlockSpec(memory_space=pltpu.VMEM),) + (any_spec,) * (len(outs) - 1),
            scratch_shapes=scratch,
            compiler_params=pltpu.CompilerParams(
                collective_id=0, has_side_effects=True, vmem_limit_bytes=67043328 - 2 * R * K),
            name='mlp',
        )(x, w1, w2)[0]

    return jax.shard_map(local_mlp, mesh=mesh, in_specs=(data_spec, up_spec, down_spec), out_specs=data_spec, check_vma=False)
```

```python
import jax
import jax.numpy as jnp
from jax import lax
from jax.experimental import pallas as pl
from jax.experimental.pallas import tpu as pltpu
from jax.sharding import PartitionSpec as P

MESH = pl.DeviceIdType.MESH
F32, BF16 = jnp.float32, jnp.bfloat16
NE = 12
NL = 4
NA = 3
NQ = 4
MT = 512
PT = 256


def gelu(c):
    return c * (0.5 * (1.0 + jnp.tanh(0.7978845608028654 * (c + 0.044715 * (c * c * c)))))


def kernel(x, w1, w2, out, ap, bo, bp, co, cp, g0, eo, ep,
           xg, he, hl, w1s, w1d, w2s, w2l, zs, ry, zo,
           lsem, lw, lv, lu, xs, xr, ws, wr, ys, yr, zys, zyr,
           ds, dr, fs, fr):
    cz, cy, cx = lax.axis_index('cz'), lax.axis_index('cy'), lax.axis_index('cx')
    X, Y, D = {'cy': 1 - cy}, {'cz': 1 - cz}, {'cx': 1 - cx}
    R, K = x.shape
    B1 = w1.shape[1]
    WC = B1 // (NE + NL)
    EC, LC = NE * WC, NL * WC
    C2 = w2.shape[1]
    QC = 2 * C2 // NQ

    def remote(src, dst, s, r, dev):
        return pltpu.make_async_remote_copy(src, dst, s, r, device_id=dev, device_id_type=MESH)

    barrier = pltpu.get_barrier_semaphore()
    for dev in (X, Y, D):
        pl.semaphore_signal(barrier, inc=1, device_id=dev, device_id_type=MESH)
    pl.semaphore_wait(barrier, 3)

    own, oth = pl.ds(0, R), pl.ds(R, R)
    klo, khi = pl.ds(0, K), pl.ds(K, K)

    x_x = remote(x, xg.at[own, khi], xs.at[0], xr.at[0], X)
    y_x = remote(x, xg.at[oth, klo], ys, yr.at[0], Y)
    y_xf = remote(xg.at[own, khi], xg.at[oth, khi], ys, yr.at[1], Y)
    y_w1 = remote(w1.at[:, pl.ds(EC, LC)], co, ys, yr.at[2], Y)

    def y_w2(b):
        return remote(w2.at[pl.ds(b * B1 + EC, LC), :], eo.at[b], ys, yr.at[3], Y)

    l_x = pltpu.make_async_copy(x, xg.at[own, klo], lsem.at[0])
    d_w1 = remote(w1, ap, ds.at[0], dr.at[0], D)
    d_w2 = remote(w2, g0, ds.at[1], dr.at[1], D)
    d_co = remote(co, cp, ds.at[2], dr.at[2], D)
    d_eo = remote(eo, ep, ds.at[3], dr.at[3], D)

    def chunk(j):
        return pl.ds(j * WC if isinstance(j, int) else pl.multiple_of(j * WC, WC), WC)

    lo_c, hi_c = pl.ds(0, WC), pl.ds(WC, WC)

    def x_w1(j):
        dst = w1d.at[0, :, lo_c] if isinstance(j, int) and j == NE - 1 else bo.at[j]
        return remote(w1.at[:, chunk(j)], dst, ws, wr.at[j], X)

    def x_co(k):
        dst = w1d.at[1, :, lo_c] if isinstance(k, int) and k == NL - 1 else bo.at[NE + NL + k]
        return remote(co.at[:, chunk(k)], dst, ws, wr.at[NE + NL + k], X)

    def f_w1(j):
        return remote(bo.at[j], bp.at[j], fs, fr.at[j], D)

    def f_w1d(i):
        j = (NE - 1, NE + 2 * NL - 1)[i]
        return remote(w1d.at[i, :, lo_c], w1d.at[i, :, hi_c], fs, fr.at[j], D)

    def quads(s, j, first, second):
        return [pltpu.make_async_copy(src, w1s.at[s, rows, pl.ds(c * WC, WC)], lw.at[s, i])
                for src, rows, c, i in (
                    (first, klo, 0, 0), (second, klo, 1, 0), (bo.at[j], khi, 0, 1), (bp.at[j], khi, 1, 2))]

    def wait_tiles(s, i):
        if i == 0:
            pltpu.make_async_copy(w1.at[:, pl.ds(0, 2 * WC)], w1s.at[s, klo, :], lw.at[s, 0]).wait()
        else:
            pltpu.make_async_copy(bo.at[0], w1s.at[s, khi, pl.ds((i - 1) * WC, WC)], lw.at[s, i]).wait()

    def wait_w2s(q):
        pltpu.make_async_copy(w2.at[pl.ds(0, 2 * EC), pl.ds(0, QC)], w2s.at[q % 2], lv.at[q % 2]).wait()

    def wait_w2l(s):
        pltpu.make_async_copy(w1.at[pl.ds(0, 2 * WC), pl.ds(0, 2 * C2)], w2l.at[s], lu.at[s]).wait()

    def quads_near(s, j):
        return quads(s, j, w1.at[:, chunk(j)], ap.at[:, chunk(j)])

    def quads_far(s, k):
        return quads(s, NE + NL + k, co.at[:, chunk(k)], cp.at[:, chunk(k)])

    base = (pl.multiple_of(cx * B1, B1), pl.multiple_of((1 - cx) * B1, B1))

    def loads(q):
        src, c = (w2, q) if q < NQ // 2 else (g0, q - NQ // 2)
        return [pltpu.make_async_copy(src.at[pl.ds(base[b], EC), pl.ds(c * QC, QC)],
                                      w2s.at[q % 2, pl.ds(b * EC, EC), :], lv.at[q % 2]) for b in range(2)]

    def late_near(s, k):
        got = []
        for b in range(2):
            rows = pl.ds(pl.multiple_of(base[b] + EC + k * WC, WC), WC)
            for c, src in enumerate((w2, g0)):
                got.append(pltpu.make_async_copy(
                    src.at[rows, :], w2l.at[s, pl.ds(b * WC, WC), pl.ds(c * C2, C2)], lu.at[s]))
        return got

    def late_far(s, k):
        got = []
        for b, blk in enumerate((cx, 1 - cx)):
            for c, src in enumerate((eo, ep)):
                got.append(pltpu.make_async_copy(
                    src.at[blk, chunk(k), :], w2l.at[s, pl.ds(b * WC, WC), pl.ds(c * C2, C2)], lu.at[s]))
        return got

    NP = R // MT

    def z_y(q, i, n=MT):
        rows = pl.ds(i * n if isinstance(i, int) else pl.multiple_of(i * n, n), n)
        return remote(zs.at[q, rows, :], ry.at[q, rows, :], zys.at[0 if q < 2 else 1], zyr.at[0 if q < NQ - 1 else 1 + i], Y)

    def layer1(dst, col, row0, rows, s, half):
        @pl.loop(0, rows // MT)
        def _(i):
            r = pl.multiple_of(i * MT, MT)
            c = jnp.dot(xg[pl.ds(row0 + r, MT), :], w1s[s, :, pl.ds(half * WC, WC)], preferred_element_type=F32)
            dst[pl.ds(row0 + r, MT), pl.ds(col, WC)] = gelu(c.astype(BF16).astype(F32)).astype(BF16)

    def layer1d(dst, col, row0, rows, s, half, i):
        lanes = pl.ds(half * WC, WC)

        @pl.loop(0, rows // MT)
        def _(n):
            r = pl.ds(pl.multiple_of(row0 + n * MT, MT), MT)
            c = (jnp.dot(xg[r, klo], w1s[s, klo, lanes], preferred_element_type=F32)
                 + jnp.dot(xg[r, khi], w1d[i, :, lanes], preferred_element_type=F32))
            dst[r, pl.ds(col, WC)] = gelu(c.astype(BF16).astype(F32)).astype(BF16)

    def step(j):
        s = lax.rem(j, 2)
        q = quads_near(s, j)
        q[0].start()
        q[1].start()
        x_w1(j).wait_recv()
        f_w1(j).start()
        q[2].start()
        wait_tiles(s, 0)
        wait_tiles(s, 1)
        layer1(he, col(j, 0), 0, R, s, 0)
        f_w1(j).wait_recv()
        q[3].start()
        wait_tiles(s, 2)
        layer1(he, col(j, 1), 0, R, s, 1)

    def col(j, half):
        return half * EC + j * WC if isinstance(j, int) else pl.multiple_of(half * EC + j * WC, WC)

    x_x.start()
    y_x.start()
    l_x.start()
    for j in range(NE):
        x_w1(j).start()
    d_w1.start()
    d_w2.start()
    for q in range(2):
        for c in loads(q):
            c.start()

    with jax.named_scope('xx'):
        x_x.wait_recv()
    y_xf.start()
    y_w1.start()
    y_w2(0).start()
    y_w2(1).start()
    l_x.wait()
    d_w1.wait_recv()

    @pl.loop(0, NA)
    def _(j):
        step(j)

    with jax.named_scope('yx'):
        y_x.wait_recv()
        y_xf.wait_recv()

    for n, j in enumerate((2, 1, 0)):
        if n == 2:
            for i in range(3):
                wait_tiles(0, i)
        for half in range(2):
            layer1(he, col(j, half), R, R, j % 2, half)
        if n == 0:
            for c in quads_near(0, 0):
                c.start()
        if n == 1:
            for c in quads_near(NA % 2, NA)[:2]:
                c.start()

    def early_second(j, s):
        wait_tiles(s, 2)
        layer1(he, col(j, 1), 0, 2 * R, s, 1)

    def early(lo, hi):
        @pl.loop(lo, hi)
        def _(j):
            s = lax.rem(j, 2)
            with jax.named_scope('xw'):
                x_w1(j).wait_recv()
            f_w1(j).start()
            q = quads_near(s, j)
            q[2].start()
            if lo == NA:
                @pl.when(j > lo)
                def _():
                    early_second(j - 1, 1 - s)
            else:
                early_second(j - 1, 1 - s)
            for c in quads_near(1 - s, j + 1)[:2]:
                c.start()
            wait_tiles(s, 0)
            wait_tiles(s, 1)
            layer1(he, col(j, 0), 0, 2 * R, s, 0)
            f_w1(j).wait_recv()
            q[3].start()

    early(NA, 8)
    y_w1.wait_recv()
    for k in range(NL):
        x_w1(NE + k).start()
    for k in range(NL):
        x_co(k).start()
    d_co.start()
    early(8, 9)

    def z_part(lo, hi, first):
        lanes = [pl.ds(b * EC + lo * WC, (hi - lo) * WC) for b in range(2)]

        @pl.loop(0, NP)
        def _(i):
            r = pl.multiple_of(i * MT, MT)
            z = sum(jnp.dot(he[pl.ds(R + r, MT), l], w2s[0, l, :], preferred_element_type=F32) for l in lanes)
            zs[0, pl.ds(r, MT), :] = z if first else zs[0, pl.ds(r, MT), :] + z

    d_w2.wait_recv()
    wait_w2s(0)
    wait_w2s(1)
    z_part(0, 8, True)
    early(9, NE - 2)
    early_second(NE - 3, (NE - 3) % 2)
    j, s = NE - 2, (NE - 2) % 2
    with jax.named_scope('xw'):
        x_w1(j).wait_recv()
    f_w1(j).start()
    q = quads_near(s, j)
    q[2].start()
    for c in quads_near(1 - s, j + 1)[:2]:
        c.start()
    wait_tiles(s, 0)
    wait_tiles(s, 1)
    layer1(he, col(j, 0), 0, 2 * R, s, 0)
    f_w1(j).wait_recv()
    q[3].start()
    early_second(j, s)
    z_part(8, NE - 1, False)
    PC = EC - WC

    j, s = NE - 1, (NE - 1) % 2
    wait_tiles(s, 0)

    @pl.loop(0, NP)
    def _(i):
        r = pl.multiple_of(i * MT, MT)
        zo[pl.ds(r, MT), pl.ds(0, 2 * WC)] = jnp.dot(
            xg[pl.ds(R + r, MT), klo], w1s[s, klo, :], preferred_element_type=F32)

    with jax.named_scope('xw_last'):
        x_w1(j).wait_recv()
    f_w1d(0).start()

    @pl.loop(0, R // PT)
    def _(i):
        r = pl.multiple_of(i * PT, PT)

        def half_chunk(half):
            lanes = pl.ds(half * WC, WC)
            c = zo[pl.ds(r, PT), lanes] + jnp.dot(
                xg[pl.ds(R + r, PT), khi], w1d[0, :, lanes], preferred_element_type=F32)
            he[pl.ds(R + r, PT), pl.ds(col(j, half), WC)] = gelu(c.astype(BF16).astype(F32)).astype(BF16)

        half_chunk(0)

        @pl.when(i == 0)
        def _():
            f_w1d(0).wait_recv()

        half_chunk(1)
        zs[0, pl.ds(r, PT), :] = zs[0, pl.ds(r, PT), :] + (
            jnp.dot(he[pl.ds(R + r, PT), pl.ds(PC, WC)], w2s[0, pl.ds(PC, WC), :], preferred_element_type=F32)
            + jnp.dot(he[pl.ds(R + r, PT), pl.ds(EC + PC, WC)], w2s[0, pl.ds(EC + PC, WC), :], preferred_element_type=F32))
        z_y(0, i, PT).start()

    def z_other(q):
        @pl.loop(0, NP)
        def _(i):
            r = pl.multiple_of(i * MT, MT)
            zs[q, pl.ds(r, MT), :] = jnp.dot(he[pl.ds(R + r, MT), :], w2s[q % 2], preferred_element_type=F32)
            z_y(q, i).start()

    def z_own(q):
        @pl.loop(0, NP)
        def _(i):
            r = pl.ds(pl.multiple_of(i * MT, MT), MT)
            zo[r, pl.ds(q * QC, QC)] = jnp.dot(he[r, :], w2s[q % 2], preferred_element_type=F32)

    layer1d(he, col(j, 0), 0, R, s, 0, 0)
    layer1d(he, col(j, 1), 0, R, s, 1, 0)
    for q in range(NQ):
        if q:
            if q >= 2:
                wait_w2s(q)
            with jax.named_scope('zs'):
                z_other(q)
        with jax.named_scope('zo'):
            z_own(q)
        if q + 2 < NQ:
            for c in loads(q + 2):
                c.start()
        if q == 0:
            with jax.named_scope('yw2'):
                remote(eo, eo, ys, yr.at[3], Y).wait_recv()
            d_eo.start()

    d_co.wait_recv()
    d_eo.wait_recv()

    def second(s):
        wait_tiles(s, 2)
        layer1(hl, WC, 0, R, s, 1)
        layer2(s)

    def layer2(s):
        wait_w2l(s)

        @pl.loop(0, NP)
        def _(i):
            r = pl.ds(pl.multiple_of(i * MT, MT), MT)
            zo[r, :] = zo[r, :] + jnp.dot(hl[r, :], w2l[s], preferred_element_type=F32)

    def late_step(near, k, s, before):
        off = NE if near else NE + NL
        quad = quads_near(s, NE + k) if near else quads_far(s, k)
        for c in quad[:2] + (late_near(s, k) if near else late_far(s, k)):
            c.start()
        with jax.named_scope('xl'):
            (x_w1(NE + k) if near else x_co(k)).wait_recv()
        f = f_w1(off + k)
        f.start()
        quad[2].start()
        before()
        wait_tiles(s, 0)
        wait_tiles(s, 1)
        with jax.named_scope('c0'):
            layer1(hl, 0, 0, R, s, 0)
        with jax.named_scope('fw'):
            f.wait_recv()
        quad[3].start()

    @pl.loop(0, NL)
    def _(k):
        s = lax.rem(NE + k, 2)

        def before():
            @pl.when(k > 0)
            def _():
                second(1 - s)

        late_step(True, k, s, before)

    @pl.loop(0, NL - 2)
    def _(k):
        s = lax.rem(NE + NL + k, 2)
        late_step(False, k, s, lambda: second(1 - s))

    k, s = NL - 2, (NE + 2 * NL - 2) % 2
    second(1 - s)
    late_step(False, k, s, lambda: None)
    second(s)
    k, s = NL - 1, 1 - s
    for c in quads_far(s, k)[:2] + late_far(s, k):
        c.start()
    wait_tiles(s, 0)

    def sent(n):
        two = pl.ds(2 * n, 2)
        return remote(zs.at[two], ry.at[two], zys.at[n], zyr.at[0], Y)

    sent(0).wait_send()
    for half in range(2):
        @pl.loop(0, NP)
        def _(i):
            r = pl.ds(pl.multiple_of(i * MT, MT), MT)
            zs[half, r, :] = jnp.dot(xg[r, klo], w1s[s, klo, pl.ds(half * WC, WC)], preferred_element_type=F32)

    def last(half):
        @pl.loop(0, NP)
        def _(i):
            r = pl.ds(pl.multiple_of(i * MT, MT), MT)
            c = zs[half, r, :] + jnp.dot(xg[r, khi], w1d[1, :, pl.ds(half * WC, WC)], preferred_element_type=F32)
            hl[r, pl.ds(half * WC, WC)] = gelu(c.astype(BF16).astype(F32)).astype(BF16)

    with jax.named_scope('xl_last'):
        x_co(k).wait_recv()
    f_w1d(1).start()
    with jax.named_scope('c0'):
        last(0)
    with jax.named_scope('fw'):
        f_w1d(1).wait_recv()
    with jax.named_scope('c1'):
        last(1)
    with jax.named_scope('l2'):
        layer2(s)

    def finish(q, i):
        r, l = pl.ds(i * MT, MT), pl.ds(q * QC, QC)
        half, c = divmod(q, NQ // 2)
        lanes = pl.multiple_of((1 - cx if half else cx) * C2 + c * QC, QC)
        out[r, pl.ds(lanes, QC)] = (zo[r, l] + ry[q, r, :]).astype(BF16)

    few = pl.ds(0, NQ - 1)
    remote(zs.at[few], ry.at[few], zys.at[0], zyr.at[0], Y).wait_recv()
    for q in range(NQ - 1):
        for i in range(NP):
            finish(q, i)
    for i in range(NP):
        with jax.named_scope('zw'):
            z_y(NQ - 1, i).wait_recv()
        finish(NQ - 1, i)
    sent(1).wait_send()
    remote(bo, bp, ws, wr.at[0], X).wait_send()
    remote(bo, bp, fs, fr.at[0], D).wait_send()
    remote(w1, ap, ys, yr.at[0], Y).wait_send()
    for c in (x_x, d_w1, d_w2, d_co, d_eo):
        c.wait_send()


def solution(mesh):
    data_spec = P(('dp', 'cx', 'cz'), 'cy')
    up_spec = P('cy', ('cz', 'cx'))
    down_spec = P('cz', ('cy', 'cx'))

    def local_mlp(x, w1, w2):
        R, K = x.shape
        B1 = w1.shape[1]
        WC = B1 // (NE + NL)
        EC, LC = NE * WC, NL * WC
        C2 = w2.shape[1]
        QC = 2 * C2 // NQ
        NX = NE + 2 * NL
        dma = pltpu.SemaphoreType.DMA
        any_spec = pl.BlockSpec(memory_space=pl.ANY)
        sds = jax.ShapeDtypeStruct
        outs = (
            pltpu.VMEM((R, K), BF16),
            sds(w1.shape, BF16),
            sds((NX, K, WC), BF16),
            sds((NX, K, WC), BF16),
            sds((K, LC), BF16),
            sds((K, LC), BF16),
            sds(w2.shape, BF16),
            sds((2, LC, C2), BF16),
            sds((2, LC, C2), BF16),
        )
        scratch = [
            pltpu.VMEM((2 * R, 2 * K), BF16),
            pltpu.VMEM((2 * R, 2 * EC), BF16),
            pltpu.VMEM((R, 2 * WC), BF16),
            pltpu.VMEM((2, 2 * K, 2 * WC), BF16),
            pltpu.VMEM((2, K, 2 * WC), BF16),
            pltpu.VMEM((2, 2 * EC, QC), BF16),
            pltpu.VMEM((2, 2 * WC, 2 * C2), BF16),
            pltpu.VMEM((NQ, R, QC), F32),
            pltpu.VMEM((NQ, R, QC), F32),
            pltpu.VMEM((R, 2 * C2), F32),
            dma((1,)), dma((2, 3)), dma((2,)), dma((2,)),
            dma((1,)), dma((1,)),
            dma, dma((NX,)),
            dma, dma((4,)),
            dma((2,)), dma((1 + R // MT,)),
            dma((4,)), dma((4,)),
            dma, dma((NX,)),
        ]
        return pl.pallas_call(
            kernel,
            out_shape=outs,
            in_specs=[any_spec] * 3,
            out_specs=(pl.BlockSpec(memory_space=pltpu.VMEM),) + (any_spec,) * (len(outs) - 1),
            scratch_shapes=scratch,
            compiler_params=pltpu.CompilerParams(
                collective_id=0, has_side_effects=True, vmem_limit_bytes=67043328 - 2 * R * K),
            name='mlp',
        )(x, w1, w2)[0]

    return jax.shard_map(local_mlp, mesh=mesh, in_specs=(data_spec, up_spec, down_spec), out_specs=data_spec, check_vma=False)
```

```python
import jax
import jax.numpy as jnp
from jax import lax
from jax.experimental import pallas as pl
from jax.experimental.pallas import tpu as pltpu
from jax.sharding import PartitionSpec as P

MESH = pl.DeviceIdType.MESH
F32, BF16 = jnp.float32, jnp.bfloat16
NE = 12
NL = 4
NA = 3
NQ = 4
MT = 512
PT = 256


def gelu(c):
    return c * (0.5 * (1.0 + jnp.tanh(0.7978845608028654 * (c + 0.044715 * (c * c * c)))))


def kernel(x, w1, w2, out, ap, bo, bp, co, cp, g0, eo, ep,
           xg, he, hl, w1s, w1d, w2s, w2l, zs, ry, zo,
           lsem, lw, lv, lu, xs, xr, ws, wr, ys, yr, zys, zyr,
           ds, dr, fs, fr):
    cz, cy, cx = lax.axis_index('cz'), lax.axis_index('cy'), lax.axis_index('cx')
    X, Y, D = {'cy': 1 - cy}, {'cz': 1 - cz}, {'cx': 1 - cx}
    R, K = x.shape
    B1 = w1.shape[1]
    WC = B1 // (NE + NL)
    EC, LC = NE * WC, NL * WC
    C2 = w2.shape[1]
    QC = 2 * C2 // NQ

    def remote(src, dst, s, r, dev):
        return pltpu.make_async_remote_copy(src, dst, s, r, device_id=dev, device_id_type=MESH)

    barrier = pltpu.get_barrier_semaphore()
    for dev in (X, Y, D):
        pl.semaphore_signal(barrier, inc=1, device_id=dev, device_id_type=MESH)
    pl.semaphore_wait(barrier, 3)

    own, oth = pl.ds(0, R), pl.ds(R, R)
    klo, khi = pl.ds(0, K), pl.ds(K, K)

    x_x = remote(x, xg.at[own, khi], xs.at[0], xr.at[0], X)
    y_x = remote(x, xg.at[oth, klo], ys, yr.at[0], Y)
    y_xf = remote(xg.at[own, khi], xg.at[oth, khi], ys, yr.at[1], Y)
    y_w1 = remote(w1.at[:, pl.ds(EC, LC)], co, ys, yr.at[2], Y)

    def y_w2(b):
        return remote(w2.at[pl.ds(b * B1 + EC, LC), :], eo.at[b], ys, yr.at[3], Y)

    l_x = pltpu.make_async_copy(x, xg.at[own, klo], lsem.at[0])
    d_w1 = remote(w1, ap, ds.at[0], dr.at[0], D)
    d_w2 = remote(w2, g0, ds.at[1], dr.at[1], D)
    d_co = remote(co, cp, ds.at[2], dr.at[2], D)
    d_eo = remote(eo, ep, ds.at[3], dr.at[3], D)

    def chunk(j):
        return pl.ds(j * WC if isinstance(j, int) else pl.multiple_of(j * WC, WC), WC)

    lo_c, hi_c = pl.ds(0, WC), pl.ds(WC, WC)

    def x_w1(j):
        dst = w1d.at[0, :, lo_c] if isinstance(j, int) and j == NE - 1 else bo.at[j]
        return remote(w1.at[:, chunk(j)], dst, ws, wr.at[j], X)

    def x_co(k):
        return remote(co.at[:, chunk(k)], bo.at[NE + NL + k], ws, wr.at[NE + NL + k], X)

    def f_w1(j):
        return remote(bo.at[j], bp.at[j], fs, fr.at[j], D)

    f_last = remote(w1d.at[0, :, lo_c], w1d.at[0, :, hi_c], fs, fr.at[NE - 1], D)
    HC = WC // 2

    def part(h, other=0):
        return pl.ds((2 * h + other) * HC, HC)

    def cols_last(h):
        return pl.ds((NL - 1) * WC + h * HC, HC)

    def x_part(h):
        return remote(co.at[:, cols_last(h)], w1d.at[1, :, part(h)], ws, wr.at[NE + 2 * NL - 1 + h], X)

    def f_part(h):
        return remote(w1d.at[1, :, part(h)], w1d.at[1, :, part(h, 1)], fs, fr.at[NE + 2 * NL - 1 + h], D)

    def quads(s, j, first, second):
        return [pltpu.make_async_copy(src, w1s.at[s, rows, pl.ds(c * WC, WC)], lw.at[s, i])
                for src, rows, c, i in (
                    (first, klo, 0, 0), (second, klo, 1, 0), (bo.at[j], khi, 0, 1), (bp.at[j], khi, 1, 2))]

    def wait_tiles(s, i):
        if i == 0:
            pltpu.make_async_copy(w1.at[:, pl.ds(0, 2 * WC)], w1s.at[s, klo, :], lw.at[s, 0]).wait()
        else:
            pltpu.make_async_copy(bo.at[0], w1s.at[s, khi, pl.ds((i - 1) * WC, WC)], lw.at[s, i]).wait()

    def wait_w2s(q):
        pltpu.make_async_copy(w2.at[pl.ds(0, 2 * EC), pl.ds(0, QC)], w2s.at[q % 2], lv.at[q % 2]).wait()

    def wait_w2l(s):
        pltpu.make_async_copy(w1.at[pl.ds(0, 2 * WC), pl.ds(0, 2 * C2)], w2l.at[s], lu.at[s]).wait()

    def quads_near(s, j):
        return quads(s, j, w1.at[:, chunk(j)], ap.at[:, chunk(j)])

    def quads_far(s, k):
        return quads(s, NE + NL + k, co.at[:, chunk(k)], cp.at[:, chunk(k)])

    base = (pl.multiple_of(cx * B1, B1), pl.multiple_of((1 - cx) * B1, B1))

    def loads(q):
        src, c = (w2, q) if q < NQ // 2 else (g0, q - NQ // 2)
        return [pltpu.make_async_copy(src.at[pl.ds(base[b], EC), pl.ds(c * QC, QC)],
                                      w2s.at[q % 2, pl.ds(b * EC, EC), :], lv.at[q % 2]) for b in range(2)]

    def late_near(s, k):
        got = []
        for b in range(2):
            rows = pl.ds(pl.multiple_of(base[b] + EC + k * WC, WC), WC)
            for c, src in enumerate((w2, g0)):
                got.append(pltpu.make_async_copy(
                    src.at[rows, :], w2l.at[s, pl.ds(b * WC, WC), pl.ds(c * C2, C2)], lu.at[s]))
        return got

    def late_far(s, k):
        got = []
        for b, blk in enumerate((cx, 1 - cx)):
            for c, src in enumerate((eo, ep)):
                got.append(pltpu.make_async_copy(
                    src.at[blk, chunk(k), :], w2l.at[s, pl.ds(b * WC, WC), pl.ds(c * C2, C2)], lu.at[s]))
        return got

    NP = R // MT

    def z_y(q, i, n=MT):
        rows = pl.ds(i * n if isinstance(i, int) else pl.multiple_of(i * n, n), n)
        return remote(zs.at[q, rows, :], ry.at[q, rows, :], zys.at[0 if q < 2 else 1], zyr.at[0 if q < NQ - 1 else 1 + i], Y)

    def layer1(dst, col, row0, rows, s, half):
        @pl.loop(0, rows // MT)
        def _(i):
            r = pl.multiple_of(i * MT, MT)
            c = jnp.dot(xg[pl.ds(row0 + r, MT), :], w1s[s, :, pl.ds(half * WC, WC)], preferred_element_type=F32)
            dst[pl.ds(row0 + r, MT), pl.ds(col, WC)] = gelu(c.astype(BF16).astype(F32)).astype(BF16)

    def layer1d(dst, col, row0, rows, s, half, i):
        lanes = pl.ds(half * WC, WC)

        @pl.loop(0, rows // MT)
        def _(n):
            r = pl.ds(pl.multiple_of(row0 + n * MT, MT), MT)
            c = (jnp.dot(xg[r, klo], w1s[s, klo, lanes], preferred_element_type=F32)
                 + jnp.dot(xg[r, khi], w1d[i, :, lanes], preferred_element_type=F32))
            dst[r, pl.ds(col, WC)] = gelu(c.astype(BF16).astype(F32)).astype(BF16)

    def step(j):
        s = lax.rem(j, 2)
        q = quads_near(s, j)
        q[0].start()
        q[1].start()
        x_w1(j).wait_recv()
        f_w1(j).start()
        q[2].start()
        wait_tiles(s, 0)
        wait_tiles(s, 1)
        layer1(he, col(j, 0), 0, R, s, 0)
        f_w1(j).wait_recv()
        q[3].start()
        wait_tiles(s, 2)
        layer1(he, col(j, 1), 0, R, s, 1)

    def col(j, half):
        return half * EC + j * WC if isinstance(j, int) else pl.multiple_of(half * EC + j * WC, WC)

    x_x.start()
    y_x.start()
    l_x.start()
    for j in range(NE):
        x_w1(j).start()
    d_w1.start()
    d_w2.start()
    for q in range(2):
        for c in loads(q):
            c.start()

    with jax.named_scope('xx'):
        x_x.wait_recv()
    y_xf.start()
    y_w1.start()
    y_w2(0).start()
    y_w2(1).start()
    l_x.wait()
    d_w1.wait_recv()

    @pl.loop(0, NA)
    def _(j):
        step(j)

    with jax.named_scope('yx'):
        y_x.wait_recv()
        y_xf.wait_recv()

    for n, j in enumerate((2, 1, 0)):
        if n == 2:
            for i in range(3):
                wait_tiles(0, i)
        for half in range(2):
            layer1(he, col(j, half), R, R, j % 2, half)
        if n == 0:
            for c in quads_near(0, 0):
                c.start()
        if n == 1:
            for c in quads_near(NA % 2, NA)[:2]:
                c.start()

    def early_second(j, s):
        wait_tiles(s, 2)
        layer1(he, col(j, 1), 0, 2 * R, s, 1)

    def early(lo, hi):
        @pl.loop(lo, hi)
        def _(j):
            s = lax.rem(j, 2)
            with jax.named_scope('xw'):
                x_w1(j).wait_recv()
            f_w1(j).start()
            q = quads_near(s, j)
            q[2].start()
            if lo == NA:
                @pl.when(j > lo)
                def _():
                    early_second(j - 1, 1 - s)
            else:
                early_second(j - 1, 1 - s)
            for c in quads_near(1 - s, j + 1)[:2]:
                c.start()
            wait_tiles(s, 0)
            wait_tiles(s, 1)
            layer1(he, col(j, 0), 0, 2 * R, s, 0)
            f_w1(j).wait_recv()
            q[3].start()

    early(NA, 8)
    y_w1.wait_recv()
    for k in range(NL):
        x_w1(NE + k).start()
    for k in range(NL - 1):
        x_co(k).start()
    x_part(0).start()
    x_part(1).start()
    d_co.start()
    early(8, 9)

    def z_part(lo, hi, first):
        lanes = [pl.ds(b * EC + lo * WC, (hi - lo) * WC) for b in range(2)]

        @pl.loop(0, NP)
        def _(i):
            r = pl.multiple_of(i * MT, MT)
            z = sum(jnp.dot(he[pl.ds(R + r, MT), l], w2s[0, l, :], preferred_element_type=F32) for l in lanes)
            zs[0, pl.ds(r, MT), :] = z if first else zs[0, pl.ds(r, MT), :] + z

    d_w2.wait_recv()
    wait_w2s(0)
    wait_w2s(1)
    z_part(0, 8, True)
    early(9, NE - 2)
    early_second(NE - 3, (NE - 3) % 2)
    j, s = NE - 2, (NE - 2) % 2
    with jax.named_scope('xw'):
        x_w1(j).wait_recv()
    f_w1(j).start()
    q = quads_near(s, j)
    q[2].start()
    for c in quads_near(1 - s, j + 1)[:2]:
        c.start()
    wait_tiles(s, 0)
    wait_tiles(s, 1)
    layer1(he, col(j, 0), 0, 2 * R, s, 0)
    f_w1(j).wait_recv()
    q[3].start()
    early_second(j, s)
    z_part(8, NE - 1, False)
    PC = EC - WC

    j, s = NE - 1, (NE - 1) % 2
    wait_tiles(s, 0)

    @pl.loop(0, NP)
    def _(i):
        r = pl.multiple_of(i * MT, MT)
        zo[pl.ds(r, MT), pl.ds(0, 2 * WC)] = jnp.dot(
            xg[pl.ds(R + r, MT), klo], w1s[s, klo, :], preferred_element_type=F32)

    with jax.named_scope('xw_last'):
        x_w1(j).wait_recv()
    f_last.start()

    @pl.loop(0, R // PT)
    def _(i):
        r = pl.multiple_of(i * PT, PT)

        def half_chunk(half):
            lanes = pl.ds(half * WC, WC)
            c = zo[pl.ds(r, PT), lanes] + jnp.dot(
                xg[pl.ds(R + r, PT), khi], w1d[0, :, lanes], preferred_element_type=F32)
            he[pl.ds(R + r, PT), pl.ds(col(j, half), WC)] = gelu(c.astype(BF16).astype(F32)).astype(BF16)

        half_chunk(0)

        @pl.when(i == 0)
        def _():
            f_last.wait_recv()

        half_chunk(1)
        zs[0, pl.ds(r, PT), :] = zs[0, pl.ds(r, PT), :] + (
            jnp.dot(he[pl.ds(R + r, PT), pl.ds(PC, WC)], w2s[0, pl.ds(PC, WC), :], preferred_element_type=F32)
            + jnp.dot(he[pl.ds(R + r, PT), pl.ds(EC + PC, WC)], w2s[0, pl.ds(EC + PC, WC), :], preferred_element_type=F32))
        z_y(0, i, PT).start()

    def z_other(q):
        @pl.loop(0, NP)
        def _(i):
            r = pl.multiple_of(i * MT, MT)
            zs[q, pl.ds(r, MT), :] = jnp.dot(he[pl.ds(R + r, MT), :], w2s[q % 2], preferred_element_type=F32)
            z_y(q, i).start()

    def z_own(q):
        @pl.loop(0, NP)
        def _(i):
            r = pl.ds(pl.multiple_of(i * MT, MT), MT)
            zo[r, pl.ds(q * QC, QC)] = jnp.dot(he[r, :], w2s[q % 2], preferred_element_type=F32)

    layer1d(he, col(j, 0), 0, R, s, 0, 0)
    layer1d(he, col(j, 1), 0, R, s, 1, 0)
    for q in range(NQ):
        if q:
            if q >= 2:
                wait_w2s(q)
            with jax.named_scope('zs'):
                z_other(q)
        with jax.named_scope('zo'):
            z_own(q)
        if q + 2 < NQ:
            for c in loads(q + 2):
                c.start()
        if q == 0:
            with jax.named_scope('yw2'):
                remote(eo, eo, ys, yr.at[3], Y).wait_recv()
            d_eo.start()

    d_co.wait_recv()
    d_eo.wait_recv()

    def second(s):
        wait_tiles(s, 2)
        layer1(hl, WC, 0, R, s, 1)
        layer2(s)

    def layer2(s):
        wait_w2l(s)

        @pl.loop(0, NP)
        def _(i):
            r = pl.ds(pl.multiple_of(i * MT, MT), MT)
            zo[r, :] = zo[r, :] + jnp.dot(hl[r, :], w2l[s], preferred_element_type=F32)

    def late_step(near, k, s, before):
        off = NE if near else NE + NL
        quad = quads_near(s, NE + k) if near else quads_far(s, k)
        for c in quad[:2] + (late_near(s, k) if near else late_far(s, k)):
            c.start()
        with jax.named_scope('xl'):
            (x_w1(NE + k) if near else x_co(k)).wait_recv()
        f = f_w1(off + k)
        f.start()
        quad[2].start()
        before()
        wait_tiles(s, 0)
        wait_tiles(s, 1)
        with jax.named_scope('c0'):
            layer1(hl, 0, 0, R, s, 0)
        with jax.named_scope('fw'):
            f.wait_recv()
        quad[3].start()

    @pl.loop(0, NL)
    def _(k):
        s = lax.rem(NE + k, 2)

        def before():
            @pl.when(k > 0)
            def _():
                second(1 - s)

        late_step(True, k, s, before)

    @pl.loop(0, NL - 2)
    def _(k):
        s = lax.rem(NE + NL + k, 2)
        late_step(False, k, s, lambda: second(1 - s))

    k, s = NL - 2, (NE + 2 * NL - 2) % 2
    second(1 - s)
    late_step(False, k, s, lambda: None)
    second(s)
    s = 1 - s
    for h in range(2):
        for o, (wk, blk) in enumerate(((co, cx), (cp, 1 - cx))):
            pltpu.make_async_copy(wk.at[:, cols_last(h)], w1s.at[s, klo, part(h, o)], lw.at[s, 0]).start()
            for c, src in enumerate((eo, ep)):
                pltpu.make_async_copy(src.at[blk, cols_last(h), :],
                                      w2l.at[s, part(h, o), pl.ds(c * C2, C2)], lu.at[s]).start()

    def sent(n):
        two = pl.ds(2 * n, 2)
        return remote(zs.at[two], ry.at[two], zys.at[n], zyr.at[0], Y)

    wait_tiles(s, 0)
    x_part(0).wait_recv()
    f_part(0).start()
    sent(0).wait_send()
    f_part(0).wait_recv()
    layer1d(hl, 0, 0, R, s, 0, 1)
    wait_w2l(s)

    @pl.loop(0, NP)
    def _(i):
        r = pl.ds(pl.multiple_of(i * MT, MT), MT)
        zo[r, :] = zo[r, :] + jnp.dot(hl[r, lo_c], w2l[s, lo_c, :], preferred_element_type=F32)

    @pl.loop(0, NP)
    def _(i):
        r = pl.ds(pl.multiple_of(i * MT, MT), MT)
        zs[0, r, :] = jnp.dot(xg[r, klo], w1s[s, klo, hi_c], preferred_element_type=F32)

    with jax.named_scope('xl_last'):
        x_part(1).wait_recv()
    f_part(1).start()
    with jax.named_scope('fw'):
        f_part(1).wait_recv()
    with jax.named_scope('c1'):
        @pl.loop(0, NP)
        def _(i):
            r = pl.ds(pl.multiple_of(i * MT, MT), MT)
            c = zs[0, r, :] + jnp.dot(xg[r, khi], w1d[1, :, hi_c], preferred_element_type=F32)
            hl[r, hi_c] = gelu(c.astype(BF16).astype(F32)).astype(BF16)

    def finish(q, i):
        r, l = pl.ds(i * MT, MT), pl.ds(q * QC, QC)
        half, c = divmod(q, NQ // 2)
        lanes = pl.multiple_of((1 - cx if half else cx) * C2 + c * QC, QC)
        z = zo[r, l] + jnp.dot(hl[r, hi_c], w2l[s, hi_c, l], preferred_element_type=F32)
        out[r, pl.ds(lanes, QC)] = (z + ry[q, r, :]).astype(BF16)

    few = pl.ds(0, NQ - 1)
    remote(zs.at[few], ry.at[few], zys.at[0], zyr.at[0], Y).wait_recv()
    with jax.named_scope('fin'):
        for q in range(NQ - 1):
            for i in range(NP):
                finish(q, i)
    for i in range(NP):
        with jax.named_scope('zw'):
            z_y(NQ - 1, i).wait_recv()
        finish(NQ - 1, i)
    sent(1).wait_send()
    remote(bo, bp, ws, wr.at[0], X).wait_send()
    remote(bo, bp, fs, fr.at[0], D).wait_send()
    remote(w1, ap, ys, yr.at[0], Y).wait_send()
    for c in (x_x, d_w1, d_w2, d_co, d_eo):
        c.wait_send()


def solution(mesh):
    data_spec = P(('dp', 'cx', 'cz'), 'cy')
    up_spec = P('cy', ('cz', 'cx'))
    down_spec = P('cz', ('cy', 'cx'))

    def local_mlp(x, w1, w2):
        R, K = x.shape
        B1 = w1.shape[1]
        WC = B1 // (NE + NL)
        EC, LC = NE * WC, NL * WC
        C2 = w2.shape[1]
        QC = 2 * C2 // NQ
        NX = NE + 2 * NL
        dma = pltpu.SemaphoreType.DMA
        any_spec = pl.BlockSpec(memory_space=pl.ANY)
        sds = jax.ShapeDtypeStruct
        outs = (
            pltpu.VMEM((R, K), BF16),
            sds(w1.shape, BF16),
            sds((NX, K, WC), BF16),
            sds((NX, K, WC), BF16),
            sds((K, LC), BF16),
            sds((K, LC), BF16),
            sds(w2.shape, BF16),
            sds((2, LC, C2), BF16),
            sds((2, LC, C2), BF16),
        )
        scratch = [
            pltpu.VMEM((2 * R, 2 * K), BF16),
            pltpu.VMEM((2 * R, 2 * EC), BF16),
            pltpu.VMEM((R, 2 * WC), BF16),
            pltpu.VMEM((2, 2 * K, 2 * WC), BF16),
            pltpu.VMEM((2, K, 2 * WC), BF16),
            pltpu.VMEM((2, 2 * EC, QC), BF16),
            pltpu.VMEM((2, 2 * WC, 2 * C2), BF16),
            pltpu.VMEM((NQ, R, QC), F32),
            pltpu.VMEM((NQ, R, QC), F32),
            pltpu.VMEM((R, 2 * C2), F32),
            dma((1,)), dma((2, 3)), dma((2,)), dma((2,)),
            dma((1,)), dma((1,)),
            dma, dma((NX + 1,)),
            dma, dma((4,)),
            dma((2,)), dma((1 + R // MT,)),
            dma((4,)), dma((4,)),
            dma, dma((NX + 1,)),
        ]
        return pl.pallas_call(
            kernel,
            out_shape=outs,
            in_specs=[any_spec] * 3,
            out_specs=(pl.BlockSpec(memory_space=pltpu.VMEM),) + (any_spec,) * (len(outs) - 1),
            scratch_shapes=scratch,
            compiler_params=pltpu.CompilerParams(
                collective_id=0, has_side_effects=True, vmem_limit_bytes=67043328 - 2 * R * K),
            name='mlp',
        )(x, w1, w2)[0]

    return jax.shard_map(local_mlp, mesh=mesh, in_specs=(data_spec, up_spec, down_spec), out_specs=data_spec, check_vma=False)
```

```python
import jax
import jax.numpy as jnp
from jax import lax
from jax.experimental import pallas as pl
from jax.experimental.pallas import tpu as pltpu
from jax.sharding import PartitionSpec as P

MESH = pl.DeviceIdType.MESH
F32, BF16 = jnp.float32, jnp.bfloat16
NE = 12
NL = 4
NA = 3
NQ = 4
MT = 512
PT = 256


def gelu(c):
    return c * (0.5 * (1.0 + jnp.tanh(0.7978845608028654 * (c + 0.044715 * (c * c * c)))))


def kernel(x, w1, w2, out, ap, bo, bp, co, cp, g0, eo, ep,
           xg, he, hl, w1s, w1d, w2s, w2l, zs, ry, zo,
           lsem, lw, lv, lu, xs, xr, ws, wr, ys, yr, zys, zyr,
           ds, dr, fs, fr):
    cz, cy, cx = lax.axis_index('cz'), lax.axis_index('cy'), lax.axis_index('cx')
    X, Y, D = {'cy': 1 - cy}, {'cz': 1 - cz}, {'cx': 1 - cx}
    R, K = x.shape
    B1 = w1.shape[1]
    WC = B1 // (NE + NL)
    EC, LC = NE * WC, NL * WC
    C2 = w2.shape[1]
    QC = 2 * C2 // NQ

    def remote(src, dst, s, r, dev):
        return pltpu.make_async_remote_copy(src, dst, s, r, device_id=dev, device_id_type=MESH)

    barrier = pltpu.get_barrier_semaphore()
    for dev in (X, Y, D):
        pl.semaphore_signal(barrier, inc=1, device_id=dev, device_id_type=MESH)
    pl.semaphore_wait(barrier, 3)

    own, oth = pl.ds(0, R), pl.ds(R, R)
    klo, khi = pl.ds(0, K), pl.ds(K, K)

    x_x = remote(x, xg.at[own, khi], xs.at[0], xr.at[0], X)
    y_x = remote(x, xg.at[oth, klo], ys, yr.at[0], Y)
    y_xf = remote(xg.at[own, khi], xg.at[oth, khi], ys, yr.at[1], Y)
    y_w1 = remote(w1.at[:, pl.ds(EC, LC)], co, ys, yr.at[2], Y)

    def y_w2(b):
        return remote(w2.at[pl.ds(b * B1 + EC, LC), :], eo.at[b], ys, yr.at[3], Y)

    l_x = pltpu.make_async_copy(x, xg.at[own, klo], lsem.at[0])
    d_w1 = remote(w1, ap, ds.at[0], dr.at[0], D)
    d_w2 = remote(w2, g0, ds.at[1], dr.at[1], D)
    d_co = remote(co, cp, ds.at[2], dr.at[2], D)
    d_eo = remote(eo, ep, ds.at[3], dr.at[3], D)

    def chunk(j):
        return pl.ds(j * WC if isinstance(j, int) else pl.multiple_of(j * WC, WC), WC)

    lo_c, hi_c = pl.ds(0, WC), pl.ds(WC, WC)

    def x_w1(j):
        dst = w1d.at[0, :, lo_c] if isinstance(j, int) and j == NE - 1 else bo.at[j]
        return remote(w1.at[:, chunk(j)], dst, ws, wr.at[j], X)

    def x_co(k):
        return remote(co.at[:, chunk(k)], bo.at[NE + NL + k], ws, wr.at[NE + NL + k], X)

    def f_w1(j):
        return remote(bo.at[j], bp.at[j], fs, fr.at[j], D)

    f_last = remote(w1d.at[0, :, lo_c], w1d.at[0, :, hi_c], fs, fr.at[NE - 1], D)
    HC = WC // 2

    def part(h, other=0):
        return pl.ds((2 * h + other) * HC, HC)

    def cols_last(h):
        return pl.ds((NL - 1) * WC + h * HC, HC)

    def x_part(h):
        return remote(co.at[:, cols_last(h)], w1d.at[1, :, part(h)], ws, wr.at[NE + 2 * NL - 1 + h], X)

    def f_part(h):
        return remote(w1d.at[1, :, part(h)], w1d.at[1, :, part(h, 1)], fs, fr.at[NE + 2 * NL - 1 + h], D)

    def quads(s, j, first, second):
        return [pltpu.make_async_copy(src, w1s.at[s, rows, pl.ds(c * WC, WC)], lw.at[s, i])
                for src, rows, c, i in (
                    (first, klo, 0, 0), (second, klo, 1, 0), (bo.at[j], khi, 0, 1), (bp.at[j], khi, 1, 2))]

    def wait_tiles(s, i):
        if i == 0:
            pltpu.make_async_copy(w1.at[:, pl.ds(0, 2 * WC)], w1s.at[s, klo, :], lw.at[s, 0]).wait()
        else:
            pltpu.make_async_copy(bo.at[0], w1s.at[s, khi, pl.ds((i - 1) * WC, WC)], lw.at[s, i]).wait()

    def wait_w2s(q):
        pltpu.make_async_copy(w2.at[pl.ds(0, 2 * EC), pl.ds(0, QC)], w2s.at[q % 2], lv.at[q % 2]).wait()

    def wait_w2l(s):
        pltpu.make_async_copy(w1.at[pl.ds(0, 2 * WC), pl.ds(0, 2 * C2)], w2l.at[s], lu.at[s]).wait()

    def quads_near(s, j):
        return quads(s, j, w1.at[:, chunk(j)], ap.at[:, chunk(j)])

    def quads_far(s, k):
        return quads(s, NE + NL + k, co.at[:, chunk(k)], cp.at[:, chunk(k)])

    base = (pl.multiple_of(cx * B1, B1), pl.multiple_of((1 - cx) * B1, B1))

    def loads(q):
        src, c = (w2, q) if q < NQ // 2 else (g0, q - NQ // 2)
        return [pltpu.make_async_copy(src.at[pl.ds(base[b], EC), pl.ds(c * QC, QC)],
                                      w2s.at[q % 2, pl.ds(b * EC, EC), :], lv.at[q % 2]) for b in range(2)]

    def late_near(s, k):
        got = []
        for b in range(2):
            rows = pl.ds(pl.multiple_of(base[b] + EC + k * WC, WC), WC)
            for c, src in enumerate((w2, g0)):
                got.append(pltpu.make_async_copy(
                    src.at[rows, :], w2l.at[s, pl.ds(b * WC, WC), pl.ds(c * C2, C2)], lu.at[s]))
        return got

    def late_far(s, k):
        got = []
        for b, blk in enumerate((cx, 1 - cx)):
            for c, src in enumerate((eo, ep)):
                got.append(pltpu.make_async_copy(
                    src.at[blk, chunk(k), :], w2l.at[s, pl.ds(b * WC, WC), pl.ds(c * C2, C2)], lu.at[s]))
        return got

    NP = R // MT

    def z_y(q, i, n=MT):
        rows = pl.ds(i * n if isinstance(i, int) else pl.multiple_of(i * n, n), n)
        return remote(zs.at[q, rows, :], ry.at[q, rows, :], zys.at[0 if q < 2 else 1], zyr.at[0 if q < NQ - 1 else 1 + i], Y)

    def layer1(dst, col, row0, rows, s, half):
        @pl.loop(0, rows // MT)
        def _(i):
            r = pl.multiple_of(i * MT, MT)
            c = jnp.dot(xg[pl.ds(row0 + r, MT), :], w1s[s, :, pl.ds(half * WC, WC)], preferred_element_type=F32)
            dst[pl.ds(row0 + r, MT), pl.ds(col, WC)] = gelu(c.astype(BF16).astype(F32)).astype(BF16)

    def layer1d(dst, col, row0, rows, s, half, i):
        lanes = pl.ds(half * WC, WC)

        @pl.loop(0, rows // MT)
        def _(n):
            r = pl.ds(pl.multiple_of(row0 + n * MT, MT), MT)
            c = (jnp.dot(xg[r, klo], w1s[s, klo, lanes], preferred_element_type=F32)
                 + jnp.dot(xg[r, khi], w1d[i, :, lanes], preferred_element_type=F32))
            dst[r, pl.ds(col, WC)] = gelu(c.astype(BF16).astype(F32)).astype(BF16)

    def step(j):
        s = lax.rem(j, 2)
        q = quads_near(s, j)
        q[0].start()
        q[1].start()
        x_w1(j).wait_recv()
        f_w1(j).start()
        q[2].start()
        wait_tiles(s, 0)
        wait_tiles(s, 1)
        layer1(he, col(j, 0), 0, R, s, 0)
        f_w1(j).wait_recv()
        q[3].start()
        wait_tiles(s, 2)
        layer1(he, col(j, 1), 0, R, s, 1)

    def col(j, half):
        return half * EC + j * WC if isinstance(j, int) else pl.multiple_of(half * EC + j * WC, WC)

    x_x.start()
    y_x.start()
    l_x.start()
    for j in range(NE):
        x_w1(j).start()
    d_w1.start()
    d_w2.start()
    for q in range(2):
        for c in loads(q):
            c.start()

    with jax.named_scope('xx'):
        x_x.wait_recv()
    y_xf.start()
    y_w1.start()
    y_w2(0).start()
    y_w2(1).start()
    l_x.wait()
    d_w1.wait_recv()

    @pl.loop(0, NA)
    def _(j):
        step(j)

    with jax.named_scope('yx'):
        y_x.wait_recv()
        y_xf.wait_recv()

    for n, j in enumerate((2, 1, 0)):
        if n == 2:
            for i in range(3):
                wait_tiles(0, i)
        for half in range(2):
            layer1(he, col(j, half), R, R, j % 2, half)
        if n == 0:
            for c in quads_near(0, 0):
                c.start()
        if n == 1:
            for c in quads_near(NA % 2, NA)[:2]:
                c.start()

    def early_second(j, s):
        wait_tiles(s, 2)
        layer1(he, col(j, 1), 0, 2 * R, s, 1)

    def early(lo, hi):
        @pl.loop(lo, hi)
        def _(j):
            s = lax.rem(j, 2)
            with jax.named_scope('xw'):
                x_w1(j).wait_recv()
            f_w1(j).start()
            q = quads_near(s, j)
            q[2].start()
            if lo == NA:
                @pl.when(j > lo)
                def _():
                    early_second(j - 1, 1 - s)
            else:
                early_second(j - 1, 1 - s)
            for c in quads_near(1 - s, j + 1)[:2]:
                c.start()
            wait_tiles(s, 0)
            wait_tiles(s, 1)
            layer1(he, col(j, 0), 0, 2 * R, s, 0)
            f_w1(j).wait_recv()
            q[3].start()

    early(NA, 8)
    y_w1.wait_recv()
    for k in range(NL):
        x_w1(NE + k).start()
    for k in range(NL - 1):
        x_co(k).start()
    x_part(0).start()
    x_part(1).start()
    d_co.start()
    early(8, 9)

    def z_part(lo, hi, first):
        lanes = [pl.ds(b * EC + lo * WC, (hi - lo) * WC) for b in range(2)]

        @pl.loop(0, NP)
        def _(i):
            r = pl.multiple_of(i * MT, MT)
            z = sum(jnp.dot(he[pl.ds(R + r, MT), l], w2s[0, l, :], preferred_element_type=F32) for l in lanes)
            zs[0, pl.ds(r, MT), :] = z if first else zs[0, pl.ds(r, MT), :] + z

    d_w2.wait_recv()
    wait_w2s(0)
    wait_w2s(1)
    z_part(0, 8, True)
    early(9, NE - 2)
    early_second(NE - 3, (NE - 3) % 2)
    j, s = NE - 2, (NE - 2) % 2
    with jax.named_scope('xw'):
        x_w1(j).wait_recv()
    f_w1(j).start()
    q = quads_near(s, j)
    q[2].start()
    for c in quads_near(1 - s, j + 1)[:2]:
        c.start()
    wait_tiles(s, 0)
    wait_tiles(s, 1)
    layer1(he, col(j, 0), 0, 2 * R, s, 0)
    f_w1(j).wait_recv()
    q[3].start()
    early_second(j, s)
    z_part(8, NE - 1, False)
    PC = EC - WC

    j, s = NE - 1, (NE - 1) % 2
    wait_tiles(s, 0)

    @pl.loop(0, NP)
    def _(i):
        r = pl.multiple_of(i * MT, MT)
        zo[pl.ds(r, MT), pl.ds(0, 2 * WC)] = jnp.dot(
            xg[pl.ds(R + r, MT), klo], w1s[s, klo, :], preferred_element_type=F32)

    with jax.named_scope('xw_last'):
        x_w1(j).wait_recv()
    f_last.start()

    @pl.loop(0, R // PT)
    def _(i):
        r = pl.multiple_of(i * PT, PT)

        def half_chunk(half):
            lanes = pl.ds(half * WC, WC)
            c = zo[pl.ds(r, PT), lanes] + jnp.dot(
                xg[pl.ds(R + r, PT), khi], w1d[0, :, lanes], preferred_element_type=F32)
            he[pl.ds(R + r, PT), pl.ds(col(j, half), WC)] = gelu(c.astype(BF16).astype(F32)).astype(BF16)

        half_chunk(0)

        @pl.when(i == 0)
        def _():
            f_last.wait_recv()

        half_chunk(1)
        zs[0, pl.ds(r, PT), :] = zs[0, pl.ds(r, PT), :] + (
            jnp.dot(he[pl.ds(R + r, PT), pl.ds(PC, WC)], w2s[0, pl.ds(PC, WC), :], preferred_element_type=F32)
            + jnp.dot(he[pl.ds(R + r, PT), pl.ds(EC + PC, WC)], w2s[0, pl.ds(EC + PC, WC), :], preferred_element_type=F32))
        z_y(0, i, PT).start()

    def z_other(q):
        @pl.loop(0, NP)
        def _(i):
            r = pl.multiple_of(i * MT, MT)
            zs[q, pl.ds(r, MT), :] = jnp.dot(he[pl.ds(R + r, MT), :], w2s[q % 2], preferred_element_type=F32)
            z_y(q, i).start()

    def z_own(q):
        @pl.loop(0, NP)
        def _(i):
            r = pl.ds(pl.multiple_of(i * MT, MT), MT)
            zo[r, pl.ds(q * QC, QC)] = jnp.dot(he[r, :], w2s[q % 2], preferred_element_type=F32)

    layer1d(he, col(j, 0), 0, R, s, 0, 0)
    layer1d(he, col(j, 1), 0, R, s, 1, 0)
    for q in range(NQ):
        if q:
            if q >= 2:
                wait_w2s(q)
            with jax.named_scope('zs'):
                z_other(q)
        with jax.named_scope('zo'):
            z_own(q)
        if q + 2 < NQ:
            for c in loads(q + 2):
                c.start()
        if q == 0:
            with jax.named_scope('yw2'):
                remote(eo, eo, ys, yr.at[3], Y).wait_recv()
            d_eo.start()

    d_co.wait_recv()
    d_eo.wait_recv()

    def second(s):
        wait_tiles(s, 2)
        layer1(hl, WC, 0, R, s, 1)
        layer2(s)

    def layer2(s):
        wait_w2l(s)

        @pl.loop(0, NP)
        def _(i):
            r = pl.ds(pl.multiple_of(i * MT, MT), MT)
            zo[r, :] = zo[r, :] + jnp.dot(hl[r, :], w2l[s], preferred_element_type=F32)

    def late_step(near, k, s, before):
        off = NE if near else NE + NL
        quad = quads_near(s, NE + k) if near else quads_far(s, k)
        for c in quad[:2] + (late_near(s, k) if near else late_far(s, k)):
            c.start()
        with jax.named_scope('xl'):
            (x_w1(NE + k) if near else x_co(k)).wait_recv()
        f = f_w1(off + k)
        f.start()
        quad[2].start()
        before()
        wait_tiles(s, 0)
        wait_tiles(s, 1)
        with jax.named_scope('c0'):
            layer1(hl, 0, 0, R, s, 0)
        with jax.named_scope('fw'):
            f.wait_recv()
        quad[3].start()

    @pl.loop(0, NL)
    def _(k):
        s = lax.rem(NE + k, 2)

        def before():
            @pl.when(k > 0)
            def _():
                second(1 - s)

        late_step(True, k, s, before)

    @pl.loop(0, NL - 2)
    def _(k):
        s = lax.rem(NE + NL + k, 2)
        late_step(False, k, s, lambda: second(1 - s))

    k, s = NL - 2, (NE + 2 * NL - 2) % 2
    second(1 - s)
    late_step(False, k, s, lambda: None)
    s = 1 - s
    for h in range(2):
        for o, (wk, blk) in enumerate(((co, cx), (cp, 1 - cx))):
            pltpu.make_async_copy(wk.at[:, cols_last(h)], w1s.at[s, klo, part(h, o)], lw.at[s, 0]).start()
            for c, src in enumerate((eo, ep)):
                pltpu.make_async_copy(src.at[blk, cols_last(h), :],
                                      w2l.at[s, part(h, o), pl.ds(c * C2, C2)], lu.at[s]).start()

    def sent(n):
        two = pl.ds(2 * n, 2)
        return remote(zs.at[two], ry.at[two], zys.at[n], zyr.at[0], Y)

    wait_tiles(1 - s, 2)
    layer1(hl, WC, 0, R, 1 - s, 1)
    x_part(0).wait_recv()
    f_part(0).start()
    layer2(1 - s)
    sent(0).wait_send()
    wait_tiles(s, 0)
    with jax.named_scope('fa'):
        f_part(0).wait_recv()
    layer1d(hl, 0, 0, R, s, 0, 1)
    wait_w2l(s)

    @pl.loop(0, NP)
    def _(i):
        r = pl.ds(pl.multiple_of(i * MT, MT), MT)
        zo[r, :] = zo[r, :] + jnp.dot(hl[r, lo_c], w2l[s, lo_c, :], preferred_element_type=F32)

    @pl.loop(0, NP)
    def _(i):
        r = pl.ds(pl.multiple_of(i * MT, MT), MT)
        zs[0, r, :] = jnp.dot(xg[r, klo], w1s[s, klo, hi_c], preferred_element_type=F32)

    with jax.named_scope('xl_last'):
        x_part(1).wait_recv()
    f_part(1).start()
    with jax.named_scope('fw'):
        f_part(1).wait_recv()
    with jax.named_scope('c1'):
        @pl.loop(0, NP)
        def _(i):
            r = pl.ds(pl.multiple_of(i * MT, MT), MT)
            c = zs[0, r, :] + jnp.dot(xg[r, khi], w1d[1, :, hi_c], preferred_element_type=F32)
            hl[r, hi_c] = gelu(c.astype(BF16).astype(F32)).astype(BF16)

    def finish(q, i):
        r, l = pl.ds(i * MT, MT), pl.ds(q * QC, QC)
        half, c = divmod(q, NQ // 2)
        lanes = pl.multiple_of((1 - cx if half else cx) * C2 + c * QC, QC)
        z = zo[r, l] + jnp.dot(hl[r, hi_c], w2l[s, hi_c, l], preferred_element_type=F32)
        out[r, pl.ds(lanes, QC)] = (z + ry[q, r, :]).astype(BF16)

    few = pl.ds(0, NQ - 1)
    remote(zs.at[few], ry.at[few], zys.at[0], zyr.at[0], Y).wait_recv()
    with jax.named_scope('fin'):
        for q in range(NQ - 1):
            for i in range(NP):
                finish(q, i)
    for i in range(NP):
        with jax.named_scope('zw'):
            z_y(NQ - 1, i).wait_recv()
        finish(NQ - 1, i)
    sent(1).wait_send()
    remote(bo, bp, ws, wr.at[0], X).wait_send()
    remote(bo, bp, fs, fr.at[0], D).wait_send()
    remote(w1, ap, ys, yr.at[0], Y).wait_send()
    for c in (x_x, d_w1, d_w2, d_co, d_eo):
        c.wait_send()


def solution(mesh):
    data_spec = P(('dp', 'cx', 'cz'), 'cy')
    up_spec = P('cy', ('cz', 'cx'))
    down_spec = P('cz', ('cy', 'cx'))

    def local_mlp(x, w1, w2):
        R, K = x.shape
        B1 = w1.shape[1]
        WC = B1 // (NE + NL)
        EC, LC = NE * WC, NL * WC
        C2 = w2.shape[1]
        QC = 2 * C2 // NQ
        NX = NE + 2 * NL
        dma = pltpu.SemaphoreType.DMA
        any_spec = pl.BlockSpec(memory_space=pl.ANY)
        sds = jax.ShapeDtypeStruct
        outs = (
            pltpu.VMEM((R, K), BF16),
            sds(w1.shape, BF16),
            sds((NX, K, WC), BF16),
            sds((NX, K, WC), BF16),
            sds((K, LC), BF16),
            sds((K, LC), BF16),
            sds(w2.shape, BF16),
            sds((2, LC, C2), BF16),
            sds((2, LC, C2), BF16),
        )
        scratch = [
            pltpu.VMEM((2 * R, 2 * K), BF16),
            pltpu.VMEM((2 * R, 2 * EC), BF16),
            pltpu.VMEM((R, 2 * WC), BF16),
            pltpu.VMEM((2, 2 * K, 2 * WC), BF16),
            pltpu.VMEM((2, K, 2 * WC), BF16),
            pltpu.VMEM((2, 2 * EC, QC), BF16),
            pltpu.VMEM((2, 2 * WC, 2 * C2), BF16),
            pltpu.VMEM((NQ, R, QC), F32),
            pltpu.VMEM((NQ, R, QC), F32),
            pltpu.VMEM((R, 2 * C2), F32),
            dma((1,)), dma((2, 3)), dma((2,)), dma((2,)),
            dma((1,)), dma((1,)),
            dma, dma((NX + 1,)),
            dma, dma((4,)),
            dma((2,)), dma((1 + R // MT,)),
            dma((4,)), dma((4,)),
            dma, dma((NX + 1,)),
        ]
        return pl.pallas_call(
            kernel,
            out_shape=outs,
            in_specs=[any_spec] * 3,
            out_specs=(pl.BlockSpec(memory_space=pltpu.VMEM),) + (any_spec,) * (len(outs) - 1),
            scratch_shapes=scratch,
            compiler_params=pltpu.CompilerParams(
                collective_id=0, has_side_effects=True, vmem_limit_bytes=67043328 - 2 * R * K),
            name='mlp',
        )(x, w1, w2)[0]

    return jax.shard_map(local_mlp, mesh=mesh, in_specs=(data_spec, up_spec, down_spec), out_specs=data_spec, check_vma=False)
```

```python
import jax
import jax.numpy as jnp
from jax import lax
from jax.experimental import pallas as pl
from jax.experimental.pallas import tpu as pltpu
from jax.sharding import PartitionSpec as P

MESH = pl.DeviceIdType.MESH
F32, BF16 = jnp.float32, jnp.bfloat16
NE = 12
NL = 4
NA = 3
NQ = 4
MT = 512
PT = 256


def gelu(c):
    return c * (0.5 * (1.0 + jnp.tanh(0.7978845608028654 * (c + 0.044715 * (c * c * c)))))


def kernel(x, w1, w2, out, ap, bo, bp, co, cp, g0, eo, ep,
           xg, he, hl, w1s, w1d, w2s, w2l, zs, ry, zo,
           lsem, lw, lv, lu, xs, xr, ws, wr, ys, yr, zys, zyr,
           ds, dr, fs, fr):
    cz, cy, cx = lax.axis_index('cz'), lax.axis_index('cy'), lax.axis_index('cx')
    X, Y, D = {'cy': 1 - cy}, {'cz': 1 - cz}, {'cx': 1 - cx}
    R, K = x.shape
    B1 = w1.shape[1]
    WC = B1 // (NE + NL)
    EC, LC = NE * WC, NL * WC
    C2 = w2.shape[1]
    QC = 2 * C2 // NQ

    def remote(src, dst, s, r, dev):
        return pltpu.make_async_remote_copy(src, dst, s, r, device_id=dev, device_id_type=MESH)

    barrier = pltpu.get_barrier_semaphore()
    for dev in (X, Y, D):
        pl.semaphore_signal(barrier, inc=1, device_id=dev, device_id_type=MESH)
    pl.semaphore_wait(barrier, 3)

    own, oth = pl.ds(0, R), pl.ds(R, R)
    klo, khi = pl.ds(0, K), pl.ds(K, K)

    x_x = remote(x, xg.at[own, khi], xs.at[0], xr.at[0], X)
    y_x = remote(x, xg.at[oth, klo], ys, yr.at[0], Y)
    y_xf = remote(xg.at[own, khi], xg.at[oth, khi], ys, yr.at[1], Y)
    y_w1 = remote(w1.at[:, pl.ds(EC, LC)], co, ys, yr.at[2], Y)

    def y_w2(b):
        return remote(w2.at[pl.ds(b * B1 + EC, LC), :], eo.at[b], ys, yr.at[3], Y)

    l_x = pltpu.make_async_copy(x, xg.at[own, klo], lsem.at[0])
    d_w1 = remote(w1, ap, ds.at[0], dr.at[0], D)
    d_w2 = remote(w2, g0, ds.at[1], dr.at[1], D)
    d_co = remote(co, cp, ds.at[2], dr.at[2], D)
    d_eo = remote(eo, ep, ds.at[3], dr.at[3], D)

    def chunk(j):
        return pl.ds(j * WC if isinstance(j, int) else pl.multiple_of(j * WC, WC), WC)

    lo_c, hi_c = pl.ds(0, WC), pl.ds(WC, WC)

    def x_w1(j):
        dst = w1d.at[0, :, lo_c] if isinstance(j, int) and j == NE - 1 else bo.at[j]
        return remote(w1.at[:, chunk(j)], dst, ws, wr.at[j], X)

    def x_co(k):
        return remote(co.at[:, chunk(k)], bo.at[NE + NL + k], ws, wr.at[NE + NL + k], X)

    def turn(j):
        return j % 2 if isinstance(j, int) else lax.rem(j, 2)

    def f_w1(j):
        return remote(bo.at[j], bp.at[j], fs, fr.at[turn(j)], D)

    f_last = remote(w1d.at[0, :, lo_c], w1d.at[0, :, hi_c], fs, fr.at[turn(NE - 1)], D)
    HC = WC // 2

    def part(h, other=0):
        return pl.ds((2 * h + other) * HC, HC)

    def cols_last(h):
        return pl.ds((NL - 1) * WC + h * HC, HC)

    def x_part(h):
        return remote(co.at[:, cols_last(h)], w1d.at[1, :, part(h)], ws, wr.at[NE + 2 * NL - 1 + h], X)

    def f_part(h):
        return remote(w1d.at[1, :, part(h)], w1d.at[1, :, part(h, 1)], fs, fr.at[turn(NE + 2 * NL - 1 + h)], D)

    def quads(s, j, first, second):
        return [pltpu.make_async_copy(src, w1s.at[s, rows, pl.ds(c * WC, WC)], lw.at[s, i])
                for src, rows, c, i in (
                    (first, klo, 0, 0), (second, klo, 1, 0), (bo.at[j], khi, 0, 1), (bp.at[j], khi, 1, 2))]

    def wait_tiles(s, i):
        if i == 0:
            pltpu.make_async_copy(w1.at[:, pl.ds(0, 2 * WC)], w1s.at[s, klo, :], lw.at[s, 0]).wait()
        else:
            pltpu.make_async_copy(bo.at[0], w1s.at[s, khi, pl.ds((i - 1) * WC, WC)], lw.at[s, i]).wait()

    def wait_w2s(q):
        pltpu.make_async_copy(w2.at[pl.ds(0, 2 * EC), pl.ds(0, QC)], w2s.at[q % 2], lv.at[q % 2]).wait()

    def wait_w2l(s):
        pltpu.make_async_copy(w1.at[pl.ds(0, 2 * WC), pl.ds(0, 2 * C2)], w2l.at[s], lu.at[s]).wait()

    def quads_near(s, j):
        return quads(s, j, w1.at[:, chunk(j)], ap.at[:, chunk(j)])

    def quads_far(s, k):
        return quads(s, NE + NL + k, co.at[:, chunk(k)], cp.at[:, chunk(k)])

    base = (pl.multiple_of(cx * B1, B1), pl.multiple_of((1 - cx) * B1, B1))

    def loads(q):
        src, c = (w2, q) if q < NQ // 2 else (g0, q - NQ // 2)
        return [pltpu.make_async_copy(src.at[pl.ds(base[b], EC), pl.ds(c * QC, QC)],
                                      w2s.at[q % 2, pl.ds(b * EC, EC), :], lv.at[q % 2]) for b in range(2)]

    def late_near(s, k):
        got = []
        for b in range(2):
            rows = pl.ds(pl.multiple_of(base[b] + EC + k * WC, WC), WC)
            for c, src in enumerate((w2, g0)):
                got.append(pltpu.make_async_copy(
                    src.at[rows, :], w2l.at[s, pl.ds(b * WC, WC), pl.ds(c * C2, C2)], lu.at[s]))
        return got

    def late_far(s, k):
        got = []
        for b, blk in enumerate((cx, 1 - cx)):
            for c, src in enumerate((eo, ep)):
                got.append(pltpu.make_async_copy(
                    src.at[blk, chunk(k), :], w2l.at[s, pl.ds(b * WC, WC), pl.ds(c * C2, C2)], lu.at[s]))
        return got

    NP = R // MT

    def z_y(q, i, n=MT):
        rows = pl.ds(i * n if isinstance(i, int) else pl.multiple_of(i * n, n), n)
        return remote(zs.at[q, rows, :], ry.at[q, rows, :], zys.at[0 if q < 2 else 1], zyr.at[0 if q < NQ - 1 else 1 + i], Y)

    def layer1(dst, col, row0, rows, s, half):
        @pl.loop(0, rows // MT)
        def _(i):
            r = pl.multiple_of(i * MT, MT)
            c = jnp.dot(xg[pl.ds(row0 + r, MT), :], w1s[s, :, pl.ds(half * WC, WC)], preferred_element_type=F32)
            dst[pl.ds(row0 + r, MT), pl.ds(col, WC)] = gelu(c.astype(BF16).astype(F32)).astype(BF16)

    def layer1d(dst, col, row0, rows, s, half, i):
        lanes = pl.ds(half * WC, WC)

        @pl.loop(0, rows // MT)
        def _(n):
            r = pl.ds(pl.multiple_of(row0 + n * MT, MT), MT)
            c = (jnp.dot(xg[r, klo], w1s[s, klo, lanes], preferred_element_type=F32)
                 + jnp.dot(xg[r, khi], w1d[i, :, lanes], preferred_element_type=F32))
            dst[r, pl.ds(col, WC)] = gelu(c.astype(BF16).astype(F32)).astype(BF16)

    def step(j):
        s = lax.rem(j, 2)
        q = quads_near(s, j)
        q[0].start()
        q[1].start()
        x_w1(j).wait_recv()
        f_w1(j).start()
        q[2].start()
        wait_tiles(s, 0)
        wait_tiles(s, 1)
        layer1(he, col(j, 0), 0, R, s, 0)
        f_w1(j).wait_recv()
        q[3].start()
        wait_tiles(s, 2)
        layer1(he, col(j, 1), 0, R, s, 1)

    def col(j, half):
        return half * EC + j * WC if isinstance(j, int) else pl.multiple_of(half * EC + j * WC, WC)

    x_x.start()
    y_x.start()
    l_x.start()
    for j in range(NE):
        x_w1(j).start()
    d_w1.start()
    d_w2.start()
    for q in range(2):
        for c in loads(q):
            c.start()

    x_x.wait_recv()
    y_xf.start()
    y_w1.start()
    y_w2(0).start()
    y_w2(1).start()
    l_x.wait()
    d_w1.wait_recv()

    @pl.loop(0, NA)
    def _(j):
        step(j)

    y_x.wait_recv()
    y_xf.wait_recv()

    for n, j in enumerate((2, 1, 0)):
        if n == 2:
            for i in range(3):
                wait_tiles(0, i)
        for half in range(2):
            layer1(he, col(j, half), R, R, j % 2, half)
        if n == 0:
            for c in quads_near(0, 0):
                c.start()
        if n == 1:
            for c in quads_near(NA % 2, NA)[:2]:
                c.start()

    def early_second(j, s):
        wait_tiles(s, 2)
        layer1(he, col(j, 1), 0, 2 * R, s, 1)

    def early(lo, hi):
        @pl.loop(lo, hi)
        def _(j):
            s = lax.rem(j, 2)
            x_w1(j).wait_recv()
            f_w1(j).start()
            q = quads_near(s, j)
            q[2].start()
            if lo == NA:
                @pl.when(j > lo)
                def _():
                    early_second(j - 1, 1 - s)
            else:
                early_second(j - 1, 1 - s)
            for c in quads_near(1 - s, j + 1)[:2]:
                c.start()
            wait_tiles(s, 0)
            wait_tiles(s, 1)
            layer1(he, col(j, 0), 0, 2 * R, s, 0)
            f_w1(j).wait_recv()
            q[3].start()

    early(NA, 8)
    y_w1.wait_recv()
    for k in range(NL):
        x_w1(NE + k).start()
    for k in range(NL - 1):
        x_co(k).start()
    x_part(0).start()
    x_part(1).start()
    d_co.start()
    early(8, 9)

    def z_part(lo, hi, first):
        lanes = [pl.ds(b * EC + lo * WC, (hi - lo) * WC) for b in range(2)]

        @pl.loop(0, NP)
        def _(i):
            r = pl.multiple_of(i * MT, MT)
            z = sum(jnp.dot(he[pl.ds(R + r, MT), l], w2s[0, l, :], preferred_element_type=F32) for l in lanes)
            zs[0, pl.ds(r, MT), :] = z if first else zs[0, pl.ds(r, MT), :] + z

    d_w2.wait_recv()
    wait_w2s(0)
    wait_w2s(1)
    z_part(0, 8, True)
    early(9, NE - 2)
    early_second(NE - 3, (NE - 3) % 2)
    j, s = NE - 2, (NE - 2) % 2
    x_w1(j).wait_recv()
    f_w1(j).start()
    q = quads_near(s, j)
    q[2].start()
    for c in quads_near(1 - s, j + 1)[:2]:
        c.start()
    wait_tiles(s, 0)
    wait_tiles(s, 1)
    layer1(he, col(j, 0), 0, 2 * R, s, 0)
    f_w1(j).wait_recv()
    q[3].start()
    early_second(j, s)
    z_part(8, NE - 1, False)
    PC = EC - WC

    j, s = NE - 1, (NE - 1) % 2
    wait_tiles(s, 0)

    @pl.loop(0, NP)
    def _(i):
        r = pl.multiple_of(i * MT, MT)
        zo[pl.ds(r, MT), pl.ds(0, 2 * WC)] = jnp.dot(
            xg[pl.ds(R + r, MT), klo], w1s[s, klo, :], preferred_element_type=F32)

    x_w1(j).wait_recv()
    f_last.start()

    @pl.loop(0, R // PT)
    def _(i):
        r = pl.multiple_of(i * PT, PT)

        def half_chunk(half):
            lanes = pl.ds(half * WC, WC)
            c = zo[pl.ds(r, PT), lanes] + jnp.dot(
                xg[pl.ds(R + r, PT), khi], w1d[0, :, lanes], preferred_element_type=F32)
            he[pl.ds(R + r, PT), pl.ds(col(j, half), WC)] = gelu(c.astype(BF16).astype(F32)).astype(BF16)

        half_chunk(0)

        @pl.when(i == 0)
        def _():
            f_last.wait_recv()

        half_chunk(1)
        zs[0, pl.ds(r, PT), :] = zs[0, pl.ds(r, PT), :] + (
            jnp.dot(he[pl.ds(R + r, PT), pl.ds(PC, WC)], w2s[0, pl.ds(PC, WC), :], preferred_element_type=F32)
            + jnp.dot(he[pl.ds(R + r, PT), pl.ds(EC + PC, WC)], w2s[0, pl.ds(EC + PC, WC), :], preferred_element_type=F32))
        z_y(0, i, PT).start()

    def z_other(q):
        @pl.loop(0, NP)
        def _(i):
            r = pl.multiple_of(i * MT, MT)
            zs[q, pl.ds(r, MT), :] = jnp.dot(he[pl.ds(R + r, MT), :], w2s[q % 2], preferred_element_type=F32)
            z_y(q, i).start()

    def z_own(q):
        @pl.loop(0, NP)
        def _(i):
            r = pl.ds(pl.multiple_of(i * MT, MT), MT)
            zo[r, pl.ds(q * QC, QC)] = jnp.dot(he[r, :], w2s[q % 2], preferred_element_type=F32)

    layer1d(he, col(j, 0), 0, R, s, 0, 0)
    layer1d(he, col(j, 1), 0, R, s, 1, 0)
    for q in range(NQ):
        if q:
            if q >= 2:
                wait_w2s(q)
            z_other(q)
        z_own(q)
        if q + 2 < NQ:
            for c in loads(q + 2):
                c.start()
        if q == 0:
            remote(eo, eo, ys, yr.at[3], Y).wait_recv()
            d_eo.start()

    d_co.wait_recv()
    d_eo.wait_recv()

    def second(s):
        wait_tiles(s, 2)
        layer1(hl, WC, 0, R, s, 1)
        layer2(s)

    def layer2(s):
        wait_w2l(s)

        @pl.loop(0, NP)
        def _(i):
            r = pl.ds(pl.multiple_of(i * MT, MT), MT)
            zo[r, :] = zo[r, :] + jnp.dot(hl[r, :], w2l[s], preferred_element_type=F32)

    def late_step(near, k, s, before):
        off = NE if near else NE + NL
        quad = quads_near(s, NE + k) if near else quads_far(s, k)
        for c in quad[:2] + (late_near(s, k) if near else late_far(s, k)):
            c.start()
        (x_w1(NE + k) if near else x_co(k)).wait_recv()
        f = f_w1(off + k)
        f.start()
        quad[2].start()
        before()
        wait_tiles(s, 0)
        wait_tiles(s, 1)
        layer1(hl, 0, 0, R, s, 0)
        f.wait_recv()
        quad[3].start()

    @pl.loop(0, NL)
    def _(k):
        s = lax.rem(NE + k, 2)

        def before():
            @pl.when(k > 0)
            def _():
                second(1 - s)

        late_step(True, k, s, before)

    @pl.loop(0, NL - 2)
    def _(k):
        s = lax.rem(NE + NL + k, 2)
        late_step(False, k, s, lambda: second(1 - s))

    k, s = NL - 2, (NE + 2 * NL - 2) % 2
    second(1 - s)
    late_step(False, k, s, lambda: None)
    s = 1 - s
    for h in range(2):
        for o, (wk, blk) in enumerate(((co, cx), (cp, 1 - cx))):
            pltpu.make_async_copy(wk.at[:, cols_last(h)], w1s.at[s, klo, part(h, o)], lw.at[s, 0]).start()
            for c, src in enumerate((eo, ep)):
                pltpu.make_async_copy(src.at[blk, cols_last(h), :],
                                      w2l.at[s, part(h, o), pl.ds(c * C2, C2)], lu.at[s]).start()

    def sent(n):
        two = pl.ds(2 * n, 2)
        return remote(zs.at[two], ry.at[two], zys.at[n], zyr.at[0], Y)

    wait_tiles(1 - s, 2)
    layer1(hl, WC, 0, R, 1 - s, 1)
    x_part(0).wait_recv()
    f_part(0).start()
    layer2(1 - s)
    sent(0).wait_send()
    wait_tiles(s, 0)
    f_part(0).wait_recv()
    layer1d(hl, 0, 0, R, s, 0, 1)
    wait_w2l(s)

    @pl.loop(0, NP)
    def _(i):
        r = pl.ds(pl.multiple_of(i * MT, MT), MT)
        zo[r, :] = zo[r, :] + jnp.dot(hl[r, lo_c], w2l[s, lo_c, :], preferred_element_type=F32)

    @pl.loop(0, NP)
    def _(i):
        r = pl.ds(pl.multiple_of(i * MT, MT), MT)
        zs[0, r, :] = jnp.dot(xg[r, klo], w1s[s, klo, hi_c], preferred_element_type=F32)

    x_part(1).wait_recv()
    f_part(1).start()
    f_part(1).wait_recv()
    @pl.loop(0, NP)
    def _(i):
        r = pl.ds(pl.multiple_of(i * MT, MT), MT)
        c = zs[0, r, :] + jnp.dot(xg[r, khi], w1d[1, :, hi_c], preferred_element_type=F32)
        hl[r, hi_c] = gelu(c.astype(BF16).astype(F32)).astype(BF16)

    def finish(q, i):
        r, l = pl.ds(i * MT, MT), pl.ds(q * QC, QC)
        half, c = divmod(q, NQ // 2)
        lanes = pl.multiple_of((1 - cx if half else cx) * C2 + c * QC, QC)
        z = zo[r, l] + jnp.dot(hl[r, hi_c], w2l[s, hi_c, l], preferred_element_type=F32)
        out[r, pl.ds(lanes, QC)] = (z + ry[q, r, :]).astype(BF16)

    few = pl.ds(0, NQ - 1)
    remote(zs.at[few], ry.at[few], zys.at[0], zyr.at[0], Y).wait_recv()
    for q in range(NQ - 1):
        for i in range(NP):
            finish(q, i)
    for i in range(NP):
        z_y(NQ - 1, i).wait_recv()
        finish(NQ - 1, i)
    sent(1).wait_send()
    remote(bo, bp, ws, wr.at[0], X).wait_send()
    remote(bo, bp, fs, fr.at[0], D).wait_send()
    remote(w1, ap, ys, yr.at[0], Y).wait_send()
    for c in (x_x, d_w1, d_w2, d_co, d_eo):
        c.wait_send()


def solution(mesh):
    data_spec = P(('dp', 'cx', 'cz'), 'cy')
    up_spec = P('cy', ('cz', 'cx'))
    down_spec = P('cz', ('cy', 'cx'))

    def local_mlp(x, w1, w2):
        R, K = x.shape
        B1 = w1.shape[1]
        WC = B1 // (NE + NL)
        EC, LC = NE * WC, NL * WC
        C2 = w2.shape[1]
        QC = 2 * C2 // NQ
        NX = NE + 2 * NL
        dma = pltpu.SemaphoreType.DMA
        any_spec = pl.BlockSpec(memory_space=pl.ANY)
        sds = jax.ShapeDtypeStruct
        outs = (
            pltpu.VMEM((R, K), BF16),
            sds(w1.shape, BF16),
            sds((NX, K, WC), BF16),
            sds((NX, K, WC), BF16),
            sds((K, LC), BF16),
            sds((K, LC), BF16),
            sds(w2.shape, BF16),
            sds((2, LC, C2), BF16),
            sds((2, LC, C2), BF16),
        )
        scratch = [
            pltpu.VMEM((2 * R, 2 * K), BF16),
            pltpu.VMEM((2 * R, 2 * EC), BF16),
            pltpu.VMEM((R, 2 * WC), BF16),
            pltpu.VMEM((2, 2 * K, 2 * WC), BF16),
            pltpu.VMEM((2, K, 2 * WC), BF16),
            pltpu.VMEM((2, 2 * EC, QC), BF16),
            pltpu.VMEM((2, 2 * WC, 2 * C2), BF16),
            pltpu.VMEM((NQ, R, QC), F32),
            pltpu.VMEM((NQ, R, QC), F32),
            pltpu.VMEM((R, 2 * C2), F32),
            dma((1,)), dma((2, 3)), dma((2,)), dma((2,)),
            dma((1,)), dma((1,)),
            dma, dma((NX + 1,)),
            dma, dma((4,)),
            dma((2,)), dma((1 + R // MT,)),
            dma((4,)), dma((4,)),
            dma, dma((2,)),
        ]
        return pl.pallas_call(
            kernel,
            out_shape=outs,
            in_specs=[any_spec] * 3,
            out_specs=(pl.BlockSpec(memory_space=pltpu.VMEM),) + (any_spec,) * (len(outs) - 1),
            scratch_shapes=scratch,
            compiler_params=pltpu.CompilerParams(
                collective_id=0, has_side_effects=True, vmem_limit_bytes=67043328 - 2 * R * K),
            name='mlp',
        )(x, w1, w2)[0]

    return jax.shard_map(local_mlp, mesh=mesh, in_specs=(data_spec, up_spec, down_spec), out_specs=data_spec, check_vma=False)
```

```python
import jax
import jax.numpy as jnp
from jax import lax
from jax.experimental import pallas as pl
from jax.experimental.pallas import tpu as pltpu
from jax.sharding import PartitionSpec as P

MESH = pl.DeviceIdType.MESH
F32, BF16 = jnp.float32, jnp.bfloat16
NE = 12
NL = 4
NA = 3
NQ = 4
MT = 512
PT = 128


def gelu(c):
    return c * (0.5 * (1.0 + jnp.tanh(0.7978845608028654 * (c + 0.044715 * (c * c * c)))))


def kernel(x, w1, w2, out, ap, bo, bp, co, cp, g0, eo, ep,
           xg, he, hl, w1s, w1d, w2s, w2l, zs, ry, zo,
           lsem, lw, lv, lu, xs, xr, ws, wr, ys, yr, zys, zyr,
           ds, dr, fs, fr):
    cz, cy, cx = lax.axis_index('cz'), lax.axis_index('cy'), lax.axis_index('cx')
    X, Y, D = {'cy': 1 - cy}, {'cz': 1 - cz}, {'cx': 1 - cx}
    R, K = x.shape
    B1 = w1.shape[1]
    WC = B1 // (NE + NL)
    EC, LC = NE * WC, NL * WC
    C2 = w2.shape[1]
    QC = 2 * C2 // NQ

    def remote(src, dst, s, r, dev):
        return pltpu.make_async_remote_copy(src, dst, s, r, device_id=dev, device_id_type=MESH)

    barrier = pltpu.get_barrier_semaphore()
    for dev in (X, Y, D):
        pl.semaphore_signal(barrier, inc=1, device_id=dev, device_id_type=MESH)
    pl.semaphore_wait(barrier, 3)

    own, oth = pl.ds(0, R), pl.ds(R, R)
    klo, khi = pl.ds(0, K), pl.ds(K, K)

    x_x = remote(x, xg.at[own, khi], xs.at[0], xr.at[0], X)
    y_x = remote(x, xg.at[oth, klo], ys, yr.at[0], Y)
    y_xf = remote(xg.at[own, khi], xg.at[oth, khi], ys, yr.at[1], Y)
    y_w1 = remote(w1.at[:, pl.ds(EC, LC)], co, ys, yr.at[2], Y)

    def y_w2(b):
        return remote(w2.at[pl.ds(b * B1 + EC, LC), :], eo.at[b], ys, yr.at[3], Y)

    l_x = pltpu.make_async_copy(x, xg.at[own, klo], lsem.at[0])
    d_w1 = remote(w1, ap, ds.at[0], dr.at[0], D)
    d_w2 = remote(w2, g0, ds.at[1], dr.at[1], D)
    d_co = remote(co, cp, ds.at[2], dr.at[2], D)
    d_eo = remote(eo, ep, ds.at[3], dr.at[3], D)

    def chunk(j):
        return pl.ds(j * WC if isinstance(j, int) else pl.multiple_of(j * WC, WC), WC)

    lo_c, hi_c = pl.ds(0, WC), pl.ds(WC, WC)

    def x_w1(j):
        dst = w1d.at[0, :, lo_c] if isinstance(j, int) and j == NE - 1 else bo.at[j]
        return remote(w1.at[:, chunk(j)], dst, ws, wr.at[j], X)

    def x_co(k):
        return remote(co.at[:, chunk(k)], bo.at[NE + NL + k], ws, wr.at[NE + NL + k], X)

    def turn(j):
        return j % 2 if isinstance(j, int) else lax.rem(j, 2)

    def f_w1(j):
        return remote(bo.at[j], bp.at[j], fs, fr.at[turn(j)], D)

    f_last = remote(w1d.at[0, :, lo_c], w1d.at[0, :, hi_c], fs, fr.at[turn(NE - 1)], D)
    HC = WC // 2

    def part(h, other=0):
        return pl.ds((2 * h + other) * HC, HC)

    def cols_last(h):
        return pl.ds((NL - 1) * WC + h * HC, HC)

    def x_part(h):
        return remote(co.at[:, cols_last(h)], w1d.at[1, :, part(h)], ws, wr.at[NE + 2 * NL - 1 + h], X)

    def f_part(h):
        return remote(w1d.at[1, :, part(h)], w1d.at[1, :, part(h, 1)], fs, fr.at[turn(NE + 2 * NL - 1 + h)], D)

    def quads(s, j, first, second):
        return [pltpu.make_async_copy(src, w1s.at[s, rows, pl.ds(c * WC, WC)], lw.at[s, i])
                for src, rows, c, i in (
                    (first, klo, 0, 0), (second, klo, 1, 0), (bo.at[j], khi, 0, 1), (bp.at[j], khi, 1, 2))]

    def wait_tiles(s, i):
        if i == 0:
            pltpu.make_async_copy(w1.at[:, pl.ds(0, 2 * WC)], w1s.at[s, klo, :], lw.at[s, 0]).wait()
        else:
            pltpu.make_async_copy(bo.at[0], w1s.at[s, khi, pl.ds((i - 1) * WC, WC)], lw.at[s, i]).wait()

    def wait_w2s(q):
        pltpu.make_async_copy(w2.at[pl.ds(0, 2 * EC), pl.ds(0, QC)], w2s.at[q % 2], lv.at[q % 2]).wait()

    def wait_w2l(s):
        pltpu.make_async_copy(w1.at[pl.ds(0, 2 * WC), pl.ds(0, 2 * C2)], w2l.at[s], lu.at[s]).wait()

    def quads_near(s, j):
        return quads(s, j, w1.at[:, chunk(j)], ap.at[:, chunk(j)])

    def quads_far(s, k):
        return quads(s, NE + NL + k, co.at[:, chunk(k)], cp.at[:, chunk(k)])

    base = (pl.multiple_of(cx * B1, B1), pl.multiple_of((1 - cx) * B1, B1))

    def loads(q):
        src, c = (w2, q) if q < NQ // 2 else (g0, q - NQ // 2)
        return [pltpu.make_async_copy(src.at[pl.ds(base[b], EC), pl.ds(c * QC, QC)],
                                      w2s.at[q % 2, pl.ds(b * EC, EC), :], lv.at[q % 2]) for b in range(2)]

    def late_near(s, k):
        got = []
        for b in range(2):
            rows = pl.ds(pl.multiple_of(base[b] + EC + k * WC, WC), WC)
            for c, src in enumerate((w2, g0)):
                got.append(pltpu.make_async_copy(
                    src.at[rows, :], w2l.at[s, pl.ds(b * WC, WC), pl.ds(c * C2, C2)], lu.at[s]))
        return got

    def late_far(s, k):
        got = []
        for b, blk in enumerate((cx, 1 - cx)):
            for c, src in enumerate((eo, ep)):
                got.append(pltpu.make_async_copy(
                    src.at[blk, chunk(k), :], w2l.at[s, pl.ds(b * WC, WC), pl.ds(c * C2, C2)], lu.at[s]))
        return got

    NP = R // MT

    def z_y(q, i, n=MT):
        rows = pl.ds(i * n if isinstance(i, int) else pl.multiple_of(i * n, n), n)
        return remote(zs.at[q, rows, :], ry.at[q, rows, :], zys.at[0 if q < 2 else 1], zyr.at[0 if q < NQ - 1 else 1 + i], Y)

    def layer1(dst, col, row0, rows, s, half):
        @pl.loop(0, rows // MT)
        def _(i):
            r = pl.multiple_of(i * MT, MT)
            c = jnp.dot(xg[pl.ds(row0 + r, MT), :], w1s[s, :, pl.ds(half * WC, WC)], preferred_element_type=F32)
            dst[pl.ds(row0 + r, MT), pl.ds(col, WC)] = gelu(c.astype(BF16).astype(F32)).astype(BF16)

    def layer1d(dst, col, row0, rows, s, half, i):
        lanes = pl.ds(half * WC, WC)

        @pl.loop(0, rows // MT)
        def _(n):
            r = pl.ds(pl.multiple_of(row0 + n * MT, MT), MT)
            c = (jnp.dot(xg[r, klo], w1s[s, klo, lanes], preferred_element_type=F32)
                 + jnp.dot(xg[r, khi], w1d[i, :, lanes], preferred_element_type=F32))
            dst[r, pl.ds(col, WC)] = gelu(c.astype(BF16).astype(F32)).astype(BF16)

    def step(j):
        s = lax.rem(j, 2)
        q = quads_near(s, j)
        q[0].start()
        q[1].start()
        x_w1(j).wait_recv()
        f_w1(j).start()
        q[2].start()
        wait_tiles(s, 0)
        wait_tiles(s, 1)
        layer1(he, col(j, 0), 0, R, s, 0)
        f_w1(j).wait_recv()
        q[3].start()
        wait_tiles(s, 2)
        layer1(he, col(j, 1), 0, R, s, 1)

    def col(j, half):
        return half * EC + j * WC if isinstance(j, int) else pl.multiple_of(half * EC + j * WC, WC)

    x_x.start()
    y_x.start()
    l_x.start()
    for j in range(NE):
        x_w1(j).start()
    d_w1.start()
    d_w2.start()
    for q in range(2):
        for c in loads(q):
            c.start()

    x_x.wait_recv()
    y_xf.start()
    y_w1.start()
    y_w2(0).start()
    y_w2(1).start()
    l_x.wait()
    d_w1.wait_recv()

    @pl.loop(0, NA)
    def _(j):
        step(j)

    y_x.wait_recv()
    y_xf.wait_recv()

    for n, j in enumerate((2, 1, 0)):
        if n == 2:
            for i in range(3):
                wait_tiles(0, i)
        for half in range(2):
            layer1(he, col(j, half), R, R, j % 2, half)
        if n == 0:
            for c in quads_near(0, 0):
                c.start()
        if n == 1:
            for c in quads_near(NA % 2, NA)[:2]:
                c.start()

    def early_second(j, s):
        wait_tiles(s, 2)
        layer1(he, col(j, 1), 0, 2 * R, s, 1)

    def early(lo, hi):
        @pl.loop(lo, hi)
        def _(j):
            s = lax.rem(j, 2)
            x_w1(j).wait_recv()
            f_w1(j).start()
            q = quads_near(s, j)
            q[2].start()
            if lo == NA:
                @pl.when(j > lo)
                def _():
                    early_second(j - 1, 1 - s)
            else:
                early_second(j - 1, 1 - s)
            for c in quads_near(1 - s, j + 1)[:2]:
                c.start()
            wait_tiles(s, 0)
            wait_tiles(s, 1)
            layer1(he, col(j, 0), 0, 2 * R, s, 0)
            f_w1(j).wait_recv()
            q[3].start()

    early(NA, 8)
    y_w1.wait_recv()
    for k in range(NL):
        x_w1(NE + k).start()
    for k in range(NL - 1):
        x_co(k).start()
    x_part(0).start()
    x_part(1).start()
    d_co.start()
    early(8, 9)

    def z_part(lo, hi, first):
        lanes = [pl.ds(b * EC + lo * WC, (hi - lo) * WC) for b in range(2)]

        @pl.loop(0, NP)
        def _(i):
            r = pl.multiple_of(i * MT, MT)
            z = sum(jnp.dot(he[pl.ds(R + r, MT), l], w2s[0, l, :], preferred_element_type=F32) for l in lanes)
            zs[0, pl.ds(r, MT), :] = z if first else zs[0, pl.ds(r, MT), :] + z

    d_w2.wait_recv()
    wait_w2s(0)
    wait_w2s(1)
    z_part(0, 8, True)
    early(9, NE - 2)
    early_second(NE - 3, (NE - 3) % 2)
    j, s = NE - 2, (NE - 2) % 2
    x_w1(j).wait_recv()
    f_w1(j).start()
    q = quads_near(s, j)
    q[2].start()
    for c in quads_near(1 - s, j + 1)[:2]:
        c.start()
    wait_tiles(s, 0)
    wait_tiles(s, 1)
    layer1(he, col(j, 0), 0, 2 * R, s, 0)
    f_w1(j).wait_recv()
    q[3].start()
    early_second(j, s)
    z_part(8, NE - 1, False)
    PC = EC - WC

    j, s = NE - 1, (NE - 1) % 2
    wait_tiles(s, 0)

    @pl.loop(0, NP)
    def _(i):
        r = pl.multiple_of(i * MT, MT)
        zo[pl.ds(r, MT), pl.ds(0, 2 * WC)] = jnp.dot(
            xg[pl.ds(R + r, MT), klo], w1s[s, klo, :], preferred_element_type=F32)

    x_w1(j).wait_recv()
    f_last.start()

    @pl.loop(0, R // PT)
    def _(i):
        r = pl.multiple_of(i * PT, PT)

        def half_chunk(half):
            lanes = pl.ds(half * WC, WC)
            c = zo[pl.ds(r, PT), lanes] + jnp.dot(
                xg[pl.ds(R + r, PT), khi], w1d[0, :, lanes], preferred_element_type=F32)
            he[pl.ds(R + r, PT), pl.ds(col(j, half), WC)] = gelu(c.astype(BF16).astype(F32)).astype(BF16)

        half_chunk(0)

        @pl.when(i == 0)
        def _():
            f_last.wait_recv()

        half_chunk(1)
        zs[0, pl.ds(r, PT), :] = zs[0, pl.ds(r, PT), :] + (
            jnp.dot(he[pl.ds(R + r, PT), pl.ds(PC, WC)], w2s[0, pl.ds(PC, WC), :], preferred_element_type=F32)
            + jnp.dot(he[pl.ds(R + r, PT), pl.ds(EC + PC, WC)], w2s[0, pl.ds(EC + PC, WC), :], preferred_element_type=F32))
        z_y(0, i, PT).start()

    def z_other(q):
        @pl.loop(0, NP)
        def _(i):
            r = pl.multiple_of(i * MT, MT)
            zs[q, pl.ds(r, MT), :] = jnp.dot(he[pl.ds(R + r, MT), :], w2s[q % 2], preferred_element_type=F32)
            z_y(q, i).start()

    def z_own(q):
        @pl.loop(0, NP)
        def _(i):
            r = pl.ds(pl.multiple_of(i * MT, MT), MT)
            zo[r, pl.ds(q * QC, QC)] = jnp.dot(he[r, :], w2s[q % 2], preferred_element_type=F32)

    layer1d(he, col(j, 0), 0, R, s, 0, 0)
    layer1d(he, col(j, 1), 0, R, s, 1, 0)
    for q in range(NQ):
        if q:
            if q >= 2:
                wait_w2s(q)
            z_other(q)
        z_own(q)
        if q + 2 < NQ:
            for c in loads(q + 2):
                c.start()
        if q == 0:
            remote(eo, eo, ys, yr.at[3], Y).wait_recv()
            d_eo.start()

    d_co.wait_recv()
    d_eo.wait_recv()

    def second(s):
        wait_tiles(s, 2)
        layer1(hl, WC, 0, R, s, 1)
        layer2(s)

    def layer2(s):
        wait_w2l(s)

        @pl.loop(0, NP)
        def _(i):
            r = pl.ds(pl.multiple_of(i * MT, MT), MT)
            zo[r, :] = zo[r, :] + jnp.dot(hl[r, :], w2l[s], preferred_element_type=F32)

    def late_step(near, k, s, before):
        off = NE if near else NE + NL
        quad = quads_near(s, NE + k) if near else quads_far(s, k)
        for c in quad[:2] + (late_near(s, k) if near else late_far(s, k)):
            c.start()
        (x_w1(NE + k) if near else x_co(k)).wait_recv()
        f = f_w1(off + k)
        f.start()
        quad[2].start()
        before()
        wait_tiles(s, 0)
        wait_tiles(s, 1)
        layer1(hl, 0, 0, R, s, 0)
        f.wait_recv()
        quad[3].start()

    @pl.loop(0, NL)
    def _(k):
        s = lax.rem(NE + k, 2)

        def before():
            @pl.when(k > 0)
            def _():
                second(1 - s)

        late_step(True, k, s, before)

    @pl.loop(0, NL - 2)
    def _(k):
        s = lax.rem(NE + NL + k, 2)
        late_step(False, k, s, lambda: second(1 - s))

    k, s = NL - 2, (NE + 2 * NL - 2) % 2
    second(1 - s)
    late_step(False, k, s, lambda: None)
    s = 1 - s
    for h in range(2):
        for o, (wk, blk) in enumerate(((co, cx), (cp, 1 - cx))):
            pltpu.make_async_copy(wk.at[:, cols_last(h)], w1s.at[s, klo, part(h, o)], lw.at[s, 0]).start()
            for c, src in enumerate((eo, ep)):
                pltpu.make_async_copy(src.at[blk, cols_last(h), :],
                                      w2l.at[s, part(h, o), pl.ds(c * C2, C2)], lu.at[s]).start()

    def sent(n):
        two = pl.ds(2 * n, 2)
        return remote(zs.at[two], ry.at[two], zys.at[n], zyr.at[0], Y)

    wait_tiles(1 - s, 2)
    layer1(hl, WC, 0, R, 1 - s, 1)
    x_part(0).wait_recv()
    f_part(0).start()
    layer2(1 - s)
    sent(0).wait_send()
    wait_tiles(s, 0)
    f_part(0).wait_recv()
    layer1d(hl, 0, 0, R, s, 0, 1)
    wait_w2l(s)

    @pl.loop(0, NP)
    def _(i):
        r = pl.ds(pl.multiple_of(i * MT, MT), MT)
        zo[r, :] = zo[r, :] + jnp.dot(hl[r, lo_c], w2l[s, lo_c, :], preferred_element_type=F32)

    def take():
        x_part(1).wait_recv()
        f_part(1).start()

    pl.when(cx == 1)(take)

    @pl.loop(0, NP)
    def _(i):
        r = pl.ds(pl.multiple_of(i * MT, MT), MT)
        zs[0, r, :] = jnp.dot(xg[r, klo], w1s[s, klo, hi_c], preferred_element_type=F32)
        pl.when((cx == 0) & (i == 0))(take)

    f_part(1).wait_recv()
    @pl.loop(0, NP)
    def _(i):
        r = pl.ds(pl.multiple_of(i * MT, MT), MT)
        c = zs[0, r, :] + jnp.dot(xg[r, khi], w1d[1, :, hi_c], preferred_element_type=F32)
        hl[r, hi_c] = gelu(c.astype(BF16).astype(F32)).astype(BF16)

    def finish(q, i):
        r, l = pl.ds(i * MT, MT), pl.ds(q * QC, QC)
        half, c = divmod(q, NQ // 2)
        lanes = pl.multiple_of((1 - cx if half else cx) * C2 + c * QC, QC)
        z = zo[r, l] + jnp.dot(hl[r, hi_c], w2l[s, hi_c, l], preferred_element_type=F32)
        out[r, pl.ds(lanes, QC)] = (z + ry[q, r, :]).astype(BF16)

    few = pl.ds(0, NQ - 1)
    remote(zs.at[few], ry.at[few], zys.at[0], zyr.at[0], Y).wait_recv()
    for q in range(NQ - 1):
        for i in range(NP):
            finish(q, i)
    for i in range(NP):
        z_y(NQ - 1, i).wait_recv()
        finish(NQ - 1, i)
    sent(1).wait_send()
    remote(bo, bp, ws, wr.at[0], X).wait_send()
    remote(bo, bp, fs, fr.at[0], D).wait_send()
    remote(w1, ap, ys, yr.at[0], Y).wait_send()
    for c in (x_x, d_w1, d_w2, d_co, d_eo):
        c.wait_send()


def solution(mesh):
    data_spec = P(('dp', 'cx', 'cz'), 'cy')
    up_spec = P('cy', ('cz', 'cx'))
    down_spec = P('cz', ('cy', 'cx'))

    def local_mlp(x, w1, w2):
        R, K = x.shape
        B1 = w1.shape[1]
        WC = B1 // (NE + NL)
        EC, LC = NE * WC, NL * WC
        C2 = w2.shape[1]
        QC = 2 * C2 // NQ
        NX = NE + 2 * NL
        dma = pltpu.SemaphoreType.DMA
        any_spec = pl.BlockSpec(memory_space=pl.ANY)
        sds = jax.ShapeDtypeStruct
        outs = (
            pltpu.VMEM((R, K), BF16),
            sds(w1.shape, BF16),
            sds((NX, K, WC), BF16),
            sds((NX, K, WC), BF16),
            sds((K, LC), BF16),
            sds((K, LC), BF16),
            sds(w2.shape, BF16),
            sds((2, LC, C2), BF16),
            sds((2, LC, C2), BF16),
        )
        scratch = [
            pltpu.VMEM((2 * R, 2 * K), BF16),
            pltpu.VMEM((2 * R, 2 * EC), BF16),
            pltpu.VMEM((R, 2 * WC), BF16),
            pltpu.VMEM((2, 2 * K, 2 * WC), BF16),
            pltpu.VMEM((2, K, 2 * WC), BF16),
            pltpu.VMEM((2, 2 * EC, QC), BF16),
            pltpu.VMEM((2, 2 * WC, 2 * C2), BF16),
            pltpu.VMEM((NQ, R, QC), F32),
            pltpu.VMEM((NQ, R, QC), F32),
            pltpu.VMEM((R, 2 * C2), F32),
            dma((1,)), dma((2, 3)), dma((2,)), dma((2,)),
            dma((1,)), dma((1,)),
            dma, dma((NX + 1,)),
            dma, dma((4,)),
            dma((2,)), dma((1 + R // MT,)),
            dma((4,)), dma((4,)),
            dma, dma((2,)),
        ]
        return pl.pallas_call(
            kernel,
            out_shape=outs,
            in_specs=[any_spec] * 3,
            out_specs=(pl.BlockSpec(memory_space=pltpu.VMEM),) + (any_spec,) * (len(outs) - 1),
            scratch_shapes=scratch,
            compiler_params=pltpu.CompilerParams(
                collective_id=0, has_side_effects=True, vmem_limit_bytes=67043328 - 2 * R * K),
            name='mlp',
        )(x, w1, w2)[0]

    return jax.shard_map(local_mlp, mesh=mesh, in_specs=(data_spec, up_spec, down_spec), out_specs=data_spec, check_vma=False)
```

```python
import jax
import jax.numpy as jnp
from jax import lax
from jax.experimental import pallas as pl
from jax.experimental.pallas import tpu as pltpu
from jax.sharding import PartitionSpec as P

MESH = pl.DeviceIdType.MESH
F32, BF16 = jnp.float32, jnp.bfloat16
NE = 12
NL = 4
NA = 3
NQ = 4
MT = 512
PT = 128
SP = 128


def gelu(c):
    return c * (0.5 * (1.0 + jnp.tanh(0.7978845608028654 * (c + 0.044715 * (c * c * c)))))


def kernel(x, w1, w2, out, ap, bo, bp, co, cp, g0, eo, ep,
           xg, he, hl, w1s, w1d, w2s, w2l, zs, ry, zo,
           lsem, lw, lv, lu, xs, xr, ws, wr, ys, yr, zys, zyr,
           ds, dr, fs, fr):
    cz, cy, cx = lax.axis_index('cz'), lax.axis_index('cy'), lax.axis_index('cx')
    X, Y, D = {'cy': 1 - cy}, {'cz': 1 - cz}, {'cx': 1 - cx}
    XD = {'cy': 1 - cy, 'cx': 1 - cx}
    R, K = x.shape
    B1 = w1.shape[1]
    WC = B1 // (NE + NL)
    EC, LC = NE * WC, NL * WC
    C2 = w2.shape[1]
    QC = 2 * C2 // NQ

    def remote(src, dst, s, r, dev):
        return pltpu.make_async_remote_copy(src, dst, s, r, device_id=dev, device_id_type=MESH)

    barrier = pltpu.get_barrier_semaphore()
    for dev in (X, Y, D, XD):
        pl.semaphore_signal(barrier, inc=1, device_id=dev, device_id_type=MESH)
    pl.semaphore_wait(barrier, 4)

    own, oth = pl.ds(0, R), pl.ds(R, R)
    klo, khi = pl.ds(0, K), pl.ds(K, K)

    x_x = remote(x, xg.at[own, khi], xs.at[0], xr.at[0], X)
    y_x = remote(x, xg.at[oth, klo], ys, yr.at[0], Y)
    y_xf = remote(xg.at[own, khi], xg.at[oth, khi], ys, yr.at[1], Y)
    y_w1 = remote(w1.at[:, pl.ds(EC, LC)], co, ys, yr.at[2], Y)

    def y_w2(b):
        return remote(w2.at[pl.ds(b * B1 + EC, LC), :], eo.at[b], ys, yr.at[3], Y)

    l_x = pltpu.make_async_copy(x, xg.at[own, klo], lsem.at[0])
    d_w1 = remote(w1, ap, ds.at[0], dr.at[0], D)
    d_w2 = remote(w2, g0, ds.at[1], dr.at[1], D)
    d_co = remote(co, cp, ds.at[2], dr.at[2], D)
    d_eo = remote(eo, ep, ds.at[3], dr.at[3], D)

    def chunk(j):
        return pl.ds(j * WC if isinstance(j, int) else pl.multiple_of(j * WC, WC), WC)

    lo_c, hi_c = pl.ds(0, WC), pl.ds(WC, WC)

    def x_w1(j):
        return remote(w1.at[:, chunk(j)], bo.at[j], ws, wr.at[j], X)

    head, tail = pl.ds(0, K - SP), pl.ds(K - SP, SP)
    x_head = remote(w1.at[head, chunk(NE - 1)], w1d.at[0, head, lo_c], xs.at[1], wr.at[NE - 1], X)

    def x_tail(src, dev):
        return remote(src.at[tail, chunk(NE - 1)], w1d.at[0, tail, lo_c], xs.at[2], wr.at[NE + 2 * NL + 1], dev)

    def x_co(k):
        return remote(co.at[:, chunk(k)], bo.at[NE + NL + k], ws, wr.at[NE + NL + k], X)

    def turn(j):
        return j % 2 if isinstance(j, int) else lax.rem(j, 2)

    def f_w1(j):
        return remote(bo.at[j], bp.at[j], fs, fr.at[turn(j)], D)

    f_last = remote(w1d.at[0, :, lo_c], w1d.at[0, :, hi_c], fs, fr.at[turn(NE - 1)], D)
    HC = WC // 2

    def part(h, other=0):
        return pl.ds((2 * h + other) * HC, HC)

    def cols_last(h):
        return pl.ds((NL - 1) * WC + h * HC, HC)

    def x_part(h):
        return remote(co.at[:, cols_last(h)], w1d.at[1, :, part(h)], ws, wr.at[NE + 2 * NL - 1 + h], X)

    def f_part(h):
        return remote(w1d.at[1, :, part(h)], w1d.at[1, :, part(h, 1)], fs, fr.at[turn(NE + 2 * NL - 1 + h)], D)

    def quads(s, j, first, second):
        return [pltpu.make_async_copy(src, w1s.at[s, rows, pl.ds(c * WC, WC)], lw.at[s, i])
                for src, rows, c, i in (
                    (first, klo, 0, 0), (second, klo, 1, 0), (bo.at[j], khi, 0, 1), (bp.at[j], khi, 1, 2))]

    def wait_tiles(s, i):
        if i == 0:
            pltpu.make_async_copy(w1.at[:, pl.ds(0, 2 * WC)], w1s.at[s, klo, :], lw.at[s, 0]).wait()
        else:
            pltpu.make_async_copy(bo.at[0], w1s.at[s, khi, pl.ds((i - 1) * WC, WC)], lw.at[s, i]).wait()

    def wait_w2s(q):
        pltpu.make_async_copy(w2.at[pl.ds(0, 2 * EC), pl.ds(0, QC)], w2s.at[q % 2], lv.at[q % 2]).wait()

    def wait_w2l(s):
        pltpu.make_async_copy(w1.at[pl.ds(0, 2 * WC), pl.ds(0, 2 * C2)], w2l.at[s], lu.at[s]).wait()

    def quads_near(s, j):
        return quads(s, j, w1.at[:, chunk(j)], ap.at[:, chunk(j)])

    def quads_far(s, k):
        return quads(s, NE + NL + k, co.at[:, chunk(k)], cp.at[:, chunk(k)])

    base = (pl.multiple_of(cx * B1, B1), pl.multiple_of((1 - cx) * B1, B1))

    def loads(q):
        src, c = (w2, q) if q < NQ // 2 else (g0, q - NQ // 2)
        return [pltpu.make_async_copy(src.at[pl.ds(base[b], EC), pl.ds(c * QC, QC)],
                                      w2s.at[q % 2, pl.ds(b * EC, EC), :], lv.at[q % 2]) for b in range(2)]

    def late_near(s, k):
        got = []
        for b in range(2):
            rows = pl.ds(pl.multiple_of(base[b] + EC + k * WC, WC), WC)
            for c, src in enumerate((w2, g0)):
                got.append(pltpu.make_async_copy(
                    src.at[rows, :], w2l.at[s, pl.ds(b * WC, WC), pl.ds(c * C2, C2)], lu.at[s]))
        return got

    def late_far(s, k):
        got = []
        for b, blk in enumerate((cx, 1 - cx)):
            for c, src in enumerate((eo, ep)):
                got.append(pltpu.make_async_copy(
                    src.at[blk, chunk(k), :], w2l.at[s, pl.ds(b * WC, WC), pl.ds(c * C2, C2)], lu.at[s]))
        return got

    NP = R // MT

    def z_y(q, i, n=MT):
        rows = pl.ds(i * n if isinstance(i, int) else pl.multiple_of(i * n, n), n)
        return remote(zs.at[q, rows, :], ry.at[q, rows, :], zys.at[0 if q < 2 else 1], zyr.at[0 if q < NQ - 1 else 1 + i], Y)

    def layer1(dst, col, row0, rows, s, half):
        @pl.loop(0, rows // MT)
        def _(i):
            r = pl.multiple_of(i * MT, MT)
            c = jnp.dot(xg[pl.ds(row0 + r, MT), :], w1s[s, :, pl.ds(half * WC, WC)], preferred_element_type=F32)
            dst[pl.ds(row0 + r, MT), pl.ds(col, WC)] = gelu(c.astype(BF16).astype(F32)).astype(BF16)

    def layer1d(dst, col, row0, rows, s, half, i):
        lanes = pl.ds(half * WC, WC)

        @pl.loop(0, rows // MT)
        def _(n):
            r = pl.ds(pl.multiple_of(row0 + n * MT, MT), MT)
            c = (jnp.dot(xg[r, klo], w1s[s, klo, lanes], preferred_element_type=F32)
                 + jnp.dot(xg[r, khi], w1d[i, :, lanes], preferred_element_type=F32))
            dst[r, pl.ds(col, WC)] = gelu(c.astype(BF16).astype(F32)).astype(BF16)

    def step(j):
        s = lax.rem(j, 2)
        q = quads_near(s, j)
        q[0].start()
        q[1].start()
        x_w1(j).wait_recv()
        f_w1(j).start()
        q[2].start()
        wait_tiles(s, 0)
        wait_tiles(s, 1)
        layer1(he, col(j, 0), 0, R, s, 0)
        f_w1(j).wait_recv()
        q[3].start()
        wait_tiles(s, 2)
        layer1(he, col(j, 1), 0, R, s, 1)

    def col(j, half):
        return half * EC + j * WC if isinstance(j, int) else pl.multiple_of(half * EC + j * WC, WC)

    x_x.start()
    y_x.start()
    l_x.start()
    for j in range(NE - 1):
        x_w1(j).start()
    x_head.start()

    @pl.when(cx == 1)
    def _():
        x_tail(w1, X).start()

    d_w1.start()
    d_w2.start()
    for q in range(2):
        for c in loads(q):
            c.start()

    x_x.wait_recv()
    y_xf.start()
    y_w1.start()
    y_w2(0).start()
    y_w2(1).start()
    l_x.wait()
    d_w1.wait_recv()

    @pl.when(cx == 1)
    def _():
        x_tail(ap, XD).start()


    @pl.loop(0, NA)
    def _(j):
        step(j)

    y_x.wait_recv()
    y_xf.wait_recv()

    for n, j in enumerate((2, 1, 0)):
        if n == 2:
            for i in range(3):
                wait_tiles(0, i)
        for half in range(2):
            layer1(he, col(j, half), R, R, j % 2, half)
        if n == 0:
            for c in quads_near(0, 0):
                c.start()
        if n == 1:
            for c in quads_near(NA % 2, NA)[:2]:
                c.start()

    def early_second(j, s):
        wait_tiles(s, 2)
        layer1(he, col(j, 1), 0, 2 * R, s, 1)

    def early(lo, hi):
        @pl.loop(lo, hi)
        def _(j):
            s = lax.rem(j, 2)
            x_w1(j).wait_recv()
            f_w1(j).start()
            q = quads_near(s, j)
            q[2].start()
            if lo == NA:
                @pl.when(j > lo)
                def _():
                    early_second(j - 1, 1 - s)
            else:
                early_second(j - 1, 1 - s)
            for c in quads_near(1 - s, j + 1)[:2]:
                c.start()
            wait_tiles(s, 0)
            wait_tiles(s, 1)
            layer1(he, col(j, 0), 0, 2 * R, s, 0)
            f_w1(j).wait_recv()
            q[3].start()

    early(NA, 8)
    y_w1.wait_recv()
    for k in range(NL):
        x_w1(NE + k).start()
    for k in range(NL - 1):
        x_co(k).start()
    x_part(0).start()
    x_part(1).start()
    d_co.start()
    early(8, 9)

    def z_part(lo, hi, first):
        lanes = [pl.ds(b * EC + lo * WC, (hi - lo) * WC) for b in range(2)]

        @pl.loop(0, NP)
        def _(i):
            r = pl.multiple_of(i * MT, MT)
            z = sum(jnp.dot(he[pl.ds(R + r, MT), l], w2s[0, l, :], preferred_element_type=F32) for l in lanes)
            zs[0, pl.ds(r, MT), :] = z if first else zs[0, pl.ds(r, MT), :] + z

    d_w2.wait_recv()
    wait_w2s(0)
    wait_w2s(1)
    z_part(0, 8, True)
    early(9, NE - 2)
    early_second(NE - 3, (NE - 3) % 2)
    j, s = NE - 2, (NE - 2) % 2
    x_w1(j).wait_recv()
    f_w1(j).start()
    q = quads_near(s, j)
    q[2].start()
    for c in quads_near(1 - s, j + 1)[:2]:
        c.start()
    wait_tiles(s, 0)
    wait_tiles(s, 1)
    layer1(he, col(j, 0), 0, 2 * R, s, 0)
    f_w1(j).wait_recv()
    q[3].start()
    early_second(j, s)
    z_part(8, NE - 1, False)
    PC = EC - WC

    j, s = NE - 1, (NE - 1) % 2
    wait_tiles(s, 0)

    @pl.loop(0, NP)
    def _(i):
        r = pl.multiple_of(i * MT, MT)
        zo[pl.ds(r, MT), pl.ds(0, 2 * WC)] = jnp.dot(
            xg[pl.ds(R + r, MT), klo], w1s[s, klo, :], preferred_element_type=F32)

    x_head.wait_recv()
    x_tail(w1, X).wait_recv()
    f_last.start()

    @pl.loop(0, R // PT)
    def _(i):
        r = pl.multiple_of(i * PT, PT)

        def half_chunk(half):
            lanes = pl.ds(half * WC, WC)
            c = zo[pl.ds(r, PT), lanes] + jnp.dot(
                xg[pl.ds(R + r, PT), khi], w1d[0, :, lanes], preferred_element_type=F32)
            he[pl.ds(R + r, PT), pl.ds(col(j, half), WC)] = gelu(c.astype(BF16).astype(F32)).astype(BF16)

        half_chunk(0)

        @pl.when(i == 0)
        def _():
            f_last.wait_recv()

        half_chunk(1)
        zs[0, pl.ds(r, PT), :] = zs[0, pl.ds(r, PT), :] + (
            jnp.dot(he[pl.ds(R + r, PT), pl.ds(PC, WC)], w2s[0, pl.ds(PC, WC), :], preferred_element_type=F32)
            + jnp.dot(he[pl.ds(R + r, PT), pl.ds(EC + PC, WC)], w2s[0, pl.ds(EC + PC, WC), :], preferred_element_type=F32))
        z_y(0, i, PT).start()

    def z_other(q):
        @pl.loop(0, NP)
        def _(i):
            r = pl.multiple_of(i * MT, MT)
            zs[q, pl.ds(r, MT), :] = jnp.dot(he[pl.ds(R + r, MT), :], w2s[q % 2], preferred_element_type=F32)
            z_y(q, i).start()

    def z_own(q):
        @pl.loop(0, NP)
        def _(i):
            r = pl.ds(pl.multiple_of(i * MT, MT), MT)
            zo[r, pl.ds(q * QC, QC)] = jnp.dot(he[r, :], w2s[q % 2], preferred_element_type=F32)

    layer1d(he, col(j, 0), 0, R, s, 0, 0)
    layer1d(he, col(j, 1), 0, R, s, 1, 0)
    for q in range(NQ):
        if q:
            if q >= 2:
                wait_w2s(q)
            z_other(q)
        z_own(q)
        if q + 2 < NQ:
            for c in loads(q + 2):
                c.start()
        if q == 0:
            remote(eo, eo, ys, yr.at[3], Y).wait_recv()
            d_eo.start()

    d_co.wait_recv()
    d_eo.wait_recv()

    def second(s):
        wait_tiles(s, 2)
        layer1(hl, WC, 0, R, s, 1)
        layer2(s)

    def layer2(s):
        wait_w2l(s)

        @pl.loop(0, NP)
        def _(i):
            r = pl.ds(pl.multiple_of(i * MT, MT), MT)
            zo[r, :] = zo[r, :] + jnp.dot(hl[r, :], w2l[s], preferred_element_type=F32)

    def late_step(near, k, s, before):
        off = NE if near else NE + NL
        quad = quads_near(s, NE + k) if near else quads_far(s, k)
        for c in quad[:2] + (late_near(s, k) if near else late_far(s, k)):
            c.start()
        (x_w1(NE + k) if near else x_co(k)).wait_recv()
        f = f_w1(off + k)
        f.start()
        quad[2].start()
        before()
        wait_tiles(s, 0)
        wait_tiles(s, 1)
        layer1(hl, 0, 0, R, s, 0)
        f.wait_recv()
        quad[3].start()

    @pl.loop(0, NL)
    def _(k):
        s = lax.rem(NE + k, 2)

        def before():
            @pl.when(k > 0)
            def _():
                second(1 - s)

        late_step(True, k, s, before)

    @pl.loop(0, NL - 2)
    def _(k):
        s = lax.rem(NE + NL + k, 2)
        late_step(False, k, s, lambda: second(1 - s))

    k, s = NL - 2, (NE + 2 * NL - 2) % 2
    second(1 - s)
    late_step(False, k, s, lambda: None)
    s = 1 - s
    for h in range(2):
        for o, (wk, blk) in enumerate(((co, cx), (cp, 1 - cx))):
            pltpu.make_async_copy(wk.at[:, cols_last(h)], w1s.at[s, klo, part(h, o)], lw.at[s, 0]).start()
            for c, src in enumerate((eo, ep)):
                pltpu.make_async_copy(src.at[blk, cols_last(h), :],
                                      w2l.at[s, part(h, o), pl.ds(c * C2, C2)], lu.at[s]).start()

    def sent(n):
        two = pl.ds(2 * n, 2)
        return remote(zs.at[two], ry.at[two], zys.at[n], zyr.at[0], Y)

    wait_tiles(1 - s, 2)
    layer1(hl, WC, 0, R, 1 - s, 1)
    x_part(0).wait_recv()
    f_part(0).start()
    layer2(1 - s)
    sent(0).wait_send()
    wait_tiles(s, 0)
    f_part(0).wait_recv()
    layer1d(hl, 0, 0, R, s, 0, 1)
    wait_w2l(s)

    @pl.loop(0, NP)
    def _(i):
        r = pl.ds(pl.multiple_of(i * MT, MT), MT)
        zo[r, :] = zo[r, :] + jnp.dot(hl[r, lo_c], w2l[s, lo_c, :], preferred_element_type=F32)

    def take():
        x_part(1).wait_recv()
        f_part(1).start()

    pl.when(cx == 1)(take)

    @pl.loop(0, NP)
    def _(i):
        r = pl.ds(pl.multiple_of(i * MT, MT), MT)
        zs[0, r, :] = jnp.dot(xg[r, klo], w1s[s, klo, hi_c], preferred_element_type=F32)
        pl.when((cx == 0) & (i == 0))(take)

    f_part(1).wait_recv()
    @pl.loop(0, NP)
    def _(i):
        r = pl.ds(pl.multiple_of(i * MT, MT), MT)
        c = zs[0, r, :] + jnp.dot(xg[r, khi], w1d[1, :, hi_c], preferred_element_type=F32)
        hl[r, hi_c] = gelu(c.astype(BF16).astype(F32)).astype(BF16)

    def finish(q, i):
        r, l = pl.ds(i * MT, MT), pl.ds(q * QC, QC)
        half, c = divmod(q, NQ // 2)
        lanes = pl.multiple_of((1 - cx if half else cx) * C2 + c * QC, QC)
        z = zo[r, l] + jnp.dot(hl[r, hi_c], w2l[s, hi_c, l], preferred_element_type=F32)
        out[r, pl.ds(lanes, QC)] = (z + ry[q, r, :]).astype(BF16)

    few = pl.ds(0, NQ - 1)
    remote(zs.at[few], ry.at[few], zys.at[0], zyr.at[0], Y).wait_recv()
    for q in range(NQ - 1):
        for i in range(NP):
            finish(q, i)
    for i in range(NP):
        z_y(NQ - 1, i).wait_recv()
        finish(NQ - 1, i)
    sent(1).wait_send()
    most = pl.ds(0, NE + 2 * NL - 1)
    remote(bo.at[most], bp.at[most], ws, wr.at[0], X).wait_send()
    x_head.wait_send()

    @pl.when(cx == 1)
    def _():
        both = pl.ds(0, 2 * SP)
        remote(w1.at[both, chunk(0)], w1d.at[0, both, lo_c], xs.at[2], wr.at[0], X).wait_send()

    remote(bo, bp, fs, fr.at[0], D).wait_send()
    remote(w1, ap, ys, yr.at[0], Y).wait_send()
    for c in (x_x, d_w1, d_w2, d_co, d_eo):
        c.wait_send()


def solution(mesh):
    data_spec = P(('dp', 'cx', 'cz'), 'cy')
    up_spec = P('cy', ('cz', 'cx'))
    down_spec = P('cz', ('cy', 'cx'))

    def local_mlp(x, w1, w2):
        R, K = x.shape
        B1 = w1.shape[1]
        WC = B1 // (NE + NL)
        EC, LC = NE * WC, NL * WC
        C2 = w2.shape[1]
        QC = 2 * C2 // NQ
        NX = NE + 2 * NL
        dma = pltpu.SemaphoreType.DMA
        any_spec = pl.BlockSpec(memory_space=pl.ANY)
        sds = jax.ShapeDtypeStruct
        outs = (
            pltpu.VMEM((R, K), BF16),
            sds(w1.shape, BF16),
            sds((NX, K, WC), BF16),
            sds((NX, K, WC), BF16),
            sds((K, LC), BF16),
            sds((K, LC), BF16),
            sds(w2.shape, BF16),
            sds((2, LC, C2), BF16),
            sds((2, LC, C2), BF16),
        )
        scratch = [
            pltpu.VMEM((2 * R, 2 * K), BF16),
            pltpu.VMEM((2 * R, 2 * EC), BF16),
            pltpu.VMEM((R, 2 * WC), BF16),
            pltpu.VMEM((2, 2 * K, 2 * WC), BF16),
            pltpu.VMEM((2, K, 2 * WC), BF16),
            pltpu.VMEM((2, 2 * EC, QC), BF16),
            pltpu.VMEM((2, 2 * WC, 2 * C2), BF16),
            pltpu.VMEM((NQ, R, QC), F32),
            pltpu.VMEM((NQ, R, QC), F32),
            pltpu.VMEM((R, 2 * C2), F32),
            dma((1,)), dma((2, 3)), dma((2,)), dma((2,)),
            dma((3,)), dma((1,)),
            dma, dma((NX + 2,)),
            dma, dma((4,)),
            dma((2,)), dma((1 + R // MT,)),
            dma((4,)), dma((4,)),
            dma, dma((2,)),
        ]
        return pl.pallas_call(
            kernel,
            out_shape=outs,
            in_specs=[any_spec] * 3,
            out_specs=(pl.BlockSpec(memory_space=pltpu.VMEM),) + (any_spec,) * (len(outs) - 1),
            scratch_shapes=scratch,
            compiler_params=pltpu.CompilerParams(
                collective_id=0, has_side_effects=True, vmem_limit_bytes=67043328 - 2 * R * K),
            name='mlp',
        )(x, w1, w2)[0]

    return jax.shard_map(local_mlp, mesh=mesh, in_specs=(data_spec, up_spec, down_spec), out_specs=data_spec, check_vma=False)
```

```python
import jax
import jax.numpy as jnp
from jax import lax
from jax.experimental import pallas as pl
from jax.experimental.pallas import tpu as pltpu
from jax.sharding import PartitionSpec as P

MESH = pl.DeviceIdType.MESH
F32, BF16 = jnp.float32, jnp.bfloat16
NE = 12
NL = 4
NA = 3
NQ = 4
MT = 512
PT = 128
SP = 128


def gelu(c):
    return c * (0.5 * (1.0 + jnp.tanh(0.7978845608028654 * (c + 0.044715 * (c * c * c)))))


def kernel(x, w1, w2, out, ap, bo, bp, co, cp, g0, eo, ep,
           xg, he, hl, w1s, w1d, w2s, w2l, zs, ry, zo,
           lsem, lw, lv, lu, xs, xr, ws, wr, ys, yr, zys, zyr,
           ds, dr, fs, fr):
    cz, cy, cx = lax.axis_index('cz'), lax.axis_index('cy'), lax.axis_index('cx')
    X, Y, D = {'cy': 1 - cy}, {'cz': 1 - cz}, {'cx': 1 - cx}
    XD = {'cy': 1 - cy, 'cx': 1 - cx}
    R, K = x.shape
    B1 = w1.shape[1]
    WC = B1 // (NE + NL)
    EC, LC = NE * WC, NL * WC
    C2 = w2.shape[1]
    QC = 2 * C2 // NQ

    def remote(src, dst, s, r, dev):
        return pltpu.make_async_remote_copy(src, dst, s, r, device_id=dev, device_id_type=MESH)

    barrier = pltpu.get_barrier_semaphore()
    for dev in (X, Y, D, XD):
        pl.semaphore_signal(barrier, inc=1, device_id=dev, device_id_type=MESH)
    pl.semaphore_wait(barrier, 4)

    own, oth = pl.ds(0, R), pl.ds(R, R)
    klo, khi = pl.ds(0, K), pl.ds(K, K)

    x_x = remote(x, xg.at[own, khi], xs.at[0], xr.at[0], X)
    y_x = remote(x, xg.at[oth, klo], ys, yr.at[0], Y)
    y_xf = remote(xg.at[own, khi], xg.at[oth, khi], ys, yr.at[1], Y)
    y_w1 = remote(w1.at[:, pl.ds(EC, LC)], co, ys, yr.at[2], Y)

    def y_w2(b):
        return remote(w2.at[pl.ds(b * B1 + EC, LC), :], eo.at[b], ys, yr.at[3], Y)

    l_x = pltpu.make_async_copy(x, xg.at[own, klo], lsem.at[0])
    d_w1 = remote(w1, ap, ds.at[0], dr.at[0], D)
    d_w2 = remote(w2, g0, ds.at[1], dr.at[1], D)
    d_co = remote(co, cp, ds.at[2], dr.at[2], D)
    d_eo = remote(eo, ep, ds.at[3], dr.at[3], D)

    def chunk(j):
        return pl.ds(j * WC if isinstance(j, int) else pl.multiple_of(j * WC, WC), WC)

    lo_c, hi_c = pl.ds(0, WC), pl.ds(WC, WC)

    def x_w1(j):
        return remote(w1.at[:, chunk(j)], bo.at[j], ws, wr.at[j], X)

    head, tail = pl.ds(0, K - SP), pl.ds(K - SP, SP)
    x_head = remote(w1.at[head, chunk(NE - 1)], w1d.at[0, head, lo_c], xs.at[1], wr.at[NE - 1], X)

    def x_tail(src, dev):
        return remote(src.at[tail, chunk(NE - 1)], w1d.at[0, tail, lo_c], xs.at[2], wr.at[NE + 2 * NL + 1], dev)

    def x_co(k):
        return remote(co.at[:, chunk(k)], bo.at[NE + NL + k], ws, wr.at[NE + NL + k], X)

    def turn(j):
        return j % 2 if isinstance(j, int) else lax.rem(j, 2)

    def f_w1(j):
        return remote(bo.at[j], bp.at[j], fs, fr.at[turn(j)], D)

    f_last = remote(w1d.at[0, :, lo_c], w1d.at[0, :, hi_c], fs, fr.at[turn(NE - 1)], D)
    HC = WC // 2

    def part(h, other=0):
        return pl.ds((2 * h + other) * HC, HC)

    def cols_last(h):
        return pl.ds((NL - 1) * WC + h * HC, HC)

    def x_part(h):
        return remote(co.at[:, cols_last(h)], w1d.at[1, :, part(h)], ws, wr.at[NE + 2 * NL - 1 + h], X)

    def f_part(h):
        return remote(w1d.at[1, :, part(h)], w1d.at[1, :, part(h, 1)], fs, fr.at[turn(NE + 2 * NL - 1 + h)], D)

    def quads(s, j, first, second):
        return [pltpu.make_async_copy(src, w1s.at[s, rows, pl.ds(c * WC, WC)], lw.at[s, i])
                for src, rows, c, i in (
                    (first, klo, 0, 0), (second, klo, 1, 0), (bo.at[j], khi, 0, 1), (bp.at[j], khi, 1, 2))]

    def wait_tiles(s, i):
        if i == 0:
            pltpu.make_async_copy(w1.at[:, pl.ds(0, 2 * WC)], w1s.at[s, klo, :], lw.at[s, 0]).wait()
        else:
            pltpu.make_async_copy(bo.at[0], w1s.at[s, khi, pl.ds((i - 1) * WC, WC)], lw.at[s, i]).wait()

    def wait_w2s(q):
        pltpu.make_async_copy(w2.at[pl.ds(0, 2 * EC), pl.ds(0, QC)], w2s.at[q % 2], lv.at[q % 2]).wait()

    def wait_w2l(s):
        pltpu.make_async_copy(w1.at[pl.ds(0, 2 * WC), pl.ds(0, 2 * C2)], w2l.at[s], lu.at[s]).wait()

    def quads_near(s, j):
        return quads(s, j, w1.at[:, chunk(j)], ap.at[:, chunk(j)])

    def quads_far(s, k):
        return quads(s, NE + NL + k, co.at[:, chunk(k)], cp.at[:, chunk(k)])

    base = (pl.multiple_of(cx * B1, B1), pl.multiple_of((1 - cx) * B1, B1))

    def loads(q):
        src, c = (w2, q) if q < NQ // 2 else (g0, q - NQ // 2)
        return [pltpu.make_async_copy(src.at[pl.ds(base[b], EC), pl.ds(c * QC, QC)],
                                      w2s.at[q % 2, pl.ds(b * EC, EC), :], lv.at[q % 2]) for b in range(2)]

    def late_near(s, k):
        got = []
        for b in range(2):
            rows = pl.ds(pl.multiple_of(base[b] + EC + k * WC, WC), WC)
            for c, src in enumerate((w2, g0)):
                got.append(pltpu.make_async_copy(
                    src.at[rows, :], w2l.at[s, pl.ds(b * WC, WC), pl.ds(c * C2, C2)], lu.at[s]))
        return got

    def late_far(s, k):
        got = []
        for b, blk in enumerate((cx, 1 - cx)):
            for c, src in enumerate((eo, ep)):
                got.append(pltpu.make_async_copy(
                    src.at[blk, chunk(k), :], w2l.at[s, pl.ds(b * WC, WC), pl.ds(c * C2, C2)], lu.at[s]))
        return got

    NP = R // MT

    def z_y(q, i, n=MT):
        rows = pl.ds(i * n if isinstance(i, int) else pl.multiple_of(i * n, n), n)
        return remote(zs.at[q, rows, :], ry.at[q, rows, :], zys.at[0 if q < 2 else 1], zyr.at[0 if q < NQ - 1 else 1 + i], Y)

    def layer1(dst, col, row0, rows, s, half):
        @pl.loop(0, rows // MT)
        def _(i):
            r = pl.multiple_of(i * MT, MT)
            c = jnp.dot(xg[pl.ds(row0 + r, MT), :], w1s[s, :, pl.ds(half * WC, WC)], preferred_element_type=F32)
            dst[pl.ds(row0 + r, MT), pl.ds(col, WC)] = gelu(c.astype(BF16).astype(F32)).astype(BF16)

    def layer1d(dst, col, row0, rows, s, half, i):
        lanes = pl.ds(half * WC, WC)

        @pl.loop(0, rows // MT)
        def _(n):
            r = pl.ds(pl.multiple_of(row0 + n * MT, MT), MT)
            c = (jnp.dot(xg[r, klo], w1s[s, klo, lanes], preferred_element_type=F32)
                 + jnp.dot(xg[r, khi], w1d[i, :, lanes], preferred_element_type=F32))
            dst[r, pl.ds(col, WC)] = gelu(c.astype(BF16).astype(F32)).astype(BF16)

    def step(j):
        s = lax.rem(j, 2)
        q = quads_near(s, j)
        q[0].start()
        q[1].start()
        x_w1(j).wait_recv()
        f_w1(j).start()
        q[2].start()
        wait_tiles(s, 0)
        wait_tiles(s, 1)
        layer1(he, col(j, 0), 0, R, s, 0)
        f_w1(j).wait_recv()
        q[3].start()
        wait_tiles(s, 2)
        layer1(he, col(j, 1), 0, R, s, 1)

    def col(j, half):
        return half * EC + j * WC if isinstance(j, int) else pl.multiple_of(half * EC + j * WC, WC)

    x_x.start()
    y_x.start()
    l_x.start()
    for j in range(NE - 1):
        x_w1(j).start()
    x_head.start()

    @pl.when(cx == 1)
    def _():
        x_tail(w1, X).start()

    d_w1.start()
    d_w2.start()
    for q in range(2):
        for c in loads(q):
            c.start()

    x_x.wait_recv()
    y_xf.start()
    y_w1.start()
    y_w2(0).start()
    y_w2(1).start()
    l_x.wait()
    d_w1.wait_recv()

    @pl.when(cx == 1)
    def _():
        x_tail(ap, XD).start()


    @pl.loop(0, NA)
    def _(j):
        step(j)

    y_x.wait_recv()
    y_xf.wait_recv()

    for n, j in enumerate((2, 1, 0)):
        if n == 2:
            for i in range(3):
                wait_tiles(0, i)
        for half in range(2):
            layer1(he, col(j, half), R, R, j % 2, half)
        if n == 0:
            for c in quads_near(0, 0):
                c.start()
        if n == 1:
            for c in quads_near(NA % 2, NA)[:2]:
                c.start()

    def early_second(j, s):
        wait_tiles(s, 2)
        layer1(he, col(j, 1), 0, 2 * R, s, 1)

    def early(lo, hi):
        @pl.loop(lo, hi)
        def _(j):
            s = lax.rem(j, 2)
            x_w1(j).wait_recv()
            f_w1(j).start()
            q = quads_near(s, j)
            q[2].start()
            if lo == NA:
                @pl.when(j > lo)
                def _():
                    early_second(j - 1, 1 - s)
            else:
                early_second(j - 1, 1 - s)
            for c in quads_near(1 - s, j + 1)[:2]:
                c.start()
            wait_tiles(s, 0)
            wait_tiles(s, 1)
            layer1(he, col(j, 0), 0, 2 * R, s, 0)
            f_w1(j).wait_recv()
            q[3].start()

    early(NA, 8)
    y_w1.wait_recv()
    for k in range(NL):
        x_w1(NE + k).start()
    for k in range(NL - 1):
        x_co(k).start()
    x_part(0).start()
    x_part(1).start()
    d_co.start()
    early(8, 9)

    def z_part(lo, hi, first):
        lanes = [pl.ds(b * EC + lo * WC, (hi - lo) * WC) for b in range(2)]

        @pl.loop(0, NP)
        def _(i):
            r = pl.multiple_of(i * MT, MT)
            z = sum(jnp.dot(he[pl.ds(R + r, MT), l], w2s[0, l, :], preferred_element_type=F32) for l in lanes)
            zs[0, pl.ds(r, MT), :] = z if first else zs[0, pl.ds(r, MT), :] + z

    d_w2.wait_recv()
    wait_w2s(0)
    wait_w2s(1)
    z_part(0, 8, True)
    early(9, NE - 2)
    early_second(NE - 3, (NE - 3) % 2)
    j, s = NE - 2, (NE - 2) % 2
    q = quads_near(s, j)

    def theirs():
        f_w1(j).wait_recv()
        q[3].start()

    pl.when(cx == 0)(theirs)
    x_w1(j).wait_recv()
    f_w1(j).start()
    q[2].start()
    for c in quads_near(1 - s, j + 1)[:2]:
        c.start()
    wait_tiles(s, 0)

    def half_of(half):
        pltpu.make_async_copy(bo.at[0], w1s.at[s, khi, lo_c], lw.at[s, 1 + half]).wait()
        lanes = pl.ds(pl.multiple_of(half * WC, WC), WC)
        cols = pl.ds(pl.multiple_of(half * EC + j * WC, WC), WC)

        @pl.loop(0, 2 * NP)
        def _(i):
            r = pl.ds(pl.multiple_of(i * MT, MT), MT)
            c = jnp.dot(xg[r, :], w1s[s, :, lanes], preferred_element_type=F32)
            he[r, cols] = gelu(c.astype(BF16).astype(F32)).astype(BF16)

    half_of(1 - cx)
    pl.when(cx == 1)(theirs)
    half_of(cx)
    z_part(8, NE - 1, False)
    PC = EC - WC

    j, s = NE - 1, (NE - 1) % 2
    wait_tiles(s, 0)

    @pl.loop(0, NP)
    def _(i):
        r = pl.multiple_of(i * MT, MT)
        zo[pl.ds(r, MT), pl.ds(0, 2 * WC)] = jnp.dot(
            xg[pl.ds(R + r, MT), klo], w1s[s, klo, :], preferred_element_type=F32)

    x_head.wait_recv()
    x_tail(w1, X).wait_recv()
    f_last.start()

    @pl.loop(0, R // PT)
    def _(i):
        r = pl.multiple_of(i * PT, PT)

        def half_chunk(half):
            lanes = pl.ds(half * WC, WC)
            c = zo[pl.ds(r, PT), lanes] + jnp.dot(
                xg[pl.ds(R + r, PT), khi], w1d[0, :, lanes], preferred_element_type=F32)
            he[pl.ds(R + r, PT), pl.ds(col(j, half), WC)] = gelu(c.astype(BF16).astype(F32)).astype(BF16)

        half_chunk(0)

        @pl.when(i == 0)
        def _():
            f_last.wait_recv()

        half_chunk(1)
        zs[0, pl.ds(r, PT), :] = zs[0, pl.ds(r, PT), :] + (
            jnp.dot(he[pl.ds(R + r, PT), pl.ds(PC, WC)], w2s[0, pl.ds(PC, WC), :], preferred_element_type=F32)
            + jnp.dot(he[pl.ds(R + r, PT), pl.ds(EC + PC, WC)], w2s[0, pl.ds(EC + PC, WC), :], preferred_element_type=F32))
        z_y(0, i, PT).start()

    def z_other(q):
        @pl.loop(0, NP)
        def _(i):
            r = pl.multiple_of(i * MT, MT)
            zs[q, pl.ds(r, MT), :] = jnp.dot(he[pl.ds(R + r, MT), :], w2s[q % 2], preferred_element_type=F32)
            z_y(q, i).start()

    def z_own(q):
        @pl.loop(0, NP)
        def _(i):
            r = pl.ds(pl.multiple_of(i * MT, MT), MT)
            zo[r, pl.ds(q * QC, QC)] = jnp.dot(he[r, :], w2s[q % 2], preferred_element_type=F32)

    layer1d(he, col(j, 0), 0, R, s, 0, 0)
    layer1d(he, col(j, 1), 0, R, s, 1, 0)
    for q in range(NQ):
        if q:
            if q >= 2:
                wait_w2s(q)
            z_other(q)
        z_own(q)
        if q + 2 < NQ:
            for c in loads(q + 2):
                c.start()
        if q == 0:
            remote(eo, eo, ys, yr.at[3], Y).wait_recv()
            d_eo.start()

    d_co.wait_recv()
    d_eo.wait_recv()

    def second(s):
        wait_tiles(s, 2)
        layer1(hl, WC, 0, R, s, 1)
        layer2(s)

    def layer2(s):
        wait_w2l(s)

        @pl.loop(0, NP)
        def _(i):
            r = pl.ds(pl.multiple_of(i * MT, MT), MT)
            zo[r, :] = zo[r, :] + jnp.dot(hl[r, :], w2l[s], preferred_element_type=F32)

    def late_step(near, k, s, before):
        off = NE if near else NE + NL
        quad = quads_near(s, NE + k) if near else quads_far(s, k)
        for c in quad[:2] + (late_near(s, k) if near else late_far(s, k)):
            c.start()
        (x_w1(NE + k) if near else x_co(k)).wait_recv()
        f = f_w1(off + k)
        f.start()
        quad[2].start()
        before()
        wait_tiles(s, 0)
        wait_tiles(s, 1)
        layer1(hl, 0, 0, R, s, 0)
        f.wait_recv()
        quad[3].start()

    @pl.loop(0, NL)
    def _(k):
        s = lax.rem(NE + k, 2)

        def before():
            @pl.when(k > 0)
            def _():
                second(1 - s)

        late_step(True, k, s, before)

    @pl.loop(0, NL - 2)
    def _(k):
        s = lax.rem(NE + NL + k, 2)
        late_step(False, k, s, lambda: second(1 - s))

    k, s = NL - 2, (NE + 2 * NL - 2) % 2
    second(1 - s)
    late_step(False, k, s, lambda: None)
    s = 1 - s
    for h in range(2):
        for o, (wk, blk) in enumerate(((co, cx), (cp, 1 - cx))):
            pltpu.make_async_copy(wk.at[:, cols_last(h)], w1s.at[s, klo, part(h, o)], lw.at[s, 0]).start()
            for c, src in enumerate((eo, ep)):
                pltpu.make_async_copy(src.at[blk, cols_last(h), :],
                                      w2l.at[s, part(h, o), pl.ds(c * C2, C2)], lu.at[s]).start()

    def sent(n):
        two = pl.ds(2 * n, 2)
        return remote(zs.at[two], ry.at[two], zys.at[n], zyr.at[0], Y)

    wait_tiles(1 - s, 2)
    layer1(hl, WC, 0, R, 1 - s, 1)
    x_part(0).wait_recv()
    f_part(0).start()
    layer2(1 - s)
    sent(0).wait_send()
    wait_tiles(s, 0)
    f_part(0).wait_recv()
    layer1d(hl, 0, 0, R, s, 0, 1)
    wait_w2l(s)

    @pl.loop(0, NP)
    def _(i):
        r = pl.ds(pl.multiple_of(i * MT, MT), MT)
        zo[r, :] = zo[r, :] + jnp.dot(hl[r, lo_c], w2l[s, lo_c, :], preferred_element_type=F32)

    def take():
        x_part(1).wait_recv()
        f_part(1).start()

    pl.when(cx == 1)(take)

    @pl.loop(0, NP)
    def _(i):
        r = pl.ds(pl.multiple_of(i * MT, MT), MT)
        zs[0, r, :] = jnp.dot(xg[r, klo], w1s[s, klo, hi_c], preferred_element_type=F32)
        pl.when((cx == 0) & (i == 0))(take)

    f_part(1).wait_recv()
    @pl.loop(0, NP)
    def _(i):
        r = pl.ds(pl.multiple_of(i * MT, MT), MT)
        c = zs[0, r, :] + jnp.dot(xg[r, khi], w1d[1, :, hi_c], preferred_element_type=F32)
        hl[r, hi_c] = gelu(c.astype(BF16).astype(F32)).astype(BF16)

    def finish(q, i):
        r, l = pl.ds(i * MT, MT), pl.ds(q * QC, QC)
        half, c = divmod(q, NQ // 2)
        lanes = pl.multiple_of((1 - cx if half else cx) * C2 + c * QC, QC)
        z = zo[r, l] + jnp.dot(hl[r, hi_c], w2l[s, hi_c, l], preferred_element_type=F32)
        out[r, pl.ds(lanes, QC)] = (z + ry[q, r, :]).astype(BF16)

    few = pl.ds(0, NQ - 1)
    remote(zs.at[few], ry.at[few], zys.at[0], zyr.at[0], Y).wait_recv()
    for q in range(NQ - 1):
        for i in range(NP):
            finish(q, i)
    for i in range(NP):
        z_y(NQ - 1, i).wait_recv()
        finish(NQ - 1, i)
    sent(1).wait_send()
    most = pl.ds(0, NE + 2 * NL - 1)
    remote(bo.at[most], bp.at[most], ws, wr.at[0], X).wait_send()
    x_head.wait_send()

    @pl.when(cx == 1)
    def _():
        both = pl.ds(0, 2 * SP)
        remote(w1.at[both, chunk(0)], w1d.at[0, both, lo_c], xs.at[2], wr.at[0], X).wait_send()

    remote(bo, bp, fs, fr.at[0], D).wait_send()
    remote(w1, ap, ys, yr.at[0], Y).wait_send()
    for c in (x_x, d_w1, d_w2, d_co, d_eo):
        c.wait_send()


def solution(mesh):
    data_spec = P(('dp', 'cx', 'cz'), 'cy')
    up_spec = P('cy', ('cz', 'cx'))
    down_spec = P('cz', ('cy', 'cx'))

    def local_mlp(x, w1, w2):
        R, K = x.shape
        B1 = w1.shape[1]
        WC = B1 // (NE + NL)
        EC, LC = NE * WC, NL * WC
        C2 = w2.shape[1]
        QC = 2 * C2 // NQ
        NX = NE + 2 * NL
        dma = pltpu.SemaphoreType.DMA
        any_spec = pl.BlockSpec(memory_space=pl.ANY)
        sds = jax.ShapeDtypeStruct
        outs = (
            pltpu.VMEM((R, K), BF16),
            sds(w1.shape, BF16),
            sds((NX, K, WC), BF16),
            sds((NX, K, WC), BF16),
            sds((K, LC), BF16),
            sds((K, LC), BF16),
            sds(w2.shape, BF16),
            sds((2, LC, C2), BF16),
            sds((2, LC, C2), BF16),
        )
        scratch = [
            pltpu.VMEM((2 * R, 2 * K), BF16),
            pltpu.VMEM((2 * R, 2 * EC), BF16),
            pltpu.VMEM((R, 2 * WC), BF16),
            pltpu.VMEM((2, 2 * K, 2 * WC), BF16),
            pltpu.VMEM((2, K, 2 * WC), BF16),
            pltpu.VMEM((2, 2 * EC, QC), BF16),
            pltpu.VMEM((2, 2 * WC, 2 * C2), BF16),
            pltpu.VMEM((NQ, R, QC), F32),
            pltpu.VMEM((NQ, R, QC), F32),
            pltpu.VMEM((R, 2 * C2), F32),
            dma((1,)), dma((2, 3)), dma((2,)), dma((2,)),
            dma((3,)), dma((1,)),
            dma, dma((NX + 2,)),
            dma, dma((4,)),
            dma((2,)), dma((1 + R // MT,)),
            dma((4,)), dma((4,)),
            dma, dma((2,)),
        ]
        return pl.pallas_call(
            kernel,
            out_shape=outs,
            in_specs=[any_spec] * 3,
            out_specs=(pl.BlockSpec(memory_space=pltpu.VMEM),) + (any_spec,) * (len(outs) - 1),
            scratch_shapes=scratch,
            compiler_params=pltpu.CompilerParams(
                collective_id=0, has_side_effects=True, vmem_limit_bytes=67043328 - 2 * R * K),
            name='mlp',
        )(x, w1, w2)[0]

    return jax.shard_map(local_mlp, mesh=mesh, in_specs=(data_spec, up_spec, down_spec), out_specs=data_spec, check_vma=False)
```

```python
import jax
import jax.numpy as jnp
from jax import lax
from jax.experimental import pallas as pl
from jax.experimental.pallas import tpu as pltpu
from jax.sharding import PartitionSpec as P

MESH = pl.DeviceIdType.MESH
F32, BF16 = jnp.float32, jnp.bfloat16
NE = 12
NL = 4
NA = 3
NQ = 4
MT = 512
PT = 128


def gelu(c):
    return c * (0.5 * (1.0 + jnp.tanh(0.7978845608028654 * (c + 0.044715 * (c * c * c)))))


def kernel(x, w1, w2, out, ap, bo, bp, co, cp, g0, eo, ep,
           xg, he, hl, w1s, w1d, w2s, w2l, zs, ry, zo,
           lsem, lw, lv, lu, xs, xr, ws, wr, ys, yr, zys, zyr,
           ds, dr, fs, fr):
    cz, cy, cx = lax.axis_index('cz'), lax.axis_index('cy'), lax.axis_index('cx')
    X, Y, D = {'cy': 1 - cy}, {'cz': 1 - cz}, {'cx': 1 - cx}
    R, K = x.shape
    B1 = w1.shape[1]
    WC = B1 // (NE + NL)
    EC, LC = NE * WC, NL * WC
    C2 = w2.shape[1]
    QC = 2 * C2 // NQ

    def remote(src, dst, s, r, dev):
        return pltpu.make_async_remote_copy(src, dst, s, r, device_id=dev, device_id_type=MESH)

    barrier = pltpu.get_barrier_semaphore()
    for dev in (X, Y, D):
        pl.semaphore_signal(barrier, inc=1, device_id=dev, device_id_type=MESH)
    pl.semaphore_wait(barrier, 3)

    own, oth = pl.ds(0, R), pl.ds(R, R)
    klo, khi = pl.ds(0, K), pl.ds(K, K)

    x_x = remote(x, xg.at[own, khi], xs.at[0], xr.at[0], X)
    y_x = remote(x, xg.at[oth, klo], ys, yr.at[0], Y)
    y_xf = remote(xg.at[own, khi], xg.at[oth, khi], ys, yr.at[1], Y)
    y_w1 = remote(w1.at[:, pl.ds(EC, LC)], co, ys, yr.at[2], Y)

    def y_w2(b):
        return remote(w2.at[pl.ds(b * B1 + EC, LC), :], eo.at[b], ys, yr.at[3], Y)

    l_x = pltpu.make_async_copy(x, xg.at[own, klo], lsem.at[0])
    d_w1 = remote(w1, ap, ds.at[0], dr.at[0], D)
    d_w2 = remote(w2, g0, ds.at[1], dr.at[1], D)
    d_co = remote(co, cp, ds.at[2], dr.at[2], D)
    d_eo = remote(eo, ep, ds.at[3], dr.at[3], D)

    def chunk(j):
        return pl.ds(j * WC if isinstance(j, int) else pl.multiple_of(j * WC, WC), WC)

    lo_c, hi_c = pl.ds(0, WC), pl.ds(WC, WC)

    def x_w1(j):
        dst = w1d.at[0, :, lo_c] if isinstance(j, int) and j == NE - 1 else bo.at[j]
        return remote(w1.at[:, chunk(j)], dst, ws, wr.at[j], X)

    def x_co(k):
        return remote(co.at[:, chunk(k)], bo.at[NE + NL + k], ws, wr.at[NE + NL + k], X)

    def turn(j):
        return j % 2 if isinstance(j, int) else lax.rem(j, 2)

    def f_w1(j):
        return remote(bo.at[j], bp.at[j], fs, fr.at[turn(j)], D)

    f_last = remote(w1d.at[0, :, lo_c], w1d.at[0, :, hi_c], fs, fr.at[turn(NE - 1)], D)
    HC = WC // 2

    def part(h, other=0):
        return pl.ds((2 * h + other) * HC, HC)

    def cols_last(h):
        return pl.ds((NL - 1) * WC + h * HC, HC)

    def x_part(h):
        return remote(co.at[:, cols_last(h)], w1d.at[1, :, part(h)], ws, wr.at[NE + 2 * NL - 1 + h], X)

    def f_part(h):
        return remote(w1d.at[1, :, part(h)], w1d.at[1, :, part(h, 1)], fs, fr.at[turn(NE + 2 * NL - 1 + h)], D)

    def quads(s, j, first, second):
        return [pltpu.make_async_copy(src, w1s.at[s, rows, pl.ds(c * WC, WC)], lw.at[s, i])
                for src, rows, c, i in (
                    (first, klo, 0, 0), (second, klo, 1, 0), (bo.at[j], khi, 0, 1), (bp.at[j], khi, 1, 2))]

    def wait_tiles(s, i):
        if i == 0:
            pltpu.make_async_copy(w1.at[:, pl.ds(0, 2 * WC)], w1s.at[s, klo, :], lw.at[s, 0]).wait()
        else:
            pltpu.make_async_copy(bo.at[0], w1s.at[s, khi, pl.ds((i - 1) * WC, WC)], lw.at[s, i]).wait()

    def wait_w2s(q):
        pltpu.make_async_copy(w2.at[pl.ds(0, 2 * EC), pl.ds(0, QC)], w2s.at[q % 2], lv.at[q % 2]).wait()

    def wait_w2l(s):
        pltpu.make_async_copy(w1.at[pl.ds(0, 2 * WC), pl.ds(0, 2 * C2)], w2l.at[s], lu.at[s]).wait()

    def quads_near(s, j):
        return quads(s, j, w1.at[:, chunk(j)], ap.at[:, chunk(j)])

    def quads_far(s, k):
        return quads(s, NE + NL + k, co.at[:, chunk(k)], cp.at[:, chunk(k)])

    base = (pl.multiple_of(cx * B1, B1), pl.multiple_of((1 - cx) * B1, B1))

    def loads(q):
        src, c = (w2, q) if q < NQ // 2 else (g0, q - NQ // 2)
        return [pltpu.make_async_copy(src.at[pl.ds(base[b], EC), pl.ds(c * QC, QC)],
                                      w2s.at[q % 2, pl.ds(b * EC, EC), :], lv.at[q % 2]) for b in range(2)]

    def late_near(s, k):
        got = []
        for b in range(2):
            rows = pl.ds(pl.multiple_of(base[b] + EC + k * WC, WC), WC)
            for c, src in enumerate((w2, g0)):
                got.append(pltpu.make_async_copy(
                    src.at[rows, :], w2l.at[s, pl.ds(b * WC, WC), pl.ds(c * C2, C2)], lu.at[s]))
        return got

    def late_far(s, k):
        got = []
        for b, blk in enumerate((cx, 1 - cx)):
            for c, src in enumerate((eo, ep)):
                got.append(pltpu.make_async_copy(
                    src.at[blk, chunk(k), :], w2l.at[s, pl.ds(b * WC, WC), pl.ds(c * C2, C2)], lu.at[s]))
        return got

    NP = R // MT

    def z_y(q, i, n=MT):
        rows = pl.ds(i * n if isinstance(i, int) else pl.multiple_of(i * n, n), n)
        return remote(zs.at[q, rows, :], ry.at[q, rows, :], zys.at[0 if q < 2 else 1], zyr.at[0 if q < NQ - 1 else 1 + i], Y)

    def layer1(dst, col, row0, rows, s, half):
        @pl.loop(0, rows // MT)
        def _(i):
            r = pl.multiple_of(i * MT, MT)
            c = jnp.dot(xg[pl.ds(row0 + r, MT), :], w1s[s, :, pl.ds(half * WC, WC)], preferred_element_type=F32)
            dst[pl.ds(row0 + r, MT), pl.ds(col, WC)] = gelu(c.astype(BF16).astype(F32)).astype(BF16)

    def layer1d(dst, col, row0, rows, s, half, i):
        lanes = pl.ds(half * WC, WC)

        @pl.loop(0, rows // MT)
        def _(n):
            r = pl.ds(pl.multiple_of(row0 + n * MT, MT), MT)
            c = (jnp.dot(xg[r, klo], w1s[s, klo, lanes], preferred_element_type=F32)
                 + jnp.dot(xg[r, khi], w1d[i, :, lanes], preferred_element_type=F32))
            dst[r, pl.ds(col, WC)] = gelu(c.astype(BF16).astype(F32)).astype(BF16)

    def step(j):
        s = lax.rem(j, 2)
        q = quads_near(s, j)
        q[0].start()
        q[1].start()
        x_w1(j).wait_recv()
        f_w1(j).start()
        q[2].start()
        wait_tiles(s, 0)
        wait_tiles(s, 1)
        layer1(he, col(j, 0), 0, R, s, 0)
        f_w1(j).wait_recv()
        q[3].start()
        wait_tiles(s, 2)
        layer1(he, col(j, 1), 0, R, s, 1)

    def col(j, half):
        return half * EC + j * WC if isinstance(j, int) else pl.multiple_of(half * EC + j * WC, WC)

    x_x.start()
    y_x.start()
    l_x.start()
    for j in range(NE):
        x_w1(j).start()
    d_w1.start()
    d_w2.start()
    for q in range(2):
        for c in loads(q):
            c.start()

    x_x.wait_recv()
    y_xf.start()
    y_w1.start()
    y_w2(0).start()
    y_w2(1).start()
    l_x.wait()
    d_w1.wait_recv()

    @pl.loop(0, NA)
    def _(j):
        step(j)

    y_x.wait_recv()
    y_xf.wait_recv()

    for n, j in enumerate((2, 1, 0)):
        if n == 2:
            for i in range(3):
                wait_tiles(0, i)
        for half in range(2):
            layer1(he, col(j, half), R, R, j % 2, half)
        if n == 0:
            for c in quads_near(0, 0):
                c.start()
        if n == 1:
            for c in quads_near(NA % 2, NA)[:2]:
                c.start()

    def early_second(j, s):
        wait_tiles(s, 2)
        layer1(he, col(j, 1), 0, 2 * R, s, 1)

    def early(lo, hi):
        @pl.loop(lo, hi)
        def _(j):
            s = lax.rem(j, 2)
            x_w1(j).wait_recv()
            f_w1(j).start()
            q = quads_near(s, j)
            q[2].start()
            if lo == NA:
                @pl.when(j > lo)
                def _():
                    early_second(j - 1, 1 - s)
            else:
                early_second(j - 1, 1 - s)
            for c in quads_near(1 - s, j + 1)[:2]:
                c.start()
            wait_tiles(s, 0)
            wait_tiles(s, 1)
            layer1(he, col(j, 0), 0, 2 * R, s, 0)
            f_w1(j).wait_recv()
            q[3].start()

    early(NA, 8)
    y_w1.wait_recv()
    for k in range(NL):
        x_w1(NE + k).start()
    for k in range(NL - 1):
        x_co(k).start()
    x_part(0).start()
    x_part(1).start()
    d_co.start()
    early(8, 9)

    def z_part(lo, hi, first):
        lanes = [pl.ds(b * EC + lo * WC, (hi - lo) * WC) for b in range(2)]

        @pl.loop(0, NP)
        def _(i):
            r = pl.multiple_of(i * MT, MT)
            z = sum(jnp.dot(he[pl.ds(R + r, MT), l], w2s[0, l, :], preferred_element_type=F32) for l in lanes)
            zs[0, pl.ds(r, MT), :] = z if first else zs[0, pl.ds(r, MT), :] + z

    d_w2.wait_recv()
    wait_w2s(0)
    wait_w2s(1)
    z_part(0, 8, True)
    early(9, NE - 2)
    early_second(NE - 3, (NE - 3) % 2)
    j, s = NE - 2, (NE - 2) % 2
    q = quads_near(s, j)

    def theirs():
        f_w1(j).wait_recv()
        q[3].start()

    pl.when(cx == 0)(theirs)
    x_w1(j).wait_recv()
    f_w1(j).start()
    q[2].start()
    for c in quads_near(1 - s, j + 1)[:2]:
        c.start()
    wait_tiles(s, 0)

    def half_of(half):
        pltpu.make_async_copy(bo.at[0], w1s.at[s, khi, lo_c], lw.at[s, 1 + half]).wait()
        lanes = pl.ds(pl.multiple_of(half * WC, WC), WC)
        cols = pl.ds(pl.multiple_of(half * EC + j * WC, WC), WC)

        @pl.loop(0, 2 * NP)
        def _(i):
            r = pl.ds(pl.multiple_of(i * MT, MT), MT)
            c = jnp.dot(xg[r, :], w1s[s, :, lanes], preferred_element_type=F32)
            he[r, cols] = gelu(c.astype(BF16).astype(F32)).astype(BF16)

    half_of(1 - cx)
    pl.when(cx == 1)(theirs)
    half_of(cx)
    z_part(8, NE - 1, False)
    PC = EC - WC

    j, s = NE - 1, (NE - 1) % 2
    wait_tiles(s, 0)

    @pl.loop(0, NP)
    def _(i):
        r = pl.multiple_of(i * MT, MT)
        zo[pl.ds(r, MT), pl.ds(0, 2 * WC)] = jnp.dot(
            xg[pl.ds(R + r, MT), klo], w1s[s, klo, :], preferred_element_type=F32)

    x_w1(j).wait_recv()
    f_last.start()

    @pl.loop(0, R // PT)
    def _(i):
        r = pl.multiple_of(i * PT, PT)

        def half_chunk(half):
            lanes = pl.ds(half * WC, WC)
            c = zo[pl.ds(r, PT), lanes] + jnp.dot(
                xg[pl.ds(R + r, PT), khi], w1d[0, :, lanes], preferred_element_type=F32)
            he[pl.ds(R + r, PT), pl.ds(col(j, half), WC)] = gelu(c.astype(BF16).astype(F32)).astype(BF16)

        half_chunk(0)

        @pl.when(i == 0)
        def _():
            f_last.wait_recv()

        half_chunk(1)
        zs[0, pl.ds(r, PT), :] = zs[0, pl.ds(r, PT), :] + (
            jnp.dot(he[pl.ds(R + r, PT), pl.ds(PC, WC)], w2s[0, pl.ds(PC, WC), :], preferred_element_type=F32)
            + jnp.dot(he[pl.ds(R + r, PT), pl.ds(EC + PC, WC)], w2s[0, pl.ds(EC + PC, WC), :], preferred_element_type=F32))
        z_y(0, i, PT).start()

    def z_other(q):
        @pl.loop(0, NP)
        def _(i):
            r = pl.multiple_of(i * MT, MT)
            zs[q, pl.ds(r, MT), :] = jnp.dot(he[pl.ds(R + r, MT), :], w2s[q % 2], preferred_element_type=F32)
            z_y(q, i).start()

    def z_own(q):
        @pl.loop(0, NP)
        def _(i):
            r = pl.ds(pl.multiple_of(i * MT, MT), MT)
            zo[r, pl.ds(q * QC, QC)] = jnp.dot(he[r, :], w2s[q % 2], preferred_element_type=F32)

    layer1d(he, col(j, 0), 0, R, s, 0, 0)
    layer1d(he, col(j, 1), 0, R, s, 1, 0)
    for q in range(NQ):
        if q:
            if q >= 2:
                wait_w2s(q)
            z_other(q)
        z_own(q)
        if q + 2 < NQ:
            for c in loads(q + 2):
                c.start()
        if q == 0:
            remote(eo, eo, ys, yr.at[3], Y).wait_recv()
            d_eo.start()

    d_co.wait_recv()
    d_eo.wait_recv()

    def second(s):
        wait_tiles(s, 2)
        layer1(hl, WC, 0, R, s, 1)
        layer2(s)

    def layer2(s):
        wait_w2l(s)

        @pl.loop(0, NP)
        def _(i):
            r = pl.ds(pl.multiple_of(i * MT, MT), MT)
            zo[r, :] = zo[r, :] + jnp.dot(hl[r, :], w2l[s], preferred_element_type=F32)

    def late_step(near, k, s, before):
        off = NE if near else NE + NL
        quad = quads_near(s, NE + k) if near else quads_far(s, k)
        for c in quad[:2] + (late_near(s, k) if near else late_far(s, k)):
            c.start()
        (x_w1(NE + k) if near else x_co(k)).wait_recv()
        f = f_w1(off + k)
        f.start()
        quad[2].start()
        before()
        wait_tiles(s, 0)
        wait_tiles(s, 1)
        layer1(hl, 0, 0, R, s, 0)
        f.wait_recv()
        quad[3].start()

    @pl.loop(0, NL)
    def _(k):
        s = lax.rem(NE + k, 2)

        def before():
            @pl.when(k > 0)
            def _():
                second(1 - s)

        late_step(True, k, s, before)

    @pl.loop(0, NL - 2)
    def _(k):
        s = lax.rem(NE + NL + k, 2)
        late_step(False, k, s, lambda: second(1 - s))

    k, s = NL - 2, (NE + 2 * NL - 2) % 2
    second(1 - s)
    late_step(False, k, s, lambda: None)
    s = 1 - s
    for h in range(2):
        for o, (wk, blk) in enumerate(((co, cx), (cp, 1 - cx))):
            pltpu.make_async_copy(wk.at[:, cols_last(h)], w1s.at[s, klo, part(h, o)], lw.at[s, 0]).start()
            for c, src in enumerate((eo, ep)):
                pltpu.make_async_copy(src.at[blk, cols_last(h), :],
                                      w2l.at[s, part(h, o), pl.ds(c * C2, C2)], lu.at[s]).start()

    def sent(n):
        two = pl.ds(2 * n, 2)
        return remote(zs.at[two], ry.at[two], zys.at[n], zyr.at[0], Y)

    wait_tiles(1 - s, 2)
    layer1(hl, WC, 0, R, 1 - s, 1)
    x_part(0).wait_recv()
    f_part(0).start()
    layer2(1 - s)
    sent(0).wait_send()
    wait_tiles(s, 0)
    f_part(0).wait_recv()
    layer1d(hl, 0, 0, R, s, 0, 1)
    wait_w2l(s)

    @pl.loop(0, NP)
    def _(i):
        r = pl.ds(pl.multiple_of(i * MT, MT), MT)
        zo[r, :] = zo[r, :] + jnp.dot(hl[r, lo_c], w2l[s, lo_c, :], preferred_element_type=F32)

    def take():
        x_part(1).wait_recv()
        f_part(1).start()

    pl.when(cx == 1)(take)

    @pl.loop(0, NP)
    def _(i):
        r = pl.ds(pl.multiple_of(i * MT, MT), MT)
        zs[0, r, :] = jnp.dot(xg[r, klo], w1s[s, klo, hi_c], preferred_element_type=F32)
        pl.when((cx == 0) & (i == 0))(take)

    f_part(1).wait_recv()
    @pl.loop(0, NP)
    def _(i):
        r = pl.ds(pl.multiple_of(i * MT, MT), MT)
        c = zs[0, r, :] + jnp.dot(xg[r, khi], w1d[1, :, hi_c], preferred_element_type=F32)
        hl[r, hi_c] = gelu(c.astype(BF16).astype(F32)).astype(BF16)

    def finish(q, i):
        r, l = pl.ds(i * MT, MT), pl.ds(q * QC, QC)
        half, c = divmod(q, NQ // 2)
        lanes = pl.multiple_of((1 - cx if half else cx) * C2 + c * QC, QC)
        z = zo[r, l] + jnp.dot(hl[r, hi_c], w2l[s, hi_c, l], preferred_element_type=F32)
        out[r, pl.ds(lanes, QC)] = (z + ry[q, r, :]).astype(BF16)

    few = pl.ds(0, NQ - 1)
    remote(zs.at[few], ry.at[few], zys.at[0], zyr.at[0], Y).wait_recv()
    for q in range(NQ - 1):
        for i in range(NP):
            finish(q, i)
    for i in range(NP):
        z_y(NQ - 1, i).wait_recv()
        finish(NQ - 1, i)
    sent(1).wait_send()
    remote(bo, bp, ws, wr.at[0], X).wait_send()
    remote(bo, bp, fs, fr.at[0], D).wait_send()
    remote(w1, ap, ys, yr.at[0], Y).wait_send()
    for c in (x_x, d_w1, d_w2, d_co, d_eo):
        c.wait_send()


def solution(mesh):
    data_spec = P(('dp', 'cx', 'cz'), 'cy')
    up_spec = P('cy', ('cz', 'cx'))
    down_spec = P('cz', ('cy', 'cx'))

    def local_mlp(x, w1, w2):
        R, K = x.shape
        B1 = w1.shape[1]
        WC = B1 // (NE + NL)
        EC, LC = NE * WC, NL * WC
        C2 = w2.shape[1]
        QC = 2 * C2 // NQ
        NX = NE + 2 * NL
        dma = pltpu.SemaphoreType.DMA
        any_spec = pl.BlockSpec(memory_space=pl.ANY)
        sds = jax.ShapeDtypeStruct
        outs = (
            pltpu.VMEM((R, K), BF16),
            sds(w1.shape, BF16),
            sds((NX, K, WC), BF16),
            sds((NX, K, WC), BF16),
            sds((K, LC), BF16),
            sds((K, LC), BF16),
            sds(w2.shape, BF16),
            sds((2, LC, C2), BF16),
            sds((2, LC, C2), BF16),
        )
        scratch = [
            pltpu.VMEM((2 * R, 2 * K), BF16),
            pltpu.VMEM((2 * R, 2 * EC), BF16),
            pltpu.VMEM((R, 2 * WC), BF16),
            pltpu.VMEM((2, 2 * K, 2 * WC), BF16),
            pltpu.VMEM((2, K, 2 * WC), BF16),
            pltpu.VMEM((2, 2 * EC, QC), BF16),
            pltpu.VMEM((2, 2 * WC, 2 * C2), BF16),
            pltpu.VMEM((NQ, R, QC), F32),
            pltpu.VMEM((NQ, R, QC), F32),
            pltpu.VMEM((R, 2 * C2), F32),
            dma((1,)), dma((2, 3)), dma((2,)), dma((2,)),
            dma((1,)), dma((1,)),
            dma, dma((NX + 1,)),
            dma, dma((4,)),
            dma((2,)), dma((1 + R // MT,)),
            dma((4,)), dma((4,)),
            dma, dma((2,)),
        ]
        return pl.pallas_call(
            kernel,
            out_shape=outs,
            in_specs=[any_spec] * 3,
            out_specs=(pl.BlockSpec(memory_space=pltpu.VMEM),) + (any_spec,) * (len(outs) - 1),
            scratch_shapes=scratch,
            compiler_params=pltpu.CompilerParams(
                collective_id=0, has_side_effects=True, vmem_limit_bytes=67043328 - 2 * R * K),
            name='mlp',
        )(x, w1, w2)[0]

    return jax.shard_map(local_mlp, mesh=mesh, in_specs=(data_spec, up_spec, down_spec), out_specs=data_spec, check_vma=False)
```

```python
import jax
import jax.numpy as jnp
from jax import lax
from jax.experimental import pallas as pl
from jax.experimental.pallas import tpu as pltpu
from jax.sharding import PartitionSpec as P

MESH = pl.DeviceIdType.MESH
F32, BF16 = jnp.float32, jnp.bfloat16
NE = 12
NL = 4
NA = 3
NQ = 4
MT = 512
PT = 128
ET = 256


def gelu(c):
    return c * (0.5 * (1.0 + jnp.tanh(0.7978845608028654 * (c + 0.044715 * (c * c * c)))))


def kernel(x, w1, w2, out, ap, bo, bp, co, cp, g0, eo, ep,
           xg, he, hl, w1s, w1d, w2s, w2l, zs, ry, zo,
           lsem, lw, lv, lu, xs, xr, ws, wr, ys, yr, zys, zyr,
           ds, dr, fs, fr):
    cz, cy, cx = lax.axis_index('cz'), lax.axis_index('cy'), lax.axis_index('cx')
    X, Y, D = {'cy': 1 - cy}, {'cz': 1 - cz}, {'cx': 1 - cx}
    R, K = x.shape
    B1 = w1.shape[1]
    WC = B1 // (NE + NL)
    EC, LC = NE * WC, NL * WC
    C2 = w2.shape[1]
    QC = 2 * C2 // NQ

    def remote(src, dst, s, r, dev):
        return pltpu.make_async_remote_copy(src, dst, s, r, device_id=dev, device_id_type=MESH)

    barrier = pltpu.get_barrier_semaphore()
    for dev in (X, Y, D):
        pl.semaphore_signal(barrier, inc=1, device_id=dev, device_id_type=MESH)
    pl.semaphore_wait(barrier, 3)

    own, oth = pl.ds(0, R), pl.ds(R, R)
    klo, khi = pl.ds(0, K), pl.ds(K, K)

    x_x = remote(x, xg.at[own, khi], xs.at[0], xr.at[0], X)
    y_x = remote(x, xg.at[oth, klo], ys, yr.at[0], Y)
    y_xf = remote(xg.at[own, khi], xg.at[oth, khi], ys, yr.at[1], Y)
    y_w1 = remote(w1.at[:, pl.ds(EC, LC)], co, ys, yr.at[2], Y)

    def y_w2(b):
        return remote(w2.at[pl.ds(b * B1 + EC, LC), :], eo.at[b], ys, yr.at[3], Y)

    l_x = pltpu.make_async_copy(x, xg.at[own, klo], lsem.at[0])
    d_w1 = remote(w1, ap, ds.at[0], dr.at[0], D)
    d_w2 = remote(w2, g0, ds.at[1], dr.at[1], D)
    d_co = remote(co, cp, ds.at[2], dr.at[2], D)
    d_eo = remote(eo, ep, ds.at[3], dr.at[3], D)

    def chunk(j):
        return pl.ds(j * WC if isinstance(j, int) else pl.multiple_of(j * WC, WC), WC)

    lo_c, hi_c = pl.ds(0, WC), pl.ds(WC, WC)

    def x_w1(j):
        dst = w1d.at[0, :, lo_c] if isinstance(j, int) and j == NE - 1 else bo.at[j]
        return remote(w1.at[:, chunk(j)], dst, ws, wr.at[j], X)

    def x_co(k):
        return remote(co.at[:, chunk(k)], bo.at[NE + NL + k], ws, wr.at[NE + NL + k], X)

    def turn(j):
        return j % 2 if isinstance(j, int) else lax.rem(j, 2)

    def f_w1(j):
        return remote(bo.at[j], bp.at[j], fs, fr.at[turn(j)], D)

    f_last = remote(w1d.at[0, :, lo_c], w1d.at[0, :, hi_c], fs, fr.at[turn(NE - 1)], D)
    HC = WC // 2

    def part(h, other=0):
        return pl.ds((2 * h + other) * HC, HC)

    def cols_last(h):
        return pl.ds((NL - 1) * WC + h * HC, HC)

    def x_part(h):
        return remote(co.at[:, cols_last(h)], w1d.at[1, :, part(h)], ws, wr.at[NE + 2 * NL - 1 + h], X)

    def f_part(h):
        return remote(w1d.at[1, :, part(h)], w1d.at[1, :, part(h, 1)], fs, fr.at[turn(NE + 2 * NL - 1 + h)], D)

    def quads(s, j, first, second):
        return [pltpu.make_async_copy(src, w1s.at[s, rows, pl.ds(c * WC, WC)], lw.at[s, i])
                for src, rows, c, i in (
                    (first, klo, 0, 0), (second, klo, 1, 0), (bo.at[j], khi, 0, 1), (bp.at[j], khi, 1, 2))]

    def wait_tiles(s, i):
        if i == 0:
            pltpu.make_async_copy(w1.at[:, pl.ds(0, 2 * WC)], w1s.at[s, klo, :], lw.at[s, 0]).wait()
        else:
            pltpu.make_async_copy(bo.at[0], w1s.at[s, khi, pl.ds((i - 1) * WC, WC)], lw.at[s, i]).wait()

    def wait_w2s(q):
        pltpu.make_async_copy(w2.at[pl.ds(0, 2 * EC), pl.ds(0, QC)], w2s.at[q % 2], lv.at[q % 2]).wait()

    def wait_w2l(s):
        pltpu.make_async_copy(w1.at[pl.ds(0, 2 * WC), pl.ds(0, 2 * C2)], w2l.at[s], lu.at[s]).wait()

    def quads_near(s, j):
        return quads(s, j, w1.at[:, chunk(j)], ap.at[:, chunk(j)])

    def quads_far(s, k):
        return quads(s, NE + NL + k, co.at[:, chunk(k)], cp.at[:, chunk(k)])

    base = (pl.multiple_of(cx * B1, B1), pl.multiple_of((1 - cx) * B1, B1))

    def loads(q):
        src, c = (w2, q) if q < NQ // 2 else (g0, q - NQ // 2)
        return [pltpu.make_async_copy(src.at[pl.ds(base[b], EC), pl.ds(c * QC, QC)],
                                      w2s.at[q % 2, pl.ds(b * EC, EC), :], lv.at[q % 2]) for b in range(2)]

    def late_near(s, k):
        got = []
        for b in range(2):
            rows = pl.ds(pl.multiple_of(base[b] + EC + k * WC, WC), WC)
            for c, src in enumerate((w2, g0)):
                got.append(pltpu.make_async_copy(
                    src.at[rows, :], w2l.at[s, pl.ds(b * WC, WC), pl.ds(c * C2, C2)], lu.at[s]))
        return got

    def late_far(s, k):
        got = []
        for b, blk in enumerate((cx, 1 - cx)):
            for c, src in enumerate((eo, ep)):
                got.append(pltpu.make_async_copy(
                    src.at[blk, chunk(k), :], w2l.at[s, pl.ds(b * WC, WC), pl.ds(c * C2, C2)], lu.at[s]))
        return got

    NP = R // MT

    def z_y(q, i, n=MT):
        rows = pl.ds(i * n if isinstance(i, int) else pl.multiple_of(i * n, n), n)
        return remote(zs.at[q, rows, :], ry.at[q, rows, :], zys.at[0 if q < 2 else 1], zyr.at[0 if q < NQ - 1 else 1 + i], Y)

    def layer1(dst, col, row0, rows, s, half):
        @pl.loop(0, rows // MT)
        def _(i):
            r = pl.multiple_of(i * MT, MT)
            c = jnp.dot(xg[pl.ds(row0 + r, MT), :], w1s[s, :, pl.ds(half * WC, WC)], preferred_element_type=F32)
            dst[pl.ds(row0 + r, MT), pl.ds(col, WC)] = gelu(c.astype(BF16).astype(F32)).astype(BF16)

    def layer1d(dst, col, row0, rows, s, half, i):
        lanes = pl.ds(half * WC, WC)

        @pl.loop(0, rows // MT)
        def _(n):
            r = pl.ds(pl.multiple_of(row0 + n * MT, MT), MT)
            c = (jnp.dot(xg[r, klo], w1s[s, klo, lanes], preferred_element_type=F32)
                 + jnp.dot(xg[r, khi], w1d[i, :, lanes], preferred_element_type=F32))
            dst[r, pl.ds(col, WC)] = gelu(c.astype(BF16).astype(F32)).astype(BF16)

    def step(j):
        s = lax.rem(j, 2)
        q = quads_near(s, j)
        q[0].start()
        q[1].start()
        x_w1(j).wait_recv()
        f_w1(j).start()
        q[2].start()
        wait_tiles(s, 0)
        wait_tiles(s, 1)
        layer1(he, col(j, 0), 0, R, s, 0)
        f_w1(j).wait_recv()
        q[3].start()
        wait_tiles(s, 2)
        layer1(he, col(j, 1), 0, R, s, 1)

    def col(j, half):
        return half * EC + j * WC if isinstance(j, int) else pl.multiple_of(half * EC + j * WC, WC)

    x_x.start()
    y_x.start()
    l_x.start()
    for j in range(NE):
        x_w1(j).start()
    d_w1.start()
    d_w2.start()
    for q in range(2):
        for c in loads(q):
            c.start()

    x_x.wait_recv()
    y_xf.start()
    y_w1.start()
    y_w2(0).start()
    y_w2(1).start()
    l_x.wait()
    d_w1.wait_recv()

    @pl.loop(0, NA)
    def _(j):
        step(j)

    y_x.wait_recv()
    y_xf.wait_recv()

    for n, j in enumerate((2, 1, 0)):
        if n == 2:
            for i in range(3):
                wait_tiles(0, i)
        for half in range(2):
            layer1(he, col(j, half), R, R, j % 2, half)
        if n == 0:
            for c in quads_near(0, 0):
                c.start()
        if n == 1:
            for c in quads_near(NA % 2, NA)[:2]:
                c.start()

    def early_second(j, s):
        wait_tiles(s, 2)
        layer1(he, col(j, 1), 0, 2 * R, s, 1)

    def early(lo, hi):
        @pl.loop(lo, hi)
        def _(j):
            s = lax.rem(j, 2)
            x_w1(j).wait_recv()
            f_w1(j).start()
            q = quads_near(s, j)
            q[2].start()
            if lo == NA:
                @pl.when(j > lo)
                def _():
                    early_second(j - 1, 1 - s)
            else:
                early_second(j - 1, 1 - s)
            for c in quads_near(1 - s, j + 1)[:2]:
                c.start()
            wait_tiles(s, 0)
            wait_tiles(s, 1)
            layer1(he, col(j, 0), 0, 2 * R, s, 0)
            f_w1(j).wait_recv()
            q[3].start()

    early(NA, 8)
    y_w1.wait_recv()
    for k in range(NL):
        x_w1(NE + k).start()
    for k in range(NL - 1):
        x_co(k).start()
    x_part(0).start()
    x_part(1).start()
    d_co.start()
    early(8, 9)

    def z_part(lo, hi, first):
        lanes = [pl.ds(b * EC + lo * WC, (hi - lo) * WC) for b in range(2)]

        @pl.loop(0, NP)
        def _(i):
            r = pl.multiple_of(i * MT, MT)
            z = sum(jnp.dot(he[pl.ds(R + r, MT), l], w2s[0, l, :], preferred_element_type=F32) for l in lanes)
            zs[0, pl.ds(r, MT), :] = z if first else zs[0, pl.ds(r, MT), :] + z

    d_w2.wait_recv()
    wait_w2s(0)
    wait_w2s(1)
    z_part(0, 8, True)
    early(9, NE - 2)
    early_second(NE - 3, (NE - 3) % 2)
    j, s = NE - 2, (NE - 2) % 2
    q = quads_near(s, j)

    def theirs():
        f_w1(j).wait_recv()
        q[3].start()

    pl.when(cx == 0)(theirs)
    x_w1(j).wait_recv()
    f_w1(j).start()
    q[2].start()
    for c in quads_near(1 - s, j + 1)[:2]:
        c.start()
    wait_tiles(s, 0)

    def half_of(half):
        pltpu.make_async_copy(bo.at[0], w1s.at[s, khi, lo_c], lw.at[s, 1 + half]).wait()
        lanes = pl.ds(pl.multiple_of(half * WC, WC), WC)
        cols = pl.ds(pl.multiple_of(half * EC + j * WC, WC), WC)

        @pl.loop(0, 2 * NP)
        def _(i):
            r = pl.ds(pl.multiple_of(i * MT, MT), MT)
            c = jnp.dot(xg[r, :], w1s[s, :, lanes], preferred_element_type=F32)
            he[r, cols] = gelu(c.astype(BF16).astype(F32)).astype(BF16)

    half_of(1 - cx)
    pl.when(cx == 1)(theirs)
    half_of(cx)
    z_part(8, NE - 1, False)
    PC = EC - WC

    j, s = NE - 1, (NE - 1) % 2
    wait_tiles(s, 0)

    @pl.loop(0, NP)
    def _(i):
        r = pl.multiple_of(i * MT, MT)
        zo[pl.ds(r, MT), pl.ds(0, 2 * WC)] = jnp.dot(
            xg[pl.ds(R + r, MT), klo], w1s[s, klo, :], preferred_element_type=F32)

    x_w1(j).wait_recv()
    f_last.start()

    @pl.loop(0, R // PT)
    def _(i):
        r = pl.multiple_of(i * PT, PT)

        def half_chunk(half):
            lanes = pl.ds(half * WC, WC)
            c = zo[pl.ds(r, PT), lanes] + jnp.dot(
                xg[pl.ds(R + r, PT), khi], w1d[0, :, lanes], preferred_element_type=F32)
            he[pl.ds(R + r, PT), pl.ds(col(j, half), WC)] = gelu(c.astype(BF16).astype(F32)).astype(BF16)

        half_chunk(0)

        @pl.when(i == 0)
        def _():
            f_last.wait_recv()

        half_chunk(1)
        zs[0, pl.ds(r, PT), :] = zs[0, pl.ds(r, PT), :] + (
            jnp.dot(he[pl.ds(R + r, PT), pl.ds(PC, WC)], w2s[0, pl.ds(PC, WC), :], preferred_element_type=F32)
            + jnp.dot(he[pl.ds(R + r, PT), pl.ds(EC + PC, WC)], w2s[0, pl.ds(EC + PC, WC), :], preferred_element_type=F32))
        z_y(0, i, PT).start()

    def z_other(q):
        @pl.loop(0, NP)
        def _(i):
            r = pl.multiple_of(i * MT, MT)
            zs[q, pl.ds(r, MT), :] = jnp.dot(he[pl.ds(R + r, MT), :], w2s[q % 2], preferred_element_type=F32)
            if q < NQ - 1:
                z_y(q, i).start()
            else:
                for n in range(MT // ET):
                    z_y(q, i * (MT // ET) + n, ET).start()

    def z_own(q):
        @pl.loop(0, NP)
        def _(i):
            r = pl.ds(pl.multiple_of(i * MT, MT), MT)
            zo[r, pl.ds(q * QC, QC)] = jnp.dot(he[r, :], w2s[q % 2], preferred_element_type=F32)

    layer1d(he, col(j, 0), 0, R, s, 0, 0)
    layer1d(he, col(j, 1), 0, R, s, 1, 0)
    for q in range(NQ):
        if q:
            if q >= 2:
                wait_w2s(q)
            z_other(q)
        z_own(q)
        if q + 2 < NQ:
            for c in loads(q + 2):
                c.start()
        if q == 0:
            remote(eo, eo, ys, yr.at[3], Y).wait_recv()
            d_eo.start()

    d_co.wait_recv()
    d_eo.wait_recv()

    def second(s):
        wait_tiles(s, 2)
        layer1(hl, WC, 0, R, s, 1)
        layer2(s)

    def layer2(s):
        wait_w2l(s)

        @pl.loop(0, NP)
        def _(i):
            r = pl.ds(pl.multiple_of(i * MT, MT), MT)
            zo[r, :] = zo[r, :] + jnp.dot(hl[r, :], w2l[s], preferred_element_type=F32)

    def late_step(near, k, s, before):
        off = NE if near else NE + NL
        quad = quads_near(s, NE + k) if near else quads_far(s, k)
        for c in quad[:2] + (late_near(s, k) if near else late_far(s, k)):
            c.start()
        (x_w1(NE + k) if near else x_co(k)).wait_recv()
        f = f_w1(off + k)
        f.start()
        quad[2].start()
        before()
        wait_tiles(s, 0)
        wait_tiles(s, 1)
        layer1(hl, 0, 0, R, s, 0)
        f.wait_recv()
        quad[3].start()

    @pl.loop(0, NL)
    def _(k):
        s = lax.rem(NE + k, 2)

        def before():
            @pl.when(k > 0)
            def _():
                second(1 - s)

        late_step(True, k, s, before)

    @pl.loop(0, NL - 2)
    def _(k):
        s = lax.rem(NE + NL + k, 2)
        late_step(False, k, s, lambda: second(1 - s))

    k, s = NL - 2, (NE + 2 * NL - 2) % 2
    second(1 - s)
    late_step(False, k, s, lambda: None)
    s = 1 - s
    for h in range(2):
        for o, (wk, blk) in enumerate(((co, cx), (cp, 1 - cx))):
            pltpu.make_async_copy(wk.at[:, cols_last(h)], w1s.at[s, klo, part(h, o)], lw.at[s, 0]).start()
            for c, src in enumerate((eo, ep)):
                pltpu.make_async_copy(src.at[blk, cols_last(h), :],
                                      w2l.at[s, part(h, o), pl.ds(c * C2, C2)], lu.at[s]).start()

    def sent(n):
        two = pl.ds(2 * n, 2)
        return remote(zs.at[two], ry.at[two], zys.at[n], zyr.at[0], Y)

    wait_tiles(1 - s, 2)
    layer1(hl, WC, 0, R, 1 - s, 1)
    x_part(0).wait_recv()
    f_part(0).start()
    layer2(1 - s)
    sent(0).wait_send()
    wait_tiles(s, 0)
    f_part(0).wait_recv()
    layer1d(hl, 0, 0, R, s, 0, 1)
    wait_w2l(s)

    @pl.loop(0, NP)
    def _(i):
        r = pl.ds(pl.multiple_of(i * MT, MT), MT)
        zo[r, :] = zo[r, :] + jnp.dot(hl[r, lo_c], w2l[s, lo_c, :], preferred_element_type=F32)

    def take():
        x_part(1).wait_recv()
        f_part(1).start()

    pl.when(cx == 1)(take)

    @pl.loop(0, NP)
    def _(i):
        r = pl.ds(pl.multiple_of(i * MT, MT), MT)
        zs[0, r, :] = jnp.dot(xg[r, klo], w1s[s, klo, hi_c], preferred_element_type=F32)
        pl.when((cx == 0) & (i == 0))(take)

    f_part(1).wait_recv()
    @pl.loop(0, NP)
    def _(i):
        r = pl.ds(pl.multiple_of(i * MT, MT), MT)
        c = zs[0, r, :] + jnp.dot(xg[r, khi], w1d[1, :, hi_c], preferred_element_type=F32)
        hl[r, hi_c] = gelu(c.astype(BF16).astype(F32)).astype(BF16)

    def finish(q, i, n=MT):
        r, l = pl.ds(i * n, n), pl.ds(q * QC, QC)
        half, c = divmod(q, NQ // 2)
        lanes = pl.multiple_of((1 - cx if half else cx) * C2 + c * QC, QC)
        z = zo[r, l] + jnp.dot(hl[r, hi_c], w2l[s, hi_c, l], preferred_element_type=F32)
        out[r, pl.ds(lanes, QC)] = (z + ry[q, r, :]).astype(BF16)

    few = pl.ds(0, NQ - 1)
    remote(zs.at[few], ry.at[few], zys.at[0], zyr.at[0], Y).wait_recv()
    for q in range(NQ - 1):
        for i in range(NP):
            finish(q, i)
    for i in range(R // ET):
        z_y(NQ - 1, i, ET).wait_recv()
        finish(NQ - 1, i, ET)
    sent(1).wait_send()
    remote(bo, bp, ws, wr.at[0], X).wait_send()
    remote(bo, bp, fs, fr.at[0], D).wait_send()
    remote(w1, ap, ys, yr.at[0], Y).wait_send()
    for c in (x_x, d_w1, d_w2, d_co, d_eo):
        c.wait_send()


def solution(mesh):
    data_spec = P(('dp', 'cx', 'cz'), 'cy')
    up_spec = P('cy', ('cz', 'cx'))
    down_spec = P('cz', ('cy', 'cx'))

    def local_mlp(x, w1, w2):
        R, K = x.shape
        B1 = w1.shape[1]
        WC = B1 // (NE + NL)
        EC, LC = NE * WC, NL * WC
        C2 = w2.shape[1]
        QC = 2 * C2 // NQ
        NX = NE + 2 * NL
        dma = pltpu.SemaphoreType.DMA
        any_spec = pl.BlockSpec(memory_space=pl.ANY)
        sds = jax.ShapeDtypeStruct
        outs = (
            pltpu.VMEM((R, K), BF16),
            sds(w1.shape, BF16),
            sds((NX, K, WC), BF16),
            sds((NX, K, WC), BF16),
            sds((K, LC), BF16),
            sds((K, LC), BF16),
            sds(w2.shape, BF16),
            sds((2, LC, C2), BF16),
            sds((2, LC, C2), BF16),
        )
        scratch = [
            pltpu.VMEM((2 * R, 2 * K), BF16),
            pltpu.VMEM((2 * R, 2 * EC), BF16),
            pltpu.VMEM((R, 2 * WC), BF16),
            pltpu.VMEM((2, 2 * K, 2 * WC), BF16),
            pltpu.VMEM((2, K, 2 * WC), BF16),
            pltpu.VMEM((2, 2 * EC, QC), BF16),
            pltpu.VMEM((2, 2 * WC, 2 * C2), BF16),
            pltpu.VMEM((NQ, R, QC), F32),
            pltpu.VMEM((NQ, R, QC), F32),
            pltpu.VMEM((R, 2 * C2), F32),
            dma((1,)), dma((2, 3)), dma((2,)), dma((2,)),
            dma((1,)), dma((1,)),
            dma, dma((NX + 1,)),
            dma, dma((4,)),
            dma((2,)), dma((1 + R // ET,)),
            dma((4,)), dma((4,)),
            dma, dma((2,)),
        ]
        return pl.pallas_call(
            kernel,
            out_shape=outs,
            in_specs=[any_spec] * 3,
            out_specs=(pl.BlockSpec(memory_space=pltpu.VMEM),) + (any_spec,) * (len(outs) - 1),
            scratch_shapes=scratch,
            compiler_params=pltpu.CompilerParams(
                collective_id=0, has_side_effects=True, vmem_limit_bytes=67043328 - 2 * R * K),
            name='mlp',
        )(x, w1, w2)[0]

    return jax.shard_map(local_mlp, mesh=mesh, in_specs=(data_spec, up_spec, down_spec), out_specs=data_spec, check_vma=False)
```

```python
import jax
import jax.numpy as jnp
from jax import lax
from jax.experimental import pallas as pl
from jax.experimental.pallas import tpu as pltpu
from jax.sharding import PartitionSpec as P

MESH = pl.DeviceIdType.MESH
F32, BF16 = jnp.float32, jnp.bfloat16
NE = 12
NL = 4
NA = 3
NQ = 4
MT = 512
PT = 128
ET = 256


def gelu(c):
    return c * (0.5 * (1.0 + jnp.tanh(0.7978845608028654 * (c + 0.044715 * (c * c * c)))))


def kernel(x, w1, w2, out, ap, bo, bp, co, cp, g0, eo, ep,
           xg, he, hl, w1s, w1d, w2s, w2l, zs, ry, zo,
           lsem, lw, lv, lu, xs, xr, ws, wr, ys, yr, zys, zyr,
           ds, dr, fs, fr):
    cz, cy, cx = lax.axis_index('cz'), lax.axis_index('cy'), lax.axis_index('cx')
    X, Y, D = {'cy': 1 - cy}, {'cz': 1 - cz}, {'cx': 1 - cx}
    R, K = x.shape
    B1 = w1.shape[1]
    WC = B1 // (NE + NL)
    EC, LC = NE * WC, NL * WC
    C2 = w2.shape[1]
    QC = 2 * C2 // NQ

    def remote(src, dst, s, r, dev):
        return pltpu.make_async_remote_copy(src, dst, s, r, device_id=dev, device_id_type=MESH)

    barrier = pltpu.get_barrier_semaphore()
    for dev in (X, Y, D):
        pl.semaphore_signal(barrier, inc=1, device_id=dev, device_id_type=MESH)
    pl.semaphore_wait(barrier, 3)

    own, oth = pl.ds(0, R), pl.ds(R, R)
    klo, khi = pl.ds(0, K), pl.ds(K, K)

    x_x = remote(x, xg.at[own, khi], xs.at[0], xr.at[0], X)
    y_x = remote(x, xg.at[oth, klo], ys, yr.at[0], Y)
    y_xf = remote(xg.at[own, khi], xg.at[oth, khi], ys, yr.at[1], Y)
    y_w1 = remote(w1.at[:, pl.ds(EC, LC)], co, ys, yr.at[2], Y)

    def y_w2(b):
        return remote(w2.at[pl.ds(b * B1 + EC, LC), :], eo.at[b], ys, yr.at[3], Y)

    l_x = pltpu.make_async_copy(x, xg.at[own, klo], lsem.at[0])
    d_w1 = remote(w1, ap, ds.at[0], dr.at[0], D)
    d_w2 = remote(w2, g0, ds.at[1], dr.at[1], D)
    d_co = remote(co, cp, ds.at[2], dr.at[2], D)
    d_eo = remote(eo, ep, ds.at[3], dr.at[3], D)

    def chunk(j):
        return pl.ds(j * WC if isinstance(j, int) else pl.multiple_of(j * WC, WC), WC)

    lo_c, hi_c = pl.ds(0, WC), pl.ds(WC, WC)

    def x_w1(j):
        dst = w1d.at[0, :, lo_c] if isinstance(j, int) and j == NE - 1 else bo.at[j]
        return remote(w1.at[:, chunk(j)], dst, ws, wr.at[j], X)

    def x_co(k):
        return remote(co.at[:, chunk(k)], bo.at[NE + NL + k], ws, wr.at[NE + NL + k], X)

    def turn(j):
        return j % 2 if isinstance(j, int) else lax.rem(j, 2)

    def f_w1(j):
        return remote(bo.at[j], bp.at[j], fs, fr.at[turn(j)], D)

    f_last = remote(w1d.at[0, :, lo_c], w1d.at[0, :, hi_c], fs, fr.at[turn(NE - 1)], D)
    HC = WC // 2

    def part(h, other=0):
        return pl.ds((2 * h + other) * HC, HC)

    def cols_last(h):
        return pl.ds((NL - 1) * WC + h * HC, HC)

    def x_part(h):
        return remote(co.at[:, cols_last(h)], w1d.at[1, :, part(h)], ws, wr.at[NE + 2 * NL - 1 + h], X)

    def f_part(h):
        return remote(w1d.at[1, :, part(h)], w1d.at[1, :, part(h, 1)], fs, fr.at[turn(NE + 2 * NL - 1 + h)], D)

    def quads(s, j, first, second):
        return [pltpu.make_async_copy(src, w1s.at[s, rows, pl.ds(c * WC, WC)], lw.at[s, i])
                for src, rows, c, i in (
                    (first, klo, 0, 0), (second, klo, 1, 0), (bo.at[j], khi, 0, 1), (bp.at[j], khi, 1, 2))]

    def wait_tiles(s, i):
        if i == 0:
            pltpu.make_async_copy(w1.at[:, pl.ds(0, 2 * WC)], w1s.at[s, klo, :], lw.at[s, 0]).wait()
        else:
            pltpu.make_async_copy(bo.at[0], w1s.at[s, khi, pl.ds((i - 1) * WC, WC)], lw.at[s, i]).wait()

    def wait_w2s(q):
        pltpu.make_async_copy(w2.at[pl.ds(0, 2 * EC), pl.ds(0, QC)], w2s.at[q % 2], lv.at[q % 2]).wait()

    def wait_w2l(s):
        pltpu.make_async_copy(w1.at[pl.ds(0, 2 * WC), pl.ds(0, 2 * C2)], w2l.at[s], lu.at[s]).wait()

    def quads_near(s, j):
        return quads(s, j, w1.at[:, chunk(j)], ap.at[:, chunk(j)])

    def quads_far(s, k):
        return quads(s, NE + NL + k, co.at[:, chunk(k)], cp.at[:, chunk(k)])

    base = (pl.multiple_of(cx * B1, B1), pl.multiple_of((1 - cx) * B1, B1))

    def loads(q):
        src, c = (w2, q) if q < NQ // 2 else (g0, q - NQ // 2)
        return [pltpu.make_async_copy(src.at[pl.ds(base[b], EC), pl.ds(c * QC, QC)],
                                      w2s.at[q % 2, pl.ds(b * EC, EC), :], lv.at[q % 2]) for b in range(2)]

    def late_near(s, k):
        got = []
        for b in range(2):
            rows = pl.ds(pl.multiple_of(base[b] + EC + k * WC, WC), WC)
            for c, src in enumerate((w2, g0)):
                got.append(pltpu.make_async_copy(
                    src.at[rows, :], w2l.at[s, pl.ds(b * WC, WC), pl.ds(c * C2, C2)], lu.at[s]))
        return got

    def late_far(s, k):
        got = []
        for b, blk in enumerate((cx, 1 - cx)):
            for c, src in enumerate((eo, ep)):
                got.append(pltpu.make_async_copy(
                    src.at[blk, chunk(k), :], w2l.at[s, pl.ds(b * WC, WC), pl.ds(c * C2, C2)], lu.at[s]))
        return got

    NP = R // MT

    def z_y(q, i, n=MT):
        rows = pl.ds(i * n if isinstance(i, int) else pl.multiple_of(i * n, n), n)
        return remote(zs.at[q, rows, :], ry.at[q, rows, :], zys.at[0 if q < 2 else 1], zyr.at[0 if q < NQ - 1 else 1 + i], Y)

    def layer1(dst, col, row0, rows, s, half):
        @pl.loop(0, rows // MT)
        def _(i):
            r = pl.multiple_of(i * MT, MT)
            c = jnp.dot(xg[pl.ds(row0 + r, MT), :], w1s[s, :, pl.ds(half * WC, WC)], preferred_element_type=F32)
            dst[pl.ds(row0 + r, MT), pl.ds(col, WC)] = gelu(c.astype(BF16).astype(F32)).astype(BF16)

    def layer1d(dst, col, row0, rows, s, half, i):
        lanes = pl.ds(half * WC, WC)

        @pl.loop(0, rows // MT)
        def _(n):
            r = pl.ds(pl.multiple_of(row0 + n * MT, MT), MT)
            c = (jnp.dot(xg[r, klo], w1s[s, klo, lanes], preferred_element_type=F32)
                 + jnp.dot(xg[r, khi], w1d[i, :, lanes], preferred_element_type=F32))
            dst[r, pl.ds(col, WC)] = gelu(c.astype(BF16).astype(F32)).astype(BF16)

    def step(j):
        s = lax.rem(j, 2)
        q = quads_near(s, j)
        q[0].start()
        q[1].start()
        x_w1(j).wait_recv()
        f_w1(j).start()
        q[2].start()
        wait_tiles(s, 0)
        wait_tiles(s, 1)
        layer1(he, col(j, 0), 0, R, s, 0)
        f_w1(j).wait_recv()
        q[3].start()
        wait_tiles(s, 2)
        layer1(he, col(j, 1), 0, R, s, 1)

    def col(j, half):
        return half * EC + j * WC if isinstance(j, int) else pl.multiple_of(half * EC + j * WC, WC)

    x_x.start()
    y_x.start()
    l_x.start()
    for j in range(NE):
        x_w1(j).start()
    d_w1.start()
    d_w2.start()
    for q in range(2):
        for c in loads(q):
            c.start()

    x_x.wait_recv()
    y_xf.start()
    y_w1.start()
    y_w2(0).start()
    y_w2(1).start()
    l_x.wait()
    d_w1.wait_recv()

    @pl.loop(0, NA)
    def _(j):
        step(j)

    y_x.wait_recv()
    y_xf.wait_recv()

    for n, j in enumerate((2, 1, 0)):
        if n == 2:
            for i in range(3):
                wait_tiles(0, i)
        for half in range(2):
            layer1(he, col(j, half), R, R, j % 2, half)
        if n == 0:
            for c in quads_near(0, 0):
                c.start()
        if n == 1:
            for c in quads_near(NA % 2, NA)[:2]:
                c.start()

    def early_second(j, s):
        wait_tiles(s, 2)
        layer1(he, col(j, 1), 0, 2 * R, s, 1)

    def early(lo, hi):
        @pl.loop(lo, hi)
        def _(j):
            s = lax.rem(j, 2)
            x_w1(j).wait_recv()
            f_w1(j).start()
            q = quads_near(s, j)
            q[2].start()
            if lo == NA:
                @pl.when(j > lo)
                def _():
                    early_second(j - 1, 1 - s)
            else:
                early_second(j - 1, 1 - s)
            for c in quads_near(1 - s, j + 1)[:2]:
                c.start()
            wait_tiles(s, 0)
            wait_tiles(s, 1)
            layer1(he, col(j, 0), 0, 2 * R, s, 0)
            f_w1(j).wait_recv()
            q[3].start()

    early(NA, 8)
    y_w1.wait_recv()
    for k in range(NL):
        x_w1(NE + k).start()
    for k in range(NL - 1):
        x_co(k).start()
    x_part(0).start()
    x_part(1).start()
    d_co.start()
    early(8, 9)

    def z_part(lo, hi, first):
        lanes = [pl.ds(b * EC + lo * WC, (hi - lo) * WC) for b in range(2)]

        @pl.loop(0, NP)
        def _(i):
            r = pl.multiple_of(i * MT, MT)
            z = sum(jnp.dot(he[pl.ds(R + r, MT), l], w2s[0, l, :], preferred_element_type=F32) for l in lanes)
            zs[0, pl.ds(r, MT), :] = z if first else zs[0, pl.ds(r, MT), :] + z

    d_w2.wait_recv()
    wait_w2s(0)
    wait_w2s(1)
    z_part(0, 8, True)
    early(9, NE - 2)
    early_second(NE - 3, (NE - 3) % 2)
    j, s = NE - 2, (NE - 2) % 2
    q = quads_near(s, j)

    def theirs():
        f_w1(j).wait_recv()
        q[3].start()

    pl.when(cx == 0)(theirs)
    x_w1(j).wait_recv()
    f_w1(j).start()
    q[2].start()
    for c in quads_near(1 - s, j + 1)[:2]:
        c.start()
    wait_tiles(s, 0)

    def half_of(half):
        pltpu.make_async_copy(bo.at[0], w1s.at[s, khi, lo_c], lw.at[s, 1 + half]).wait()
        lanes = pl.ds(pl.multiple_of(half * WC, WC), WC)
        cols = pl.ds(pl.multiple_of(half * EC + j * WC, WC), WC)

        @pl.loop(0, 2 * NP)
        def _(i):
            r = pl.ds(pl.multiple_of(i * MT, MT), MT)
            c = jnp.dot(xg[r, :], w1s[s, :, lanes], preferred_element_type=F32)
            he[r, cols] = gelu(c.astype(BF16).astype(F32)).astype(BF16)

    half_of(1 - cx)
    pl.when(cx == 1)(theirs)
    half_of(cx)
    z_part(8, NE - 1, False)
    PC = EC - WC

    j, s = NE - 1, (NE - 1) % 2
    wait_tiles(s, 0)

    @pl.loop(0, NP)
    def _(i):
        r = pl.multiple_of(i * MT, MT)
        zo[pl.ds(r, MT), pl.ds(0, 2 * WC)] = jnp.dot(
            xg[pl.ds(R + r, MT), klo], w1s[s, klo, :], preferred_element_type=F32)

    x_w1(j).wait_recv()
    f_last.start()

    @pl.loop(0, R // PT)
    def _(i):
        r = pl.multiple_of(i * PT, PT)

        def half_chunk(half):
            lanes = pl.ds(half * WC, WC)
            c = zo[pl.ds(r, PT), lanes] + jnp.dot(
                xg[pl.ds(R + r, PT), khi], w1d[0, :, lanes], preferred_element_type=F32)
            he[pl.ds(R + r, PT), pl.ds(col(j, half), WC)] = gelu(c.astype(BF16).astype(F32)).astype(BF16)

        half_chunk(0)

        @pl.when(i == 0)
        def _():
            f_last.wait_recv()

        half_chunk(1)
        zs[0, pl.ds(r, PT), :] = zs[0, pl.ds(r, PT), :] + (
            jnp.dot(he[pl.ds(R + r, PT), pl.ds(PC, WC)], w2s[0, pl.ds(PC, WC), :], preferred_element_type=F32)
            + jnp.dot(he[pl.ds(R + r, PT), pl.ds(EC + PC, WC)], w2s[0, pl.ds(EC + PC, WC), :], preferred_element_type=F32))
        z_y(0, i, PT).start()

    def z_other(q):
        @pl.loop(0, NP)
        def _(i):
            r = pl.multiple_of(i * MT, MT)
            zs[q, pl.ds(r, MT), :] = jnp.dot(he[pl.ds(R + r, MT), :], w2s[q % 2], preferred_element_type=F32)
            if q < NQ - 1:
                z_y(q, i).start()
            else:
                for n in range(MT // ET):
                    z_y(q, i * (MT // ET) + n, ET).start()

    def z_own(q):
        @pl.loop(0, NP)
        def _(i):
            r = pl.ds(pl.multiple_of(i * MT, MT), MT)
            zo[r, pl.ds(q * QC, QC)] = jnp.dot(he[r, :], w2s[q % 2], preferred_element_type=F32)

    layer1d(he, col(j, 0), 0, R, s, 0, 0)
    layer1d(he, col(j, 1), 0, R, s, 1, 0)
    for q in range(NQ):
        if q:
            if q >= 2:
                wait_w2s(q)
            z_other(q)
        z_own(q)
        if q + 2 < NQ:
            for c in loads(q + 2):
                c.start()
        if q == 0:
            remote(eo, eo, ys, yr.at[3], Y).wait_recv()
            d_eo.start()

    d_co.wait_recv()
    d_eo.wait_recv()

    def second(s):
        wait_tiles(s, 2)
        layer1(hl, WC, 0, R, s, 1)
        layer2(s)

    def layer2(s):
        wait_w2l(s)

        @pl.loop(0, NP)
        def _(i):
            r = pl.ds(pl.multiple_of(i * MT, MT), MT)
            zo[r, :] = zo[r, :] + jnp.dot(hl[r, :], w2l[s], preferred_element_type=F32)

    def late_step(near, k, s, before):
        off = NE if near else NE + NL
        quad = quads_near(s, NE + k) if near else quads_far(s, k)
        for c in quad[:2] + (late_near(s, k) if near else late_far(s, k)):
            c.start()
        (x_w1(NE + k) if near else x_co(k)).wait_recv()
        f = f_w1(off + k)
        f.start()
        quad[2].start()
        before()
        wait_tiles(s, 0)
        wait_tiles(s, 1)
        layer1(hl, 0, 0, R, s, 0)
        f.wait_recv()
        quad[3].start()

    @pl.loop(0, NL)
    def _(k):
        s = lax.rem(NE + k, 2)

        def before():
            @pl.when(k > 0)
            def _():
                second(1 - s)

        late_step(True, k, s, before)

    @pl.loop(0, NL - 2)
    def _(k):
        s = lax.rem(NE + NL + k, 2)
        late_step(False, k, s, lambda: second(1 - s))

    k, s = NL - 2, (NE + 2 * NL - 2) % 2
    second(1 - s)
    late_step(False, k, s, lambda: None)
    s = 1 - s
    for h in range(2):
        for o, (wk, blk) in enumerate(((co, cx), (cp, 1 - cx))):
            pltpu.make_async_copy(wk.at[:, cols_last(h)], w1s.at[s, klo, part(h, o)], lw.at[s, 0]).start()
            for c, src in enumerate((eo, ep)):
                pltpu.make_async_copy(src.at[blk, cols_last(h), :],
                                      w2l.at[s, part(h, o), pl.ds(c * C2, C2)], lu.at[s]).start()

    def sent(n):
        two = pl.ds(2 * n, 2)
        return remote(zs.at[two], ry.at[two], zys.at[n], zyr.at[0], Y)

    wait_tiles(1 - s, 2)
    layer1(hl, WC, 0, R, 1 - s, 1)
    x_part(0).wait_recv()
    f_part(0).start()
    layer2(1 - s)
    sent(0).wait_send()
    wait_tiles(s, 0)
    f_part(0).wait_recv()
    layer1d(hl, 0, 0, R, s, 0, 1)
    wait_w2l(s)

    @pl.loop(0, NP)
    def _(i):
        r = pl.ds(pl.multiple_of(i * MT, MT), MT)
        zo[r, :] = zo[r, :] + jnp.dot(hl[r, lo_c], w2l[s, lo_c, :], preferred_element_type=F32)

    def take():
        x_part(1).wait_recv()
        f_part(1).start()

    pl.when(cx == 1)(take)

    @pl.loop(0, NP)
    def _(i):
        r = pl.ds(pl.multiple_of(i * MT, MT), MT)
        zs[0, r, :] = jnp.dot(xg[r, klo], w1s[s, klo, hi_c], preferred_element_type=F32)
        pl.when((cx == 0) & (i == 0))(take)

    f_part(1).wait_recv()
    c = zs[0] + jnp.dot(xg[own, khi], w1d[1, :, hi_c], preferred_element_type=F32)
    hl[:, hi_c] = gelu(c.astype(BF16).astype(F32)).astype(BF16)

    def finish(q, i, n=MT):
        r, l = pl.ds(i * n, n), pl.ds(q * QC, QC)
        half, c = divmod(q, NQ // 2)
        lanes = pl.multiple_of((1 - cx if half else cx) * C2 + c * QC, QC)
        z = zo[r, l] + jnp.dot(hl[r, hi_c], w2l[s, hi_c, l], preferred_element_type=F32)
        out[r, pl.ds(lanes, QC)] = (z + ry[q, r, :]).astype(BF16)

    few = pl.ds(0, NQ - 1)
    remote(zs.at[few], ry.at[few], zys.at[0], zyr.at[0], Y).wait_recv()
    for q in range(NQ - 1):
        for i in range(NP):
            finish(q, i)
    for i in range(R // ET):
        z_y(NQ - 1, i, ET).wait_recv()
        finish(NQ - 1, i, ET)
    sent(1).wait_send()
    remote(bo, bp, ws, wr.at[0], X).wait_send()
    remote(bo, bp, fs, fr.at[0], D).wait_send()
    remote(w1, ap, ys, yr.at[0], Y).wait_send()
    for c in (x_x, d_w1, d_w2, d_co, d_eo):
        c.wait_send()


def solution(mesh):
    data_spec = P(('dp', 'cx', 'cz'), 'cy')
    up_spec = P('cy', ('cz', 'cx'))
    down_spec = P('cz', ('cy', 'cx'))

    def local_mlp(x, w1, w2):
        R, K = x.shape
        B1 = w1.shape[1]
        WC = B1 // (NE + NL)
        EC, LC = NE * WC, NL * WC
        C2 = w2.shape[1]
        QC = 2 * C2 // NQ
        NX = NE + 2 * NL
        dma = pltpu.SemaphoreType.DMA
        any_spec = pl.BlockSpec(memory_space=pl.ANY)
        sds = jax.ShapeDtypeStruct
        outs = (
            pltpu.VMEM((R, K), BF16),
            sds(w1.shape, BF16),
            sds((NX, K, WC), BF16),
            sds((NX, K, WC), BF16),
            sds((K, LC), BF16),
            sds((K, LC), BF16),
            sds(w2.shape, BF16),
            sds((2, LC, C2), BF16),
            sds((2, LC, C2), BF16),
        )
        scratch = [
            pltpu.VMEM((2 * R, 2 * K), BF16),
            pltpu.VMEM((2 * R, 2 * EC), BF16),
            pltpu.VMEM((R, 2 * WC), BF16),
            pltpu.VMEM((2, 2 * K, 2 * WC), BF16),
            pltpu.VMEM((2, K, 2 * WC), BF16),
            pltpu.VMEM((2, 2 * EC, QC), BF16),
            pltpu.VMEM((2, 2 * WC, 2 * C2), BF16),
            pltpu.VMEM((NQ, R, QC), F32),
            pltpu.VMEM((NQ, R, QC), F32),
            pltpu.VMEM((R, 2 * C2), F32),
            dma((1,)), dma((2, 3)), dma((2,)), dma((2,)),
            dma((1,)), dma((1,)),
            dma, dma((NX + 1,)),
            dma, dma((4,)),
            dma((2,)), dma((1 + R // ET,)),
            dma((4,)), dma((4,)),
            dma, dma((2,)),
        ]
        return pl.pallas_call(
            kernel,
            out_shape=outs,
            in_specs=[any_spec] * 3,
            out_specs=(pl.BlockSpec(memory_space=pltpu.VMEM),) + (any_spec,) * (len(outs) - 1),
            scratch_shapes=scratch,
            compiler_params=pltpu.CompilerParams(
                collective_id=0, has_side_effects=True, vmem_limit_bytes=67043328 - 2 * R * K),
            name='mlp',
        )(x, w1, w2)[0]

    return jax.shard_map(local_mlp, mesh=mesh, in_specs=(data_spec, up_spec, down_spec), out_specs=data_spec, check_vma=False)
```
